32 devices in a mesh: gx: 2 (over core), gy: 4 (over y, x), gz: 4 (over z).
Axes of the slice: x: 2, y: 2, z: 4, core: 2. Of those that a mesh axis runs over, the one named last changes fastest.
Arguments:
- displacement: float32 [3, 12, 24, 1536], P(None, 'gx', 'gy', 'gz'), may hold values from -0.18 to 0.18
- size_field_modes: float32 [27, 4, 8, 512], P(None, 'gx', 'gy', 'gz'), may hold values from -6 to 6
- velocity: float32 [3, 4, 8, 512], P(None, 'gx', 'gy', 'gz'), may hold values from -1 to 1
Outputs:
- advected_field: float32 [27, 4, 8, 512], P(None, 'gx', 'gy', 'gz')
- gradient: float32 [3, 12, 24, 1536], P(None, 'gx', 'gy', 'gz')
- checks: float32 [3], replicated
The draws below stay inside these ranges and needn't reach their ends.
All inputs are finite; a program needn't handle non-finite values. Where the reference program divides by a largest or mean magnitude, that divisor is 1e-20 or more.
Results may differ from the reference program's by a relative error of at most 0.0001.
Values sent between devices are 32-bit elements; how exact they have to be, the bound alone decides.
A program may use at most 64 MiB of HBM per device.

```python
import math
import jax
import jax.numpy as jnp
import numpy as np
from jax import lax

LOCAL_ELEMS_X = 2
LOCAL_ELEMS_Y = 2
LOCAL_ELEMS_Z = 128
SUBSTEPS = 4
GLOBAL_ELEMS_X = 4
GLOBAL_ELEMS_Y = 8
GLOBAL_ELEMS_Z = 512
ELEMENTS = 16384


def draw_size_field_modes(key, part):
    random_key_noise, random_key_blocks = jax.random.split(key)
    noise_component = jnp.clip(0.5 * jax.random.normal(random_key_noise, (27, GLOBAL_ELEMS_X, GLOBAL_ELEMS_Y, GLOBAL_ELEMS_Z), jnp.float32), -3.0, 3.0)
    block_list = jax.random.uniform(random_key_blocks, (GLOBAL_ELEMS_X // LOCAL_ELEMS_X, GLOBAL_ELEMS_Y // LOCAL_ELEMS_Y, GLOBAL_ELEMS_Z // LOCAL_ELEMS_Z), jnp.float32, -3.0, 3.0)
    offset = jnp.repeat(jnp.repeat(jnp.repeat(block_list, LOCAL_ELEMS_X, axis=0), LOCAL_ELEMS_Y, axis=1), LOCAL_ELEMS_Z, axis=2)
    return noise_component.at[0].add(offset)


def draw_velocity(key, part):
    random_key_heading, random_key_scale = jax.random.split(key)
    heading_text = jax.random.uniform(random_key_heading, (3, GLOBAL_ELEMS_X, GLOBAL_ELEMS_Y, GLOBAL_ELEMS_Z), jnp.float32, -1.0, 1.0)
    scale_factors = jnp.exp(jax.random.uniform(random_key_scale, (GLOBAL_ELEMS_X // LOCAL_ELEMS_X, GLOBAL_ELEMS_Y // LOCAL_ELEMS_Y, GLOBAL_ELEMS_Z // LOCAL_ELEMS_Z), jnp.float32, math.log(0.15), 0.0))
    expanded = jnp.repeat(jnp.repeat(jnp.repeat(scale_factors, LOCAL_ELEMS_X, axis=0), LOCAL_ELEMS_Y, axis=1), LOCAL_ELEMS_Z, axis=2)
    return heading_text * expanded[None]


def block_levels(rng, shape, shards, low, largest):
    gain = 1.0
    for axis_at, blocks in shards:
        draws = jax.random.uniform(jax.random.fold_in(jax.random.fold_in(rng, 6), axis_at), (blocks,), jnp.float32, low / len(shards), largest / len(shards))
        gain = gain * jnp.repeat(jnp.exp(draws), shape[axis_at] // blocks).reshape((-1,) + (1,) * (len(shape) - 1 - axis_at))
    return gain


def normal_values(own_key, shape, scale, most, cuts=(), kind=jnp.bfloat16):
    drawn = jax.random.normal(own_key, shape, jnp.float32) * scale
    if len(cuts) > 0:
        drawn = block_levels(own_key, shape, cuts, -0.22, 0.18) * drawn
    return jnp.clip(drawn, min=-most, max=most).astype(kind)


def setup_inputs(seed: int = 0) -> dict:
    key_list = jax.random.split(jax.random.key(seed), 4)
    displacement = normal_values(key_list[0], (3, 3 * GLOBAL_ELEMS_X, 3 * GLOBAL_ELEMS_Y, 3 * GLOBAL_ELEMS_Z), 0.03, 0.18, ((1, 2), (2, 4), (3, 4)), jnp.float32)
    size_field_modes = draw_size_field_modes(jax.random.fold_in(key_list[3], 71), 0)
    velocity = draw_velocity(jax.random.fold_in(key_list[3], 71), 0)
    return {"displacement": displacement, "size_field_modes": size_field_modes, "velocity": velocity}


root_half = 0.7071067811865476
root_three_half = 1.224744871391589
root_five_half = 1.5811388300841898
plus_values = (0.7071067811865476, 1.224744871391589, 1.5811388300841898)
minus_values = (0.7071067811865476, -1.224744871391589, 1.5811388300841898)
stiffness = ((0.0, 0.0, 0.0), (1.7320508075688772, 0.0, 0.0), (0.0, 3.872983346207417, 0.0))
courant = 0.1
theta_size = 0.3
trial_step = 0.05

def build_tables():
    points = np.array([-0.8611363115940526, -0.3399810435848563, 0.3399810435848563, 0.8611363115940526])
    weights = np.array([0.3478548451374538, 0.6521451548625461, 0.6521451548625461, 0.3478548451374538])
    points = 0.5 * (points + 1.0)
    weights = 0.5 * weights
    node_points = np.array([0.0, 1.0 / 3.0, 2.0 / 3.0, 1.0])
    value_table = np.zeros((4, 4))
    slope_table = np.zeros((4, 4))
    for column in range(4):
        others = [node_points[member] for member in range(4) if member != column]
        denominator = np.prod([node_points[column] - member for member in others])
        for quad_row in range(4):
            gauss_point = points[quad_row]
            value_table[quad_row, column] = np.prod([gauss_point - member for member in others]) / denominator
            slope_table[quad_row, column] = sum((np.prod([gauss_point - others[position] for position in range(3) if position != skipped]) for skipped in range(3))) / denominator
    centred = 2.0 * points - 1.0
    legendre_table = np.stack([np.full(4, root_half), root_three_half * centred, root_five_half * 0.5 * (3.0 * centred ** 2 - 1.0)], axis=1)
    cube_table = (weights[:, None, None] * weights[None, :, None] * weights[None, None, :]).reshape(4, 4, 4, 1, 1, 1)
    return (value_table, slope_table, legendre_table, cube_table)

def as_table(operand):
    return jnp.asarray(np.asarray(operand), jnp.float32)

def contract(weights_table, operand, along):
    product = jnp.tensordot(as_table(weights_table), operand, axes=([1], [along]), precision=lax.Precision.HIGHEST)
    return jnp.moveaxis(product, 0, along)

def trace_along(modal_coefficients, vector, direction):
    return jnp.tensordot(as_table(vector), modal_coefficients, axes=([0], [direction]), precision=lax.Precision.HIGHEST)

def spread_shape(vector, direction):
    broadcast_shape = [1] * 6
    broadcast_shape[direction] = 3
    return as_table(vector).reshape(broadcast_shape)

def boundary_terms(modal_coefficients, local_speed, right_ext, left_ext, speed_ext, direction):
    extent = modal_coefficients.shape[3 + direction]
    face_speed = 0.5 * (lax.slice_in_dim(speed_ext, 0, extent + 1, axis=direction) + lax.slice_in_dim(speed_ext, 1, extent + 2, axis=direction))
    flux = jnp.maximum(face_speed, 0.0)[None, None] * right_ext + jnp.minimum(face_speed, 0.0)[None, None] * left_ext
    flux_left = lax.slice_in_dim(flux, 0, extent, axis=2 + direction)
    flux_right = lax.slice_in_dim(flux, 1, extent + 1, axis=2 + direction)
    lifted = contract(stiffness, modal_coefficients, direction)
    faces = spread_shape(plus_values, direction) * jnp.expand_dims(flux_right, direction) - spread_shape(minus_values, direction) * jnp.expand_dims(flux_left, direction)
    return local_speed[None, None, None] * lifted - faces

def element_energy(corners, modal_coefficients):
    lagrange_values, lagrange_slopes, legendre_values, cube_weights = build_tables()
    along_value = contract(lagrange_values, corners, 1)
    along_slope = contract(lagrange_slopes, corners, 1)
    value_value = contract(lagrange_values, along_value, 2)
    jac_first = contract(lagrange_values, contract(lagrange_values, along_slope, 2), 3)
    jac_second = contract(lagrange_values, contract(lagrange_slopes, along_value, 2), 3)
    jac_third = contract(lagrange_slopes, value_value, 3)
    columns = (jac_first, jac_second, jac_third)
    sample = contract(legendre_values, contract(legendre_values, contract(legendre_values, modal_coefficients, 0), 1), 2)
    target_size = jnp.exp(theta_size * sample)
    inverse = 1.0 / target_size
    mapped = [[((1.0 if component == column else 0.0) + columns[column][component]) * inverse for column in range(3)] for component in range(3)]
    metric = jnp.zeros_like(sample)
    for first_column in range(3):
        for second_column in range(3):
            gram_entry = mapped[0][first_column] * mapped[0][second_column] + mapped[1][first_column] * mapped[1][second_column] + mapped[2][first_column] * mapped[2][second_column]
            deviation = gram_entry - (1.0 if first_column == second_column else 0.0)
            metric = metric + deviation * deviation
    return jnp.sum(as_table(cube_weights) * target_size ** 3 * metric)

def element_corners(padded):
    gathered = padded
    for along, stack_axis in ((1, 1), (3, 2), (5, 3)):
        extent = (gathered.shape[along] - 1) // 3
        gathered = jnp.stack([lax.slice_in_dim(gathered, node_offset, node_offset + 3 * extent - 2, stride=3, axis=along) for node_offset in range(4)], axis=stack_axis)
    return gathered

def pad_one(operand, node_offset, along):
    config = [(0, 0, 0)] * operand.ndim
    config[along] = (node_offset, 3 - node_offset, 2)
    return lax.pad(operand, jnp.zeros((), operand.dtype), config)

def spread_corners(corner_grad):
    spread = corner_grad
    for stack_axis, along in ((3, 5), (2, 3), (1, 1)):
        pieces = [pad_one(lax.index_in_dim(spread, node_offset, axis=stack_axis, keepdims=False), node_offset, along) for node_offset in range(4)]
        spread = pieces[0] + pieces[1] + pieces[2] + pieces[3]
    return spread

def advection_rate(modal_coefficients, velocity):
    accumulated = jnp.zeros_like(modal_coefficients)
    for direction in range(3):
        element_axis = 2 + direction
        extent = modal_coefficients.shape[3 + direction]
        local_speed = velocity[direction]
        speed_ext = jnp.concatenate([lax.slice_in_dim(local_speed, extent - 1, extent, axis=direction), local_speed, lax.slice_in_dim(local_speed, 0, 1, axis=direction)], axis=direction)
        right_trace = trace_along(modal_coefficients, plus_values, direction)
        left_trace = trace_along(modal_coefficients, minus_values, direction)
        right_ext = jnp.concatenate([lax.slice_in_dim(right_trace, extent - 1, extent, axis=element_axis), right_trace], axis=element_axis)
        left_ext = jnp.concatenate([left_trace, lax.slice_in_dim(left_trace, 0, 1, axis=element_axis)], axis=element_axis)
        accumulated = accumulated + boundary_terms(modal_coefficients, local_speed, right_ext, left_ext, speed_ext, direction)
    return 2.0 * accumulated

def periodic_pad(nodal):
    for along in (1, 2, 3):
        nodal = jnp.concatenate([nodal, lax.slice_in_dim(nodal, 0, 1, axis=along)], axis=along)
    return nodal

def periodic_fold(gradient_pad):
    for along in (1, 2, 3):
        extent = gradient_pad.shape[along] - 1
        gradient_pad = jnp.concatenate([lax.slice_in_dim(gradient_pad, 0, 1, axis=along) + lax.slice_in_dim(gradient_pad, extent, extent + 1, axis=along), lax.slice_in_dim(gradient_pad, 1, extent, axis=along)], axis=along)
    return gradient_pad

def gradient_scan(padded, modal_coefficients):

    def advance(running, slab_start):
        energy_sum, gradient_pad = running
        nodes_slab = lax.dynamic_slice_in_dim(padded, 3 * slab_start, 4, axis=1)
        field_slab = lax.dynamic_slice_in_dim(modal_coefficients, slab_start, 1, axis=3)
        energy_here, corner_grad = jax.value_and_grad(element_energy)(element_corners(nodes_slab), field_slab)
        contribution = spread_corners(corner_grad)
        current = lax.dynamic_slice_in_dim(gradient_pad, 3 * slab_start, 4, axis=1)
        gradient_pad = lax.dynamic_update_slice_in_dim(gradient_pad, current + contribution, 3 * slab_start, axis=1)
        return ((energy_sum + energy_here, gradient_pad), None)
    start_value = (jnp.zeros((), jnp.float32), jnp.zeros_like(padded))
    finished, unused = lax.scan(advance, start_value, jnp.arange(GLOBAL_ELEMS_X, dtype=jnp.int32))
    return finished

def energy_scan(padded, modal_coefficients):

    def advance(energy_sum, slab_start):
        nodes_slab = lax.dynamic_slice_in_dim(padded, 3 * slab_start, 4, axis=1)
        field_slab = lax.dynamic_slice_in_dim(modal_coefficients, slab_start, 1, axis=3)
        return (energy_sum + element_energy(element_corners(nodes_slab), field_slab), None)
    finished, unused = lax.scan(advance, jnp.zeros((), jnp.float32), jnp.arange(GLOBAL_ELEMS_X, dtype=jnp.int32))
    return finished

def reference(displacement, size_field_modes, velocity):
    modal_coefficients = size_field_modes.reshape(3, 3, 3, GLOBAL_ELEMS_X, GLOBAL_ELEMS_Y, GLOBAL_ELEMS_Z)
    fastest = jnp.max(lax.optimization_barrier(jnp.sum(jnp.abs(velocity), axis=0)))
    time_step = courant / jnp.maximum(fastest, 0.25)
    for substep in range(SUBSTEPS):
        midway = modal_coefficients + time_step * advection_rate(modal_coefficients, velocity)
        modal_coefficients = 0.5 * modal_coefficients + 0.5 * (midway + time_step * advection_rate(midway, velocity))
    energy_total, gradient_pad = gradient_scan(periodic_pad(displacement), modal_coefficients)
    gradient = periodic_fold(gradient_pad)
    elements = 1.0 * ELEMENTS
    entries = 81.0 * ELEMENTS
    square_total = jnp.sum(gradient * gradient)
    step_length = trial_step / jnp.sqrt(1.0 + square_total / entries)
    trial_nodes = displacement - step_length * gradient
    trial_total = energy_scan(periodic_pad(trial_nodes), modal_coefficients)
    checks = jnp.stack([energy_total / elements, square_total / entries, trial_total / elements])
    return (modal_coefficients.reshape(27, GLOBAL_ELEMS_X, GLOBAL_ELEMS_Y, GLOBAL_ELEMS_Z), gradient, checks)
```

```python
import functools

import jax
import jax.numpy as jnp
import numpy as np
from jax import lax
from jax.experimental import pallas as pl
from jax.experimental.pallas import tpu as pltpu
from jax.sharding import PartitionSpec as P

SUBSTEPS = 4
MESH = pl.DeviceIdType.MESH
AXES = ("gx", "gy", "gz")

plus_values = (0.7071067811865476, 1.224744871391589, 1.5811388300841898)
g10 = 1.7320508075688772
g21 = 3.872983346207417
courant = 0.1
theta_size = 0.3
trial_step = 0.05


def tables_1d():
    points = np.array(
        [-0.8611363115940526, -0.3399810435848563, 0.3399810435848563, 0.8611363115940526]
    )
    weights = np.array(
        [0.3478548451374538, 0.6521451548625461, 0.6521451548625461, 0.3478548451374538]
    )
    points = 0.5 * (points + 1.0)
    weights = 0.5 * weights
    nodes = np.array([0.0, 1.0 / 3.0, 2.0 / 3.0, 1.0])
    value = np.zeros((4, 4))
    slope = np.zeros((4, 4))
    for m in range(4):
        others = [nodes[o] for o in range(4) if o != m]
        den = np.prod([nodes[m] - o for o in others])
        for q in range(4):
            g = points[q]
            value[q, m] = np.prod([g - o for o in others]) / den
            slope[q, m] = (
                sum(np.prod([g - others[t] for t in range(3) if t != s]) for s in range(3)) / den
            )
    c = 2.0 * points - 1.0
    legendre = np.stack(
        [
            np.full(4, plus_values[0]),
            plus_values[1] * c,
            plus_values[2] * 0.5 * (3.0 * c**2 - 1.0),
        ],
        axis=1,
    )
    return value, slope, legendre, weights


def row_tables(Y, Z):
    value, slope, legendre, weights = tables_1d()
    rows, nodes = 4 * Y, 3 * Y + 1
    tv = np.zeros((rows, rows))
    td = np.zeros((rows, rows))
    for e in range(Y):
        tv[4 * e : 4 * e + 4, 3 * e : 3 * e + 4] = value
        td[4 * e : 4 * e + 4, 3 * e : 3 * e + 4] = slope
    blocks = [tv[:, j] for j in range(nodes)] + [td[:, j] for j in range(nodes)]
    blocks += [tv[s, :] for s in range(rows)] + [td[s, :] for s in range(rows)]
    for b in range(3):
        for e in range(Y):
            col = np.zeros(rows)
            col[4 * e : 4 * e + 4] = legendre[:, b]
            blocks.append(col)
    blocks.append(np.tile(weights, Y))
    stacked = np.stack(blocks).astype(np.float32)
    return np.ascontiguousarray(np.broadcast_to(stacked[:, :, None], stacked.shape + (Z,)))


def kernel(sizes, X, Y, Z, disp_in, modes_in, vel_in, tab, adv, grad, checks,
           disp, GU, ZP, ZR, ZA, UM, WM, VM, CM, FM, US, WS, VS, CS, FT,
           perm, slab, U,
           RED, REDR, N, GN, A, G, J, B, SIZ, DT,
           NXR, NYS, NYR, NZS, NZR, FXR, FYS, FYR, FZS, FZR,
           ls, g1s, g1r, g2s, g2r, zs, zr, y2s, y2r, rs, rr, ns, nr, fs, fr):
    value, slope, legendre, weights = tables_1d()
    NX, NY = 3 * X, 3 * Y
    ROWS = 4 * Y
    EL = X * Y
    f32 = jnp.float32
    index = [lax.axis_index(a) for a in AXES]
    lane = lax.broadcasted_iota(jnp.int32, (ROWS, Z), 1)
    row = lax.broadcasted_iota(jnp.int32, (ROWS, Z), 0)
    oTV, oTD, oGV, oGD, oL, oW = 0, NY + 1, 2 * NY + 2, 2 * NY + 2 + ROWS, 2 * NY + 2 + 2 * ROWS, 2 * NY + 2 + 2 * ROWS + 3 * Y

    def at(axis, by):
        n = sizes[axis]
        return {AXES[axis]: lax.rem(index[axis] + (by + n), n)}

    loads = [
        pltpu.make_async_copy(modes_in, GU.at[0, 0, 0:27], ls.at[0]),
        pltpu.make_async_copy(vel_in, GU.at[0, 0, 27:30], ls.at[1]),
        pltpu.make_async_copy(disp_in, disp, ls.at[2]),
    ]
    for cp in loads:
        cp.start()
    barrier = pltpu.get_barrier_semaphore()
    total = 0
    for a in range(sizes[0]):
        for b in range(sizes[1]):
            for c in range(sizes[2]):
                move = (a, b, c)
                if not any(move):
                    continue
                target = {}
                for axis in range(3):
                    if move[axis]:
                        target.update(at(axis, move[axis]))
                pl.semaphore_signal(barrier, inc=1, device_id=target, device_id_type=MESH)
                total += 1

    def copy(src, dst, ss, sr, axis, by):
        return pltpu.make_async_remote_copy(
            src_ref=src, dst_ref=dst, send_sem=ss, recv_sem=sr,
            device_id=at(axis, by), device_id_type=MESH,
        )

    GX, GY = sizes[0], sizes[1]
    XG, YG, NS, EDGE = GX * X, GY * Y, GX * X // 2, 2 * SUBSTEPS
    HALF, FIELDS, SLOTS = Z // 2, 30, Z // EDGE

    def moved(move):
        target = {}
        for axis in range(3):
            if move[axis] % sizes[axis]:
                target.update(at(axis, move[axis] % sizes[axis] ))
        return target

    def remote(src, dst, ss, sr, move):
        return pltpu.make_async_remote_copy(
            src_ref=src, dst_ref=dst, send_sem=ss, recv_sem=sr,
            device_id=moved(move), device_id_type=MESH,
        )

    def plane_copy(ry):
        return remote(GU.at[0, 0], GU.at[0, ry], g1s.at[ry], g1r.at[ry], (0, -ry, 0))

    def core_copies(ry):
        return [
            remote(GU.at[0, ry], GU.at[rx, ry], g2s.at[rx, ry], g2r.at[rx, ry], (-rx, 0, 0))
            for rx in range(1, GX)
        ]

    def edge_copies():
        return [
            remote(ZP.at[side], ZR.at[0, ry, side], zs.at[side, ry], zr.at[side, ry], (0, -ry, 2 * side - 1))
            for side in range(2) for ry in range(GY)
        ]

    def edge_core_copies():
        return [
            remote(ZR.at[0], ZR.at[rx], y2s.at[rx], y2r.at[rx], (-rx, 0, 0)) for rx in range(1, GX)
        ]

    slot2 = lax.broadcasted_iota(jnp.int32, (Y, Z), 1) // EDGE
    packs = -(-FIELDS * X // SLOTS)

    def pack_edges():
        acc = [[jnp.zeros((Y, Z), f32) for _ in range(packs)] for _ in range(2)]
        for m in range(FIELDS):
            for ix in range(X):
                t = m * X + ix
                v, p = t // SLOTS, EDGE * (t % SLOTS)
                x = GU[0, 0, m, ix]
                low = pltpu.roll(x, p, 1) if p else x
                high = pltpu.roll(x, (p + EDGE) % Z, 1) if (p + EDGE) % Z else x
                acc[0][v] = jnp.where(slot2 == t % SLOTS, low, acc[0][v])
                acc[1][v] = jnp.where(slot2 == t % SLOTS, high, acc[1][v])
        for side in range(2):
            for v in range(packs):
                ZP[side, v] = acc[side][v]

    for cp in loads[:2]:
        cp.wait()
    RED[0, 0] = jnp.zeros_like(RED[0, 0])
    speed = None
    for ix in range(X):
        here = jnp.abs(GU[0, 0, 27, ix]) + jnp.abs(GU[0, 0, 28, ix]) + jnp.abs(GU[0, 0, 29, ix])
        speed = here if speed is None else jnp.maximum(speed, here)
    RED[0, 0, 0, 0:Y] = speed
    pack_edges()

    def unweave():
        a_i = lax.broadcasted_iota(jnp.int32, (3 * Z, 3 * Z), 0)
        b_i = lax.broadcasted_iota(jnp.int32, (3 * Z, 3 * Z), 1)
        b_k = (b_i >= Z).astype(jnp.int32) + (b_i >= 2 * Z).astype(jnp.int32)
        perm[...] = (a_i == 3 * (b_i - b_k * Z) + b_k).astype(f32)
        slab[...] = jnp.zeros_like(slab)
        for c in range(3):
            for i in range(NX):
                slab[c * NX + i, 0:NY, :] = disp[c, i]
        spread = jnp.dot(
            slab[...].reshape(3 * NX * ROWS, 3 * Z), perm[...],
            precision=lax.Precision.HIGHEST, preferred_element_type=f32,
        ).reshape(3, NX, ROWS, 3 * Z)
        for c in range(3):
            for k in range(3):
                N[c, 0:NX, k] = spread[c, :, :, k * Z : (k + 1) * Z]

    loads[2].wait()
    unweave()
    pl.semaphore_wait(barrier, total)
    for cp in core_copies(0):
        cp.start()
    for ry in range(1, GY):
        plane_copy(ry).start()
    for cp in edge_copies():
        cp.start()

    def peers_of(phase):
        if phase == 0:
            return [(by, 0, 0) for by in range(1, sizes[0])]
        return [(0, b, c) for b in range(sizes[1]) for c in range(sizes[2]) if b or c]

    def red_copies(r, phase):
        off = 0 if phase == 0 else sizes[0] - 1
        out = []
        for n, move in enumerate(peers_of(phase)):
            target = {}
            for axis in range(3):
                if move[axis]:
                    target.update(at(axis, move[axis]))
            out.append(pltpu.make_async_remote_copy(
                src_ref=RED.at[r, phase], dst_ref=REDR.at[r, off + n],
                send_sem=rs.at[r, off + n], recv_sem=rr.at[r, off + n],
                device_id=target, device_id_type=MESH,
            ))
        return out

    def red_start(r, phase):
        for cp in red_copies(r, phase):
            cp.start()

    def red_finish(r, phase, op):
        off = 0 if phase == 0 else sizes[0] - 1
        copies = red_copies(r, phase)
        for cp in copies:
            cp.wait_recv()
        total = RED[r, phase]
        for n in range(len(copies)):
            total = op(total, REDR[r, off + n])
        RED[r, phase + 1] = total

    def rim_x(a, t):
        return copy(a.at[:, 0, 0:3], NXR.at[t], ns.at[t, 0], nr.at[t, 0], 0, -1)

    def rim_y(t):
        return copy(NYS.at[t], NYR.at[t], ns.at[t, 1], nr.at[t, 1], 1, -1)

    def rim_y_pack(a, t):
        for c in range(3):
            for k in range(3):
                a[c, NX, k] = NXR[t, c, k]
        for c in range(3):
            for i in range(NX + 1):
                for k in range(3):
                    NYS[t, c, i, k : k + 1, :] = a[c, i, k, 0:1, :]

    def rim_y_unpack(a, t):
        for c in range(3):
            for i in range(NX + 1):
                for k in range(3):
                    a[c, i, k, NY : NY + 1, :] = NYR[t, c, i, k : k + 1, :]

    def rim_z(t):
        return copy(NZS.at[t], NZR.at[t], ns.at[t, 2], nr.at[t, 2], 2, -1)

    def rim_z_pack(a, t):
        packed = jnp.zeros((ROWS, Z), f32)
        for c in range(3):
            for i in range(NX + 1):
                packed = jnp.where(lane == c * (NX + 1) + i, a[c, i, 0][:, 0:1], packed)
        NZS[t] = packed

    def rim_z_unpack(a, t):
        packed = NZR[t]
        for c in range(3):
            for i in range(NX + 1):
                at_ = c * (NX + 1) + i
                a[c, i, 3] = jnp.where(lane == Z - 1, packed[:, at_ : at_ + 1], pltpu.roll(a[c, i, 0], Z - 1, 1))

    scale = [plus_values[m // 9] * plus_values[m // 3 % 3] * plus_values[m % 3] for m in range(27)]

    def assemble():
        def plane(x, carry):
            rx, ix = x // X, x % X
            for ry in range(GY):
                for m in range(FIELDS):
                    v = GU[rx, ry, m, ix]
                    if m < 27:
                        UM[m, x, ry * Y : ry * Y + Y, :] = scale[m] * v
                    else:
                        VM[m - 27, x, ry * Y : ry * Y + Y, :] = v
            return carry

        lax.fori_loop(0, XG, plane, 0)

    lanes = lax.broadcasted_iota(jnp.int32, (YG, Z), 1)
    W2, W3 = 2 * EDGE, 3 * EDGE

    def within(lo, hi):
        return (lanes >= lo) & (lanes < hi)

    def strip_own():
        def one(q, carry):
            for m in range(FIELDS):
                out = jnp.zeros((YG, Z), f32)
                for h in range(2):
                    t = UM[m, q + h * NS] if m < 27 else VM[m - 27, q + h * NS]
                    o = h * HALF
                    out = jnp.where(within(o, o + W2), pltpu.roll(t, o + W2, 1), out)
                    out = jnp.where(within(o + 2 * W2, o + 3 * W2), pltpu.roll(t, o + 2 * W2, 1), out)
                if m < 27:
                    US[m, q] = out
                else:
                    VS[m - 27, q] = out
            return carry

        lax.fori_loop(0, NS, one, 0)

    def strip_halo():
        for rx in range(GX):
            for ry in range(GY):
                ZA[rx, :, :, ry * Y : ry * Y + Y, :] = ZR[rx, ry]
        for q in range(NS):
            for m in range(FIELDS):
                out = US[m, q] if m < 27 else VS[m - 27, q]
                for h in range(2):
                    x = q + h * NS
                    rx, ix = x // X, x % X
                    t = m * X + ix
                    v, p = t // SLOTS, EDGE * (t % SLOTS)
                    for side in range(2):
                        o = h * HALF + W2 + side * EDGE
                        piece = ZA[rx, side, v]
                        by = (o - p) % Z
                        piece = pltpu.roll(piece, by, 1) if by else piece
                        if m < 27:
                            piece = scale[m] * piece
                        out = jnp.where(within(o, o + EDGE), piece, out)
                if m < 27:
                    US[m, q] = out
                else:
                    VS[m - 27, q] = out

    def ynext(t):
        return pltpu.roll(t, YG - 1, 0)

    def yprev(t):
        return pltpu.roll(t, 1, 0)

    def znext(t):
        return pltpu.roll(t, Z - 1, 1)

    def zprev(t):
        return pltpu.roll(t, 1, 1)

    def coefficients(V, C, nx, wrap):
        dt = DT[...]
        for q in range(nx):
            nxt = V[0, q + 1] if q < nx - 1 else wrap(V[0, 0])
            for d in range(3):
                v = V[d, q]
                ahead = nxt if d == 0 else ynext(v) if d == 1 else znext(v)
                face = (0.5 * dt) * (v + ahead)
                C[q, 3 * d] = jnp.maximum(face, 0.0)
                C[q, 3 * d + 1] = jnp.minimum(face, 0.0)
                C[q, 3 * d + 2] = (2.0 * dt) * v

    def line(u, hp, hm, v2, ahead, behind):
        e = u[0] + u[2]
        up = hp * (e + u[1]) + hm * ahead(e - u[1])
        low = behind(up)
        diff = low - up
        return diff, 3.0 * (v2 * u[0] - (low + up)), 5.0 * (v2 * u[1] + diff)

    def rate(src, C, F, nx, wrap, write):
        for n in range(9):
            tp, tm = [], []
            for q in range(nx):
                u0, u1, u2 = src[n, q], src[9 + n, q], src[18 + n, q]
                e = u0 + u2
                tp.append(e + u1)
                tm.append(e - u1)
            for q in range(nx):
                nxt = tm[q + 1] if q < nx - 1 else wrap(tm[0])
                f = C[q, 0] * tp[q] + C[q, 1] * nxt
                F[q + 1, n] = f
                if q == nx - 1:
                    F[0, n] = wrap(f)

        def block(q, carry):
            vx = C[q, 2]
            for a in range(3):
                u = [src[9 * a + n, q] for n in range(9)]
                acc = []
                for n in range(9):
                    up, low = F[q + 1, n], F[q, n]
                    if a == 0:
                        acc.append(low - up)
                    elif a == 1:
                        acc.append(3.0 * (vx * src[n, q] - (low + up)))
                    else:
                        acc.append(5.0 * (vx * src[9 + n, q] + (low - up)))
                for d, st, ot, ahead, behind in ((1, 3, 1, ynext, yprev), (2, 1, 3, znext, zprev)):
                    hp, hm, v2 = C[q, 3 * d], C[q, 3 * d + 1], C[q, 3 * d + 2]
                    for o in range(3):
                        at_ = [ot * o + st * t for t in range(3)]
                        out = line([u[t] for t in at_], hp, hm, v2, ahead, behind)
                        for t in range(3):
                            acc[at_[t]] = acc[at_[t]] + out[t]
                for n in range(9):
                    write(9 * a + n, q, acc[n])
            return carry

        lax.fori_loop(0, nx, block, 0)

    def advance(Ur, Wr, C, F, nx, wrap):
        def put(m, q, value):
            Wr[m, q] = value

        def step(m, q, value):
            Ur[m, q] = (Ur[m, q] + Wr[m, q]) + 0.5 * value

        def substep(t, carry):
            rate(Ur, C, F, nx, wrap, put)
            rate(Wr, C, F, nx, wrap, step)
            return carry

        lax.fori_loop(0, SUBSTEPS, substep, 0)

    def same(t):
        return t

    def half_turn(t):
        return pltpu.roll(t, HALF, 1)

    def finish_field():
        U[...] = jnp.zeros_like(U)
        for m in range(27):
            for ix in range(X):
                t = UM[m, ix]
                h, q = ix // NS, ix % NS
                s = US[m, q]
                o = h * HALF
                left = pltpu.roll(s, (Z - o - 2 * W2) % Z, 1)
                right = pltpu.roll(s, (Z - W2 - o) % Z, 1)
                t = jnp.where(lanes < EDGE, left, jnp.where(lanes >= Z - EDGE, right, t))
                U[m, ix * Y : ix * Y + Y, :] = (1.0 / scale[m]) * t[0:Y]

    def yz_of(src):
        def yz(i, carry):
            for c in range(3):
                yv, yd = [], []
                for k in range(4):
                    sv = sd = None
                    for j in range(NY + 1):
                        x = src[c, i, k, j : j + 1, :]
                        tv, td = tab[oTV + j] * x, tab[oTD + j] * x
                        sv = tv if sv is None else sv + tv
                        sd = td if sd is None else sd + td
                    yv.append(sv)
                    yd.append(sd)
                for r in range(4):
                    A[0, c, i, r] = sum(float(value[r, k]) * yv[k] for k in range(4))
                    A[1, c, i, r] = sum(float(value[r, k]) * yd[k] for k in range(4))
                    A[2, c, i, r] = sum(float(slope[r, k]) * yv[k] for k in range(4))
            return carry

        lax.fori_loop(0, NX + 1, yz, 0)

    def slope_at(ix, p, r, c, d):
        tb = slope if d == 0 else value
        return sum(float(tb[p, m]) * A[d, c, 3 * ix + m, r] for m in range(4))

    def jacobians(t):
        ix, r = t // 4, t % 4
        for p in range(4):
            for c in range(3):
                for d in range(3):
                    jac = slope_at(ix, p, r, c, d)
                    J[d, c, ix, p, r] = jac + 1.0 if c == d else jac

    red_start(0, 0)
    rim_x(N, 0).start()
    rim_x(N, 0).wait()
    rim_y_pack(N, 0)
    rim_y(0).start()
    red_finish(0, 0, jnp.maximum)
    red_start(0, 1)
    for ry in range(1, GY):
        plane_copy(ry).wait_recv()
        for cp in core_copies(ry):
            cp.start()
    rim_y(0).wait()
    rim_y_unpack(N, 0)
    rim_z_pack(N, 0)
    rim_z(0).start()
    for cp in edge_copies():
        cp.wait_recv()
    for cp in edge_core_copies():
        cp.start()
    red_finish(0, 1, jnp.maximum)
    fastest = jnp.max(RED[0, 2, 0], axis=(0, 1), keepdims=True)
    DT[...] = jnp.broadcast_to(courant / jnp.maximum(fastest, 0.25), (YG, Z))
    for ry in range(GY):
        for cp in core_copies(ry):
            cp.wait_recv()
    assemble()
    strip_own()
    coefficients(VM, CM, XG, same)
    advance(UM, WM, CM, FM, XG, same)
    for cp in edge_core_copies():
        cp.wait_recv()
    strip_halo()
    coefficients(VS, CS, NS, half_turn)
    advance(US, WS, CS, FT, NS, half_turn)
    finish_field()
    rim_z(0).wait()
    rim_z_unpack(N, 0)
    yz_of(N)

    def all_jacobians(t, carry):
        jacobians(t)
        return carry

    lax.fori_loop(0, 4 * X, all_jacobians, 0)

    def size_of(ix, carry):
        mid = {}
        for a in range(3):
            for r in range(4):
                mid[a, r] = None
            for c in range(3):
                t = None
                for b in range(3):
                    for e in range(Y):
                        term = tab[oL + b * Y + e] * U[a * 9 + b * 3 + c, pl.ds(ix * Y + e, 1), :]
                        t = term if t is None else t + term
                for r in range(4):
                    term = float(legendre[r, c]) * t
                    mid[a, r] = term if mid[a, r] is None else mid[a, r] + term
        for p in range(4):
            for r in range(4):
                s = sum(float(legendre[p, a]) * mid[a, r] for a in range(3))
                SIZ[ix, p, r] = jnp.exp(theta_size * s)
        return carry

    lax.fori_loop(0, X, size_of, 0)

    wrow = tab[oW]
    pairs = [(d, e) for d in range(3) for e in range(d, 3)]

    def dot3(p, q, d, e):
        return p[0][d] * q[0][e] + p[1][d] * q[1][e] + p[2][d] * q[2][e]

    def gauss_weight(r):
        return jnp.where((r == 0) | (r == 3), float(weights[0]), float(weights[1]))

    def gauss(t, esum):
        ix, r = t // 4, t % 4
        for p in range(4):
            size = SIZ[ix, p, r]
            inv = 1.0 / size
            M = [[J[d, c, ix, p, r] * inv for d in range(3)] for c in range(3)]
            D = [[None] * 3 for _ in range(3)]
            metric = None
            for d, e in pairs:
                dev = dot3(M, M, d, e)
                if d == e:
                    dev = dev - 1.0
                D[d][e] = D[e][d] = dev
                sq = dev * dev if d == e else 2.0 * (dev * dev)
                metric = sq if metric is None else metric + sq
            w = wrow * (gauss_weight(r) * float(weights[p]))
            size2 = size * size
            esum = esum + w * (size2 * size) * metric
            scale = (4.0 * w) * size2
            for c in range(3):
                for d in range(3):
                    g = M[c][0] * D[0][d] + M[c][1] * D[1][d] + M[c][2] * D[2][d]
                    G[d, c, ix, p, r] = scale * g
        return esum

    zero = jnp.zeros((ROWS, Z), f32)
    esum = lax.fori_loop(0, 4 * X, gauss, zero)

    def back_c(c, carry):
        for i in range(NX + 1):
            bv = [None] * 4
            bd = [None] * 4
            for r in range(4):
                ga = []
                for d in range(3):
                    tb = slope if d == 0 else value
                    acc = None
                    for ix in range(X):
                        m = i - 3 * ix
                        if 0 <= m <= 3:
                            for p in range(4):
                                term = float(tb[p, m]) * G[d, c, ix, p, r]
                                acc = term if acc is None else acc + term
                    ga.append(acc)
                for k in range(4):
                    tv = float(value[r, k]) * ga[0] + float(slope[r, k]) * ga[2]
                    td = float(value[r, k]) * ga[1]
                    bv[k] = tv if bv[k] is None else bv[k] + tv
                    bd[k] = td if bd[k] is None else bd[k] + td
            for k in range(4):
                B[0, i, k] = bv[k]
                B[1, i, k] = bd[k]
        for i in range(NX + 1):
            for k in range(4):
                acc = None
                for s in range(ROWS):
                    term = tab[oGV + s] * B[0, i, k, s : s + 1, :] + tab[oGD + s] * B[1, i, k, s : s + 1, :]
                    acc = term if acc is None else acc + term
                GN[c, i, k] = acc
        return carry

    lax.fori_loop(0, 3, back_c, 0)

    def both_ways(src_up, src_down, axis, slot, up, down):
        copies = [
            copy(src_up, up, fs.at[slot], fr.at[slot], axis, 1),
            copy(src_down, down, fs.at[slot + 1], fr.at[slot + 1], axis, -1),
        ]
        for cp in copies:
            cp.start()
        for cp in copies:
            cp.wait()

    up, down = zero, zero
    for c in range(3):
        for i in range(NX + 1):
            here = lane == c * (NX + 1) + i
            up = jnp.where(here, GN[c, i, 3][:, Z - 1 : Z], up)
            down = jnp.where(here, GN[c, i, 0][:, 0:1], down)
    FZS[0] = up
    FZS[1] = down
    both_ways(FZS.at[0], FZS.at[1], 2, 0, FZR.at[0], FZR.at[1])
    up, down = FZR[0], FZR[1]
    for c in range(3):
        for i in range(NX + 1):
            n = c * (NX + 1) + i
            g0, g3 = GN[c, i, 0], GN[c, i, 3]
            full = g0 + jnp.where(lane == 0, up[:, n : n + 1], pltpu.roll(g3, 1, 1))
            GN[c, i, 0] = full
            GN[c, i, 3] = jnp.where(lane == Z - 1, g3 + down[:, n : n + 1], pltpu.roll(full, Z - 1, 1))
    both_ways(GN.at[:, NX], GN.at[:, 0], 0, 2, FXR.at[0], FXR.at[1])
    for c in range(3):
        for k in range(4):
            GN[c, 0, k] = GN[c, 0, k] + FXR[0, c, k]
            GN[c, NX, k] = GN[c, NX, k] + FXR[1, c, k]
    for c in range(3):
        for i in range(NX + 1):
            for k in range(4):
                FYS[0, c, i, k : k + 1, :] = GN[c, i, k, NY : NY + 1, :]
                FYS[1, c, i, k : k + 1, :] = GN[c, i, k, 0:1, :]
    both_ways(FYS.at[0], FYS.at[1], 1, 4, FYR.at[0], FYR.at[1])
    for c in range(3):
        for i in range(NX + 1):
            for k in range(4):
                GN[c, i, k, 0:1, :] = GN[c, i, k, 0:1, :] + FYR[0, c, i, k : k + 1, :]
                GN[c, i, k, NY : NY + 1, :] = GN[c, i, k, NY : NY + 1, :] + FYR[1, c, i, k : k + 1, :]
    ssum = zero
    for c in range(3):
        for i in range(NX):
            for k in range(3):
                g = GN[c, i, k]
                ssum = ssum + g * g
    ssum = jnp.where(row < NY, ssum, 0.0)
    devices = sizes[0] * sizes[1] * sizes[2]
    elements = float(EL * Z * devices)
    entries = 81.0 * elements
    mine = jnp.sum(ssum, axis=(0, 1), keepdims=True)
    bound = trial_step / jnp.sqrt(1.0 + mine / entries)
    bound = jnp.broadcast_to(bound, (ROWS, Z))
    yz_of(GN)

    def trial(t, sums):
        ix, r = t // 4, t % 4
        s1, s2, s3, s4 = sums
        for p in range(4):
            size = SIZ[ix, p, r]
            inv = 1.0 / size
            move = -(inv * bound)
            M = [[J[d, c, ix, p, r] * inv for d in range(3)] for c in range(3)]
            K = [[slope_at(ix, p, r, c, d) * move for d in range(3)] for c in range(3)]
            w = wrow * (gauss_weight(r) * float(weights[p])) * (size * size * size)
            q = [None] * 4
            for d, e in pairs:
                d0 = dot3(M, M, d, e)
                d2 = dot3(K, K, d, e)
                if d == e:
                    d0 = d0 - 1.0
                    d1 = 2.0 * dot3(M, K, d, d)
                else:
                    d1 = dot3(M, K, d, e) + dot3(K, M, d, e)
                terms = [2.0 * (d0 * d1), d1 * d1 + 2.0 * (d0 * d2), 2.0 * (d1 * d2), d2 * d2]
                for n in range(4):
                    term = terms[n] if d == e else 2.0 * terms[n]
                    q[n] = term if q[n] is None else q[n] + term
            s1, s2, s3, s4 = s1 + w * q[0], s2 + w * q[1], s3 + w * q[2], s4 + w * q[3]
        return s1, s2, s3, s4

    sums = lax.fori_loop(0, 4 * X, trial, (zero,) * 4)
    block = zero
    for n, part in enumerate((esum, ssum) + tuple(sums)):
        block = jnp.where(row == n, jnp.sum(part, axis=0, keepdims=True), block)
    column = jnp.sum(block, axis=1, keepdims=True)
    column = jnp.where(row == 6, bound, jnp.broadcast_to(column, (ROWS, Z)))
    me = (index[0] * sizes[1] + index[1]) * sizes[2] + index[2]
    groups = RED.shape[2]
    for n in range(groups):
        RED[1, 0, n] = jnp.where(lane + n * Z == me, column, 0.0)
    red_start(1, 0)
    for c in range(3):
        for k in range(3):
            slab[c * NX : (c + 1) * NX, :, k * Z : (k + 1) * Z] = GN[c, 0:NX, k]
    red_finish(1, 0, jnp.add)
    red_start(1, 1)
    woven = lax.dot_general(
        slab[...].reshape(3 * NX * ROWS, 3 * Z), perm[...], (((1,), (1,)), ((), ())),
        precision=lax.Precision.HIGHEST, preferred_element_type=f32,
    ).reshape(3, NX, ROWS, 3 * Z)
    grad[...] = woven[:, :, 0:NY, :]
    for ix in range(X):
        adv[:, ix] = U[:, ix * Y : ix * Y + Y, :]
    red_finish(1, 1, jnp.add)
    every = [RED[1, 2, n] for n in range(groups)]

    def over_all(parts):
        return sum(jnp.sum(x, axis=1, keepdims=True) for x in parts)

    etot = over_all([x[0:1] for x in every])
    stot = over_all([x[1:2] for x in every])
    step = trial_step / jnp.sqrt(1.0 + stot / entries)
    parts = []
    for n, x in enumerate(every):
        own = jnp.where(lane[0:1] + n * Z < devices, x[6:7], 1.0)
        h = step / own
        parts.append(x[0:1] + h * (x[2:3] + h * (x[3:4] + h * (x[4:5] + h * x[5:6]))))
    ttot = over_all(parts)
    for ry in range(GY):
        if ry:
            plane_copy(ry).wait_send()
        for cp in core_copies(ry):
            cp.wait_send()
    for cp in edge_copies() + edge_core_copies():
        cp.wait_send()
    for r in range(2):
        for phase in range(2):
            for cp in red_copies(r, phase):
                cp.wait_send()
    l1 = lax.broadcasted_iota(jnp.int32, (1, Z), 1)
    checks[...] = jnp.where(
        l1 == 0, etot / elements, jnp.where(l1 == 1, stot / entries, ttot / elements)
    )


def solution(mesh):
    sizes = tuple(mesh.shape[a] for a in AXES)

    def on_device(displacement, size_field_modes, velocity):
        modes, X, Y, Z = size_field_modes.shape
        assert Y == 2 and displacement.shape == (3, 3 * X, 3 * Y, 3 * Z)
        R, NX, NY = 4 * Y, 3 * X, 3 * Y
        tab = jnp.asarray(row_tables(Y, Z))
        peers = sizes[0] - 1 + sizes[1] * sizes[2] - 1
        groups = -(-sizes[0] * sizes[1] * sizes[2] // Z)
        GX, GY = sizes[0], sizes[1]
        XG, YG, NS = GX * X, GY * Y, GX * X // 2
        packs = -(-30 * X // (Z // (2 * SUBSTEPS)))
        assert YG == 8 and XG % 2 == 0 and min(sizes) > 1
        vm = lambda *shape: pltpu.VMEM(shape, jnp.float32)
        dma = lambda *shape: pltpu.SemaphoreType.DMA(shape)
        spec = pl.BlockSpec(memory_space=pltpu.VMEM)
        adv, grad, checks = pl.pallas_call(
            functools.partial(kernel, sizes, X, Y, Z),
            out_shape=(
                jax.ShapeDtypeStruct(size_field_modes.shape, jnp.float32),
                jax.ShapeDtypeStruct(displacement.shape, jnp.float32),
                jax.ShapeDtypeStruct((1, Z), jnp.float32),
            ),
            in_specs=[pl.BlockSpec(memory_space=pl.ANY)] * 3 + [spec],
            out_specs=(spec,) * 3,
            scratch_shapes=[
                vm(3, NX, NY, 3 * Z), vm(GX, GY, 30, X, Y, Z), vm(2, packs, Y, Z), vm(GX, GY, 2, packs, Y, Z), vm(GX, 2, packs, YG, Z),
                vm(27, XG, YG, Z), vm(27, XG, YG, Z), vm(3, XG, YG, Z), vm(XG, 9, YG, Z), vm(XG + 1, 9, YG, Z),
                vm(27, NS, YG, Z), vm(27, NS, YG, Z), vm(3, NS, YG, Z), vm(NS, 9, YG, Z), vm(NS + 1, 9, YG, Z),
                vm(3 * Z, 3 * Z), vm(3 * NX, R, 3 * Z), vm(27, R, Z),
                vm(2, 3, groups, R, Z), vm(2, peers, groups, R, Z),
                vm(3, NX + 1, 4, R, Z), vm(3, NX + 1, 4, R, Z),
                vm(3, 3, NX + 1, 4, R, Z), vm(3, 3, X, 4, 4, R, Z), vm(3, 3, X, 4, 4, R, Z), vm(2, NX + 1, 4, R, Z), vm(X, 4, 4, R, Z), vm(R, Z),
                vm(1, 3, 3, R, Z), vm(1, 3, NX + 1, 3, Z), vm(1, 3, NX + 1, 3, Z), vm(1, R, Z), vm(1, R, Z),
                vm(2, 3, 4, R, Z), vm(2, 3, NX + 1, 4, Z), vm(2, 3, NX + 1, 4, Z), vm(2, R, Z), vm(2, R, Z),
                dma(3), dma(GY), dma(GY), dma(GX, GY), dma(GX, GY), dma(2, GY), dma(2, GY), dma(GX), dma(GX), dma(2, peers), dma(2, peers), dma(1, 3), dma(1, 3), dma(6), dma(6),
            ],
            compiler_params=pltpu.CompilerParams(collective_id=0, has_side_effects=True),
        )(displacement, size_field_modes, velocity, tab)
        return adv, grad, checks[0, 0:3]

    return jax.shard_map(
        on_device,
        mesh=mesh,
        in_specs=(P(None, "gx", "gy", "gz"),) * 3,
        out_specs=(P(None, "gx", "gy", "gz"), P(None, "gx", "gy", "gz"), P()),
        check_vma=False,
    )
```

```python
import functools

import jax
import jax.numpy as jnp
import numpy as np
from jax import lax
from jax.experimental import pallas as pl
from jax.experimental.pallas import tpu as pltpu
from jax.sharding import PartitionSpec as P

SUBSTEPS = 4
MESH = pl.DeviceIdType.MESH
AXES = ("gx", "gy", "gz")

plus_values = (0.7071067811865476, 1.224744871391589, 1.5811388300841898)
g10 = 1.7320508075688772
g21 = 3.872983346207417
courant = 0.1
theta_size = 0.3
trial_step = 0.05


def tables_1d():
    points = np.array(
        [-0.8611363115940526, -0.3399810435848563, 0.3399810435848563, 0.8611363115940526]
    )
    weights = np.array(
        [0.3478548451374538, 0.6521451548625461, 0.6521451548625461, 0.3478548451374538]
    )
    points = 0.5 * (points + 1.0)
    weights = 0.5 * weights
    nodes = np.array([0.0, 1.0 / 3.0, 2.0 / 3.0, 1.0])
    value = np.zeros((4, 4))
    slope = np.zeros((4, 4))
    for m in range(4):
        others = [nodes[o] for o in range(4) if o != m]
        den = np.prod([nodes[m] - o for o in others])
        for q in range(4):
            g = points[q]
            value[q, m] = np.prod([g - o for o in others]) / den
            slope[q, m] = (
                sum(np.prod([g - others[t] for t in range(3) if t != s]) for s in range(3)) / den
            )
    c = 2.0 * points - 1.0
    legendre = np.stack(
        [
            np.full(4, plus_values[0]),
            plus_values[1] * c,
            plus_values[2] * 0.5 * (3.0 * c**2 - 1.0),
        ],
        axis=1,
    )
    return value, slope, legendre, weights


def row_tables(Y, Z):
    value, slope, legendre, weights = tables_1d()
    rows, nodes = 4 * Y, 3 * Y + 1
    tv = np.zeros((rows, rows))
    td = np.zeros((rows, rows))
    for e in range(Y):
        tv[4 * e : 4 * e + 4, 3 * e : 3 * e + 4] = value
        td[4 * e : 4 * e + 4, 3 * e : 3 * e + 4] = slope
    blocks = [tv[:, j] for j in range(nodes)] + [td[:, j] for j in range(nodes)]
    blocks += [tv[s, :] for s in range(rows)] + [td[s, :] for s in range(rows)]
    for b in range(3):
        for e in range(Y):
            col = np.zeros(rows)
            col[4 * e : 4 * e + 4] = legendre[:, b]
            blocks.append(col)
    blocks.append(np.tile(weights, Y))
    stacked = np.stack(blocks).astype(np.float32)
    return np.ascontiguousarray(np.broadcast_to(stacked[:, :, None], stacked.shape + (Z,)))


def kernel(sizes, X, Y, Z, disp_in, modes_in, vel_in, tab, adv, grad, checks,
           disp, GU, ZP, ZR, ZA, UM, WM, VM, CM, FM, US, WS, VS, CS, FT,
           perm, slab, U, ROWS, N, GN, A, G, J, B, SIZ, DT,
           NXR, NYS, NYR, NXYR, NZS, NZR, FXR, FYS, FYR, FXYR, FZS, FZR, FES, FER,
           ls, g1s, g1r, g2s, g2r, zs, zr, y2s, y2r, rs, rr, ns, nr, fs, fr):
    value, slope, legendre, weights = tables_1d()
    NX, NY = 3 * X, 3 * Y
    ROWS_Y = 4 * Y
    EL = X * Y
    f32 = jnp.float32
    index = [lax.axis_index(a) for a in AXES]
    lane = lax.broadcasted_iota(jnp.int32, (ROWS_Y, Z), 1)
    row = lax.broadcasted_iota(jnp.int32, (ROWS_Y, Z), 0)
    oTV, oTD, oGV, oGD, oL, oW = 0, NY + 1, 2 * NY + 2, 2 * NY + 2 + ROWS_Y, 2 * NY + 2 + 2 * ROWS_Y, 2 * NY + 2 + 2 * ROWS_Y + 3 * Y

    def at(axis, by):
        n = sizes[axis]
        return {AXES[axis]: lax.rem(index[axis] + (by + n), n)}

    loads = [
        pltpu.make_async_copy(modes_in, GU.at[0, 0, 0:27], ls.at[0]),
        pltpu.make_async_copy(vel_in, GU.at[0, 0, 27:30], ls.at[1]),
        pltpu.make_async_copy(disp_in, disp, ls.at[2]),
    ]
    for cp in loads:
        cp.start()
    barrier = pltpu.get_barrier_semaphore()
    total = 0
    for a in range(sizes[0]):
        for b in range(sizes[1]):
            for c in range(sizes[2]):
                move = (a, b, c)
                if not any(move):
                    continue
                target = {}
                for axis in range(3):
                    if move[axis]:
                        target.update(at(axis, move[axis]))
                pl.semaphore_signal(barrier, inc=1, device_id=target, device_id_type=MESH)
                total += 1

    def copy(src, dst, ss, sr, axis, by):
        return pltpu.make_async_remote_copy(
            src_ref=src, dst_ref=dst, send_sem=ss, recv_sem=sr,
            device_id=at(axis, by), device_id_type=MESH,
        )

    GX, GY = sizes[0], sizes[1]
    XG, YG, NS, EDGE = GX * X, GY * Y, GX * X // 2, 2 * SUBSTEPS
    HALF, FIELDS, SLOTS = Z // 2, 30, Z // EDGE

    def moved(move):
        target = {}
        for axis in range(3):
            if move[axis] % sizes[axis]:
                target.update(at(axis, move[axis] % sizes[axis] ))
        return target

    def remote(src, dst, ss, sr, move):
        return pltpu.make_async_remote_copy(
            src_ref=src, dst_ref=dst, send_sem=ss, recv_sem=sr,
            device_id=moved(move), device_id_type=MESH,
        )

    def plane_copy(ry):
        return remote(GU.at[0, 0], GU.at[0, ry], g1s.at[ry], g1r.at[ry], (0, -ry, 0))

    def core_copies(ry):
        return [
            remote(GU.at[0, ry], GU.at[rx, ry], g2s.at[rx, ry], g2r.at[rx, ry], (-rx, 0, 0))
            for rx in range(1, GX)
        ]

    def edge_copies():
        return [
            remote(ZP.at[side], ZR.at[0, ry, side], zs.at[side, ry], zr.at[side, ry], (0, -ry, 2 * side - 1))
            for side in range(2) for ry in range(GY)
        ]

    def edge_core_copies():
        return [
            remote(ZR.at[0], ZR.at[rx], y2s.at[rx], y2r.at[rx], (-rx, 0, 0)) for rx in range(1, GX)
        ]

    slot2 = lax.broadcasted_iota(jnp.int32, (Y, Z), 1) // EDGE
    packs = -(-FIELDS * X // SLOTS)

    def pack_edges():
        acc = [[jnp.zeros((Y, Z), f32) for _ in range(packs)] for _ in range(2)]
        for m in range(FIELDS):
            for ix in range(X):
                t = m * X + ix
                v, p = t // SLOTS, EDGE * (t % SLOTS)
                x = GU[0, 0, m, ix]
                low = pltpu.roll(x, p, 1) if p else x
                high = pltpu.roll(x, (p + EDGE) % Z, 1) if (p + EDGE) % Z else x
                acc[0][v] = jnp.where(slot2 == t % SLOTS, low, acc[0][v])
                acc[1][v] = jnp.where(slot2 == t % SLOTS, high, acc[1][v])
        for side in range(2):
            for v in range(packs):
                ZP[side, v] = acc[side][v]

    for cp in loads[:2]:
        cp.wait()
    speed = None
    for ix in range(X):
        here = jnp.abs(GU[0, 0, 27, ix]) + jnp.abs(GU[0, 0, 28, ix]) + jnp.abs(GU[0, 0, 29, ix])
        speed = here if speed is None else jnp.maximum(speed, here)
    ROWS[0, 0] = jnp.broadcast_to(jnp.max(speed, axis=0, keepdims=True), (2, Z))
    pack_edges()

    def unweave():
        a_i = lax.broadcasted_iota(jnp.int32, (3 * Z, 3 * Z), 0)
        b_i = lax.broadcasted_iota(jnp.int32, (3 * Z, 3 * Z), 1)
        b_k = (b_i >= Z).astype(jnp.int32) + (b_i >= 2 * Z).astype(jnp.int32)
        perm[...] = (a_i == 3 * (b_i - b_k * Z) + b_k).astype(f32)
        slab[...] = jnp.zeros_like(slab)
        for c in range(3):
            for i in range(NX):
                slab[c * NX + i, 0:NY, :] = disp[c, i]
        spread = jnp.dot(
            slab[...].reshape(3 * NX * ROWS_Y, 3 * Z), perm[...],
            precision=lax.Precision.HIGHEST, preferred_element_type=f32,
        ).reshape(3, NX, ROWS_Y, 3 * Z)
        for c in range(3):
            for k in range(3):
                N[c, 0:NX, k] = spread[c, :, :, k * Z : (k + 1) * Z]

    loads[2].wait()
    unweave()
    pl.semaphore_wait(barrier, total)
    for cp in core_copies(0):
        cp.start()
    for ry in range(1, GY):
        plane_copy(ry).start()
    for cp in edge_copies():
        cp.start()

    devices = sizes[0] * sizes[1] * sizes[2]
    stages = [(0, 1, 2)] if devices <= 64 else [(0,), (1, 2)]

    def row_stage(r, stage):
        block = 1
        for axes in stages[:stage]:
            for axis in axes:
                block *= sizes[axis]
        moves = [()]
        for axis in range(3):
            moves = [m + (b,) for m in moves for b in range(sizes[axis] if axis in stages[stage] else 1)]
        src = ROWS.at[r, 0:block]
        copies = [
            remote(src, ROWS.at[r, n * block : (n + 1) * block], rs.at[r, stage], rr.at[r, stage], m)
            for n, m in enumerate(moves) if n
        ]
        rest = ROWS.at[r, block : len(moves) * block]
        return copies, remote(rest, rest, rs.at[r, stage], rr.at[r, stage], moves[1])

    def rows_start(r, stage):
        for cp in row_stage(r, stage)[0]:
            cp.start()

    def rows_finish(r):
        for stage in range(len(stages)):
            row_stage(r, stage)[1].wait_recv()
            if stage + 1 < len(stages):
                rows_start(r, stage + 1)

    def rows_sent(r):
        for stage in range(len(stages)):
            row_stage(r, stage)[1].wait_send()

    in_lane = lambda n: functools.reduce(jnp.logical_or, [lane == c * (NX + 1) + n for c in range(3)])

    def rim_copies():
        out = [
            remote(N.at[:, 0, 0:3], NXR, ns.at[0], nr.at[0], (-1, 0, 0)),
            remote(NYS, NYR, ns.at[1], nr.at[1], (0, -1, 0)),
            remote(NYS.at[:, 0], NXYR, ns.at[2], nr.at[2], (-1, -1, 0)),
        ]
        for n, move in enumerate(((0, 0, -1), (-1, 0, -1), (0, -1, -1), (-1, -1, -1))):
            out.append(remote(NZS, NZR.at[n], ns.at[3 + n], nr.at[3 + n], move))
        return out

    def rim_pack():
        packed = jnp.zeros((ROWS_Y, Z), f32)
        for c in range(3):
            for i in range(NX):
                for k in range(3):
                    NYS[c, i, k : k + 1, :] = N[c, i, k, 0:1, :]
                packed = jnp.where(lane == c * (NX + 1) + i, N[c, i, 0][:, 0:1], packed)
        NZS[...] = packed

    def rim_unpack():
        for c in range(3):
            for k in range(3):
                N[c, NX, k] = NXR[c, k]
                N[c, NX, k, NY : NY + 1, :] = NXYR[c, k : k + 1, :]
                for i in range(NX):
                    N[c, i, k, NY : NY + 1, :] = NYR[c, i, k : k + 1, :]
        last = in_lane(NX)
        packed = jnp.where(last, pltpu.roll(NZR[1], NX, 1), NZR[0])
        below = jnp.where(last[0:1], pltpu.roll(NZR[3], NX, 1)[0:1], NZR[2][0:1])
        packed = jnp.where(row == NY, jnp.broadcast_to(below, (ROWS_Y, Z)), packed)
        for c in range(3):
            for i in range(NX + 1):
                at_ = c * (NX + 1) + i
                N[c, i, 3] = jnp.where(lane == Z - 1, packed[:, at_ : at_ + 1], pltpu.roll(N[c, i, 0], Z - 1, 1))

    scale = [plus_values[m // 9] * plus_values[m // 3 % 3] * plus_values[m % 3] for m in range(27)]

    def assemble():
        def plane(x, carry):
            rx, ix = x // X, x % X
            for ry in range(GY):
                for m in range(FIELDS):
                    v = GU[rx, ry, m, ix]
                    if m < 27:
                        UM[m, x, ry * Y : ry * Y + Y, :] = scale[m] * v
                    else:
                        VM[m - 27, x, ry * Y : ry * Y + Y, :] = v
            return carry

        lax.fori_loop(0, XG, plane, 0)

    lanes = lax.broadcasted_iota(jnp.int32, (YG, Z), 1)
    W2, W3 = 2 * EDGE, 3 * EDGE

    def within(lo, hi):
        return (lanes >= lo) & (lanes < hi)

    def strip_own():
        def one(q, carry):
            for m in range(FIELDS):
                out = jnp.zeros((YG, Z), f32)
                for h in range(2):
                    t = UM[m, q + h * NS] if m < 27 else VM[m - 27, q + h * NS]
                    o = h * HALF
                    out = jnp.where(within(o, o + W2), pltpu.roll(t, o + W2, 1), out)
                    out = jnp.where(within(o + 2 * W2, o + 3 * W2), pltpu.roll(t, o + 2 * W2, 1), out)
                if m < 27:
                    US[m, q] = out
                else:
                    VS[m - 27, q] = out
            return carry

        lax.fori_loop(0, NS, one, 0)

    def strip_halo():
        for rx in range(GX):
            for ry in range(GY):
                ZA[rx, :, :, ry * Y : ry * Y + Y, :] = ZR[rx, ry]
        for q in range(NS):
            for m in range(FIELDS):
                out = US[m, q] if m < 27 else VS[m - 27, q]
                for h in range(2):
                    x = q + h * NS
                    rx, ix = x // X, x % X
                    t = m * X + ix
                    v, p = t // SLOTS, EDGE * (t % SLOTS)
                    for side in range(2):
                        o = h * HALF + W2 + side * EDGE
                        piece = ZA[rx, side, v]
                        by = (o - p) % Z
                        piece = pltpu.roll(piece, by, 1) if by else piece
                        if m < 27:
                            piece = scale[m] * piece
                        out = jnp.where(within(o, o + EDGE), piece, out)
                if m < 27:
                    US[m, q] = out
                else:
                    VS[m - 27, q] = out

    def ynext(t):
        return pltpu.roll(t, YG - 1, 0)

    def yprev(t):
        return pltpu.roll(t, 1, 0)

    def znext(t):
        return pltpu.roll(t, Z - 1, 1)

    def zprev(t):
        return pltpu.roll(t, 1, 1)

    def coefficients(V, C, nx, wrap):
        dt = DT[...]
        for q in range(nx):
            nxt = V[0, q + 1] if q < nx - 1 else wrap(V[0, 0])
            for d in range(3):
                v = V[d, q]
                ahead = nxt if d == 0 else ynext(v) if d == 1 else znext(v)
                face = (0.5 * dt) * (v + ahead)
                C[q, 3 * d] = jnp.maximum(face, 0.0)
                C[q, 3 * d + 1] = jnp.minimum(face, 0.0)
                C[q, 3 * d + 2] = (2.0 * dt) * v

    def line(u, hp, hm, v2, ahead, behind):
        e = u[0] + u[2]
        up = hp * (e + u[1]) + hm * ahead(e - u[1])
        low = behind(up)
        diff = low - up
        return diff, 3.0 * (v2 * u[0] - (low + up)), 5.0 * (v2 * u[1] + diff)

    def rate(src, C, F, nx, wrap, write):
        for n in range(9):
            tp, tm = [], []
            for q in range(nx):
                u0, u1, u2 = src[n, q], src[9 + n, q], src[18 + n, q]
                e = u0 + u2
                tp.append(e + u1)
                tm.append(e - u1)
            for q in range(nx):
                nxt = tm[q + 1] if q < nx - 1 else wrap(tm[0])
                f = C[q, 0] * tp[q] + C[q, 1] * nxt
                F[q + 1, n] = f
                if q == nx - 1:
                    F[0, n] = wrap(f)

        def block(q, carry):
            vx = C[q, 2]
            for a in range(3):
                u = [src[9 * a + n, q] for n in range(9)]
                acc = []
                for n in range(9):
                    up, low = F[q + 1, n], F[q, n]
                    if a == 0:
                        acc.append(low - up)
                    elif a == 1:
                        acc.append(3.0 * (vx * src[n, q] - (low + up)))
                    else:
                        acc.append(5.0 * (vx * src[9 + n, q] + (low - up)))
                for d, st, ot, ahead, behind in ((1, 3, 1, ynext, yprev), (2, 1, 3, znext, zprev)):
                    hp, hm, v2 = C[q, 3 * d], C[q, 3 * d + 1], C[q, 3 * d + 2]
                    for o in range(3):
                        at_ = [ot * o + st * t for t in range(3)]
                        out = line([u[t] for t in at_], hp, hm, v2, ahead, behind)
                        for t in range(3):
                            acc[at_[t]] = acc[at_[t]] + out[t]
                for n in range(9):
                    write(9 * a + n, q, acc[n])
            return carry

        if nx <= 4:
            for q in range(nx):
                block(q, 0)
        else:
            lax.fori_loop(0, nx, block, 0)

    def advance(Ur, Wr, C, F, nx, wrap):
        def put(m, q, value):
            Wr[m, q] = value

        def step(m, q, value):
            Ur[m, q] = (Ur[m, q] + Wr[m, q]) + 0.5 * value

        def substep(t, carry):
            rate(Ur, C, F, nx, wrap, put)
            rate(Wr, C, F, nx, wrap, step)
            return carry

        lax.fori_loop(0, SUBSTEPS, substep, 0)

    def same(t):
        return t

    def half_turn(t):
        return pltpu.roll(t, HALF, 1)

    def finish_field():
        U[...] = jnp.zeros_like(U)
        for m in range(27):
            for ix in range(X):
                t = UM[m, ix]
                h, q = ix // NS, ix % NS
                s = US[m, q]
                o = h * HALF
                left = pltpu.roll(s, (Z - o - 2 * W2) % Z, 1)
                right = pltpu.roll(s, (Z - W2 - o) % Z, 1)
                t = jnp.where(lanes < EDGE, left, jnp.where(lanes >= Z - EDGE, right, t))
                U[m, ix * Y : ix * Y + Y, :] = (1.0 / scale[m]) * t[0:Y]

    def yz_of(src):
        def yz(i, carry):
            for c in range(3):
                yv, yd = [], []
                for k in range(4):
                    sv = sd = None
                    for j in range(NY + 1):
                        x = src[c, i, k, j : j + 1, :]
                        tv, td = tab[oTV + j] * x, tab[oTD + j] * x
                        sv = tv if sv is None else sv + tv
                        sd = td if sd is None else sd + td
                    yv.append(sv)
                    yd.append(sd)
                for r in range(4):
                    A[0, c, i, r] = sum(float(value[r, k]) * yv[k] for k in range(4))
                    A[1, c, i, r] = sum(float(value[r, k]) * yd[k] for k in range(4))
                    A[2, c, i, r] = sum(float(slope[r, k]) * yv[k] for k in range(4))
            return carry

        lax.fori_loop(0, NX + 1, yz, 0)

    def slope_at(ix, p, r, c, d):
        tb = slope if d == 0 else value
        return sum(float(tb[p, m]) * A[d, c, 3 * ix + m, r] for m in range(4))

    def jacobians(t):
        ix, r = t // 4, t % 4
        for p in range(4):
            for c in range(3):
                for d in range(3):
                    jac = slope_at(ix, p, r, c, d)
                    J[d, c, ix, p, r] = jac + 1.0 if c == d else jac

    rows_start(0, 0)
    rim_pack()
    for cp in rim_copies():
        cp.start()
    for ry in range(1, GY):
        plane_copy(ry).wait_recv()
        for cp in core_copies(ry):
            cp.start()
    for cp in edge_copies():
        cp.wait_recv()
    for cp in edge_core_copies():
        cp.start()
    for cp in rim_copies():
        cp.wait()
    rim_unpack()
    yz_of(N)

    def all_jacobians(t, carry):
        jacobians(t)
        return carry

    lax.fori_loop(0, 4 * X, all_jacobians, 0)
    rows_finish(0)
    fastest = functools.reduce(jnp.maximum, [ROWS[0, n] for n in range(devices)])
    fastest = jnp.max(fastest, axis=(0, 1), keepdims=True)
    DT[...] = jnp.broadcast_to(courant / jnp.maximum(fastest, 0.25), (YG, Z))
    for ry in range(GY):
        for cp in core_copies(ry):
            cp.wait_recv()
    assemble()
    strip_own()
    coefficients(VM, CM, XG, same)
    advance(UM, WM, CM, FM, XG, same)
    for cp in edge_core_copies():
        cp.wait_recv()
    strip_halo()
    coefficients(VS, CS, NS, half_turn)
    advance(US, WS, CS, FT, NS, half_turn)
    finish_field()
    def size_of(ix, carry):
        mid = {}
        for a in range(3):
            for r in range(4):
                mid[a, r] = None
            for c in range(3):
                t = None
                for b in range(3):
                    for e in range(Y):
                        term = tab[oL + b * Y + e] * U[a * 9 + b * 3 + c, pl.ds(ix * Y + e, 1), :]
                        t = term if t is None else t + term
                for r in range(4):
                    term = float(legendre[r, c]) * t
                    mid[a, r] = term if mid[a, r] is None else mid[a, r] + term
        for p in range(4):
            for r in range(4):
                s = sum(float(legendre[p, a]) * mid[a, r] for a in range(3))
                SIZ[ix, p, r] = jnp.exp(theta_size * s)
        return carry

    lax.fori_loop(0, X, size_of, 0)

    wrow = tab[oW]
    pairs = [(d, e) for d in range(3) for e in range(d, 3)]

    def dot3(p, q, d, e):
        return p[0][d] * q[0][e] + p[1][d] * q[1][e] + p[2][d] * q[2][e]

    def gauss_weight(r):
        return jnp.where((r == 0) | (r == 3), float(weights[0]), float(weights[1]))

    def gauss(t, esum):
        ix, r = t // 4, t % 4
        for p in range(4):
            size = SIZ[ix, p, r]
            inv = 1.0 / size
            M = [[J[d, c, ix, p, r] * inv for d in range(3)] for c in range(3)]
            D = [[None] * 3 for _ in range(3)]
            metric = None
            for d, e in pairs:
                dev = dot3(M, M, d, e)
                if d == e:
                    dev = dev - 1.0
                D[d][e] = D[e][d] = dev
                sq = dev * dev if d == e else 2.0 * (dev * dev)
                metric = sq if metric is None else metric + sq
            w = wrow * (gauss_weight(r) * float(weights[p]))
            size2 = size * size
            esum = esum + w * (size2 * size) * metric
            scale = (4.0 * w) * size2
            for c in range(3):
                for d in range(3):
                    g = M[c][0] * D[0][d] + M[c][1] * D[1][d] + M[c][2] * D[2][d]
                    G[d, c, ix, p, r] = scale * g
        return esum

    zero = jnp.zeros((ROWS_Y, Z), f32)
    esum = lax.fori_loop(0, 4 * X, gauss, zero)

    def back_c(c, carry):
        for i in range(NX + 1):
            bv = [None] * 4
            bd = [None] * 4
            for r in range(4):
                ga = []
                for d in range(3):
                    tb = slope if d == 0 else value
                    acc = None
                    for ix in range(X):
                        m = i - 3 * ix
                        if 0 <= m <= 3:
                            for p in range(4):
                                term = float(tb[p, m]) * G[d, c, ix, p, r]
                                acc = term if acc is None else acc + term
                    ga.append(acc)
                for k in range(4):
                    tv = float(value[r, k]) * ga[0] + float(slope[r, k]) * ga[2]
                    td = float(value[r, k]) * ga[1]
                    bv[k] = tv if bv[k] is None else bv[k] + tv
                    bd[k] = td if bd[k] is None else bd[k] + td
            for k in range(4):
                B[0, i, k] = bv[k]
                B[1, i, k] = bd[k]
        for i in range(NX + 1):
            for k in range(4):
                acc = None
                for s in range(ROWS_Y):
                    term = tab[oGV + s] * B[0, i, k, s : s + 1, :] + tab[oGD + s] * B[1, i, k, s : s + 1, :]
                    acc = term if acc is None else acc + term
                GN[c, i, k] = acc
        return carry

    lax.fori_loop(0, 3, back_c, 0)

    def row_of(column_of):
        out = zero
        for c in range(3):
            out = jnp.where(lane == c * ROWS_Y + row, column_of(c), out)
        return jnp.sum(out, axis=0, keepdims=True)

    far, near = zero, zero
    for c in range(3):
        for i in range(NX + 1):
            here = lane == c * (NX + 1) + i
            far = jnp.where(here, GN[c, i, 3][:, Z - 1 : Z], far)
            near = jnp.where(here, GN[c, i, 0][:, 0:1], near)
    FZS[0] = far
    FZS[1] = near
    for zs_, (k, at_) in enumerate(((3, Z - 1), (0, 0))):
        for xs_, i in enumerate((NX, 0)):
            FES[zs_, xs_] = row_of(lambda c: GN[c, i, k][:, at_ : at_ + 1])
        for ys_, j in enumerate((NY, 0)):
            FES[zs_, 2 + ys_] = FZS[zs_][j : j + 1]
    for c in range(3):
        for i in range(NX + 1):
            GN[c, i, 0] = GN[c, i, 0] + jnp.where(lane == 0, 0.0, pltpu.roll(GN[c, i, 3], 1, 1))
            for k in range(4):
                FYS[0, c, i, k : k + 1, :] = GN[c, i, k, NY : NY + 1, :]
                FYS[1, c, i, k : k + 1, :] = GN[c, i, k, 0:1, :]
    ways = (1, -1)

    def fold_copies():
        out = []

        def add(src, dst, move):
            n = len(out)
            out.append(remote(src, dst, fs.at[n], fr.at[n], move))

        for zs_ in range(2):
            for xs_ in range(2):
                for ys_ in range(2):
                    add(FES.at[zs_, xs_], FER.at[zs_, 4 + 2 * xs_ + ys_], (ways[xs_], ways[ys_], ways[zs_]))
            for ys_ in range(2):
                add(FES.at[zs_, 2 + ys_], FER.at[zs_, 2 + ys_], (0, ways[ys_], ways[zs_]))
            for xs_ in range(2):
                add(FES.at[zs_, xs_], FER.at[zs_, xs_], (ways[xs_], 0, ways[zs_]))
            add(FZS.at[zs_], FZR.at[zs_], (0, 0, ways[zs_]))
        for ys_ in range(2):
            for xs_ in range(2):
                add(FYS.at[ys_, :, (NX, 0)[xs_]], FXYR.at[xs_, ys_], (ways[xs_], ways[ys_], 0))
            add(FYS.at[ys_], FYR.at[ys_], (0, ways[ys_], 0))
        for xs_ in range(2):
            add(GN.at[:, (NX, 0)[xs_]], FXR.at[xs_], (ways[xs_], 0, 0))
        return out

    for cp in fold_copies():
        cp.start()
    for cp in fold_copies():
        cp.wait()

    lane1, row_j = lane[0:1], lane[0:1] % ROWS_Y
    planes = []
    for zs_ in range(2):
        p = FZR[zs_]
        p = p + jnp.where(row == 0, FER[zs_, 2], 0.0) + jnp.where(row == NY, FER[zs_, 3], 0.0)
        for xs_, i in enumerate((0, NX)):
            edge = FER[zs_, xs_]
            edge = edge + jnp.where(row_j == 0, pltpu.roll(FER[zs_, 4 + 2 * xs_], Z - NY, 1), 0.0)
            edge = edge + jnp.where(row_j == NY, pltpu.roll(FER[zs_, 5 + 2 * xs_], NY, 1), 0.0)
            for c in range(3):
                col = jnp.sum(jnp.where(lane == c * ROWS_Y + row, edge, 0.0), axis=1, keepdims=True)
                p = p + jnp.where(lane == c * (NX + 1) + i, col, 0.0)
        planes.append(p)
    for c in range(3):
        for k in range(4):
            for xs_, i in enumerate((0, NX)):
                GN[c, i, k] = GN[c, i, k] + FXR[xs_, c, k]
                for ys_, j in enumerate((0, NY)):
                    GN[c, i, k, j : j + 1, :] = GN[c, i, k, j : j + 1, :] + FXYR[xs_, ys_, c, k : k + 1, :]
            for i in range(NX + 1):
                for ys_, j in enumerate((0, NY)):
                    GN[c, i, k, j : j + 1, :] = GN[c, i, k, j : j + 1, :] + FYR[ys_, c, i, k : k + 1, :]
        for i in range(NX + 1):
            n = c * (NX + 1) + i
            full = GN[c, i, 0] + jnp.where(lane == 0, planes[0][:, n : n + 1], 0.0)
            GN[c, i, 0] = full
            GN[c, i, 3] = jnp.where(lane == Z - 1, GN[c, i, 3] + planes[1][:, n : n + 1], pltpu.roll(full, Z - 1, 1))
    ssum = zero
    for c in range(3):
        for i in range(NX):
            for k in range(3):
                g = GN[c, i, k]
                ssum = ssum + g * g
    ssum = jnp.where(row < NY, ssum, 0.0)
    elements = float(EL * Z * devices)
    entries = 81.0 * elements
    mine = jnp.sum(ssum, axis=(0, 1), keepdims=True)
    bound = trial_step / jnp.sqrt(1.0 + mine / entries)
    bound = jnp.broadcast_to(bound, (ROWS_Y, Z))
    yz_of(GN)

    def trial(t, sums):
        ix, r = t // 4, t % 4
        s2, s3, s4 = sums
        for p in range(4):
            size = SIZ[ix, p, r]
            inv = 1.0 / size
            move = -(inv * bound)
            M = [[J[d, c, ix, p, r] * inv for d in range(3)] for c in range(3)]
            K = [[slope_at(ix, p, r, c, d) * move for d in range(3)] for c in range(3)]
            w = wrow * (gauss_weight(r) * float(weights[p])) * (size * size * size)
            q = [None] * 3
            for d, e in pairs:
                d0 = dot3(M, M, d, e)
                d2 = dot3(K, K, d, e)
                if d == e:
                    d0 = d0 - 1.0
                    d1 = 2.0 * dot3(M, K, d, d)
                else:
                    d1 = dot3(M, K, d, e) + dot3(K, M, d, e)
                terms = [d1 * d1 + 2.0 * (d0 * d2), 2.0 * (d1 * d2), d2 * d2]
                for n in range(3):
                    term = terms[n] if d == e else 2.0 * terms[n]
                    q[n] = term if q[n] is None else q[n] + term
            s2, s3, s4 = s2 + w * q[0], s3 + w * q[1], s4 + w * q[2]
        return s2, s3, s4

    sums = lax.fori_loop(0, 4 * X, trial, (zero,) * 3)
    block = zero
    for n, part in enumerate((esum, ssum) + tuple(sums)):
        block = jnp.where(row == n, jnp.sum(part, axis=0, keepdims=True), block)
    column = jnp.sum(block, axis=1, keepdims=True)
    ROWS[1, 0, 0:1] = jnp.sum(jnp.where(lane == row, column, 0.0), axis=0, keepdims=True)
    ROWS[1, 0, 1:2] = 1.0 / bound[0:1]
    rows_start(1, 0)
    for c in range(3):
        for k in range(3):
            slab[c * NX : (c + 1) * NX, :, k * Z : (k + 1) * Z] = GN[c, 0:NX, k]
    woven = lax.dot_general(
        slab[...].reshape(3 * NX * ROWS_Y, 3 * Z), perm[...], (((1,), (1,)), ((), ())),
        precision=lax.Precision.HIGHEST, preferred_element_type=f32,
    ).reshape(3, NX, ROWS_Y, 3 * Z)
    grad[...] = woven[:, :, 0:NY, :]
    for ix in range(X):
        adv[:, ix] = U[:, ix * Y : ix * Y + Y, :]
    rows_finish(1)
    every = [ROWS[1, n] for n in range(devices)]
    l1 = lax.broadcasted_iota(jnp.int32, (1, Z), 1)

    def lane_sum(x, n):
        return jnp.sum(jnp.where(l1 == n, x, 0.0), axis=1, keepdims=True)

    sums = sum(x[0:1] for x in every)
    etot, stot = lane_sum(sums, 0), lane_sum(sums, 1)
    step = trial_step / jnp.sqrt(1.0 + stot / entries)
    higher = jnp.zeros((1, Z), f32)
    for x in every:
        h = step * x[1:2]
        h2 = h * h
        power = jnp.where(l1 == 2, h2, jnp.where(l1 == 3, h2 * h, h2 * h2))
        higher = higher + x[0:1] * power
    higher = jnp.sum(jnp.where((l1 >= 2) & (l1 < 5), higher, 0.0), axis=1, keepdims=True)
    ttot = (etot - step * stot) + higher
    for ry in range(GY):
        if ry:
            plane_copy(ry).wait_send()
        for cp in core_copies(ry):
            cp.wait_send()
    for cp in edge_copies() + edge_core_copies():
        cp.wait_send()
    rows_sent(0)
    rows_sent(1)
    checks[...] = jnp.where(
        l1 == 0, etot / elements, jnp.where(l1 == 1, stot / entries, ttot / elements)
    )


def solution(mesh):
    sizes = tuple(mesh.shape[a] for a in AXES)

    def on_device(displacement, size_field_modes, velocity):
        modes, X, Y, Z = size_field_modes.shape
        assert Y == 2 and displacement.shape == (3, 3 * X, 3 * Y, 3 * Z)
        R, NX, NY = 4 * Y, 3 * X, 3 * Y
        tab = jnp.asarray(row_tables(Y, Z))
        devices = sizes[0] * sizes[1] * sizes[2]
        GX, GY = sizes[0], sizes[1]
        XG, YG, NS = GX * X, GY * Y, GX * X // 2
        packs = -(-30 * X // (Z // (2 * SUBSTEPS)))
        assert YG == 8 and XG % 2 == 0 and min(sizes) > 1
        vm = lambda *shape: pltpu.VMEM(shape, jnp.float32)
        dma = lambda *shape: pltpu.SemaphoreType.DMA(shape)
        spec = pl.BlockSpec(memory_space=pltpu.VMEM)
        adv, grad, checks = pl.pallas_call(
            functools.partial(kernel, sizes, X, Y, Z),
            out_shape=(
                jax.ShapeDtypeStruct(size_field_modes.shape, jnp.float32),
                jax.ShapeDtypeStruct(displacement.shape, jnp.float32),
                jax.ShapeDtypeStruct((1, Z), jnp.float32),
            ),
            in_specs=[pl.BlockSpec(memory_space=pl.ANY)] * 3 + [spec],
            out_specs=(spec,) * 3,
            scratch_shapes=[
                vm(3, NX, NY, 3 * Z), vm(GX, GY, 30, X, Y, Z), vm(2, packs, Y, Z), vm(GX, GY, 2, packs, Y, Z), vm(GX, 2, packs, YG, Z),
                vm(27, XG, YG, Z), vm(27, XG, YG, Z), vm(3, XG, YG, Z), vm(XG, 9, YG, Z), vm(XG + 1, 9, YG, Z),
                vm(27, NS, YG, Z), vm(27, NS, YG, Z), vm(3, NS, YG, Z), vm(NS, 9, YG, Z), vm(NS + 1, 9, YG, Z),
                vm(3 * Z, 3 * Z), vm(3 * NX, R, 3 * Z), vm(27, R, Z),
                vm(2, devices, 2, Z),
                vm(3, NX + 1, 4, R, Z), vm(3, NX + 1, 4, R, Z),
                vm(3, 3, NX + 1, 4, R, Z), vm(3, 3, X, 4, 4, R, Z), vm(3, 3, X, 4, 4, R, Z), vm(2, NX + 1, 4, R, Z), vm(X, 4, 4, R, Z), vm(R, Z),
                vm(3, 3, R, Z), vm(3, NX, 3, Z), vm(3, NX, 3, Z), vm(3, 3, Z), vm(R, Z), vm(4, R, Z),
                vm(2, 3, 4, R, Z), vm(2, 3, NX + 1, 4, Z), vm(2, 3, NX + 1, 4, Z), vm(2, 2, 3, 4, Z), vm(2, R, Z), vm(2, R, Z), vm(2, 4, 1, Z), vm(2, 8, 1, Z),
                dma(3), dma(GY), dma(GY), dma(GX, GY), dma(GX, GY), dma(2, GY), dma(2, GY), dma(GX), dma(GX), dma(2, 2), dma(2, 2), dma(7), dma(7), dma(26), dma(26),
            ],
            compiler_params=pltpu.CompilerParams(collective_id=0, has_side_effects=True),
        )(displacement, size_field_modes, velocity, tab)
        return adv, grad, checks[0, 0:3]

    return jax.shard_map(
        on_device,
        mesh=mesh,
        in_specs=(P(None, "gx", "gy", "gz"),) * 3,
        out_specs=(P(None, "gx", "gy", "gz"), P(None, "gx", "gy", "gz"), P()),
        check_vma=False,
    )
```

```python
import functools

import jax
import jax.numpy as jnp
import numpy as np
from jax import lax
from jax.experimental import pallas as pl
from jax.experimental.pallas import tpu as pltpu
from jax.sharding import PartitionSpec as P

SUBSTEPS = 4
MESH = pl.DeviceIdType.MESH
AXES = ("gx", "gy", "gz")

plus_values = (0.7071067811865476, 1.224744871391589, 1.5811388300841898)
g10 = 1.7320508075688772
g21 = 3.872983346207417
courant = 0.1
theta_size = 0.3
trial_step = 0.05


def tables_1d():
    points = np.array(
        [-0.8611363115940526, -0.3399810435848563, 0.3399810435848563, 0.8611363115940526]
    )
    weights = np.array(
        [0.3478548451374538, 0.6521451548625461, 0.6521451548625461, 0.3478548451374538]
    )
    points = 0.5 * (points + 1.0)
    weights = 0.5 * weights
    nodes = np.array([0.0, 1.0 / 3.0, 2.0 / 3.0, 1.0])
    value = np.zeros((4, 4))
    slope = np.zeros((4, 4))
    for m in range(4):
        others = [nodes[o] for o in range(4) if o != m]
        den = np.prod([nodes[m] - o for o in others])
        for q in range(4):
            g = points[q]
            value[q, m] = np.prod([g - o for o in others]) / den
            slope[q, m] = (
                sum(np.prod([g - others[t] for t in range(3) if t != s]) for s in range(3)) / den
            )
    c = 2.0 * points - 1.0
    legendre = np.stack(
        [
            np.full(4, plus_values[0]),
            plus_values[1] * c,
            plus_values[2] * 0.5 * (3.0 * c**2 - 1.0),
        ],
        axis=1,
    )
    return value, slope, legendre, weights


def row_tables(Y, Z):
    value, slope, legendre, weights = tables_1d()
    rows, nodes = 4 * Y, 3 * Y + 1
    tv = np.zeros((rows, rows))
    td = np.zeros((rows, rows))
    for e in range(Y):
        tv[4 * e : 4 * e + 4, 3 * e : 3 * e + 4] = value
        td[4 * e : 4 * e + 4, 3 * e : 3 * e + 4] = slope
    blocks = [tv[:, j] for j in range(nodes)] + [td[:, j] for j in range(nodes)]
    blocks += [tv[s, :] for s in range(rows)] + [td[s, :] for s in range(rows)]
    for b in range(3):
        for e in range(Y):
            col = np.zeros(rows)
            col[4 * e : 4 * e + 4] = legendre[:, b]
            blocks.append(col)
    blocks.append(np.tile(weights, Y))
    stacked = np.stack(blocks).astype(np.float32)
    return np.ascontiguousarray(np.broadcast_to(stacked[:, :, None], stacked.shape + (Z,)))


def kernel(sizes, X, Y, Z, disp_in, modes_in, vel_in, tab, adv, grad, checks,
           disp, GU, ZP, ZR, ZA, UM, WM, VM, CM, FM, US, WS, VS, CS, FT,
           perm, slab, U, ROWS, N, GN, A, G, J, B, SIZ, DT,
           NXR, NYS, NYR, NXYR, NZS, NZR, FXR, FYS, FYR, FXYR, FZS, FZR, FES, FER,
           ls, g1s, g1r, g2s, g2r, zs, zr, y2s, y2r, rs, rr, ns, nr, fs, fr):
    value, slope, legendre, weights = tables_1d()
    NX, NY = 3 * X, 3 * Y
    ROWS_Y = 4 * Y
    EL = X * Y
    f32 = jnp.float32
    index = [lax.axis_index(a) for a in AXES]
    lane = lax.broadcasted_iota(jnp.int32, (ROWS_Y, Z), 1)
    row = lax.broadcasted_iota(jnp.int32, (ROWS_Y, Z), 0)
    oTV, oTD, oGV, oGD, oL, oW = 0, NY + 1, 2 * NY + 2, 2 * NY + 2 + ROWS_Y, 2 * NY + 2 + 2 * ROWS_Y, 2 * NY + 2 + 2 * ROWS_Y + 3 * Y

    def at(axis, by):
        n = sizes[axis]
        return {AXES[axis]: lax.rem(index[axis] + (by + n), n)}

    loads = [
        pltpu.make_async_copy(modes_in, GU.at[0, 0, 0:27], ls.at[0]),
        pltpu.make_async_copy(vel_in, GU.at[0, 0, 27:30], ls.at[1]),
        pltpu.make_async_copy(disp_in, disp, ls.at[2]),
    ]
    for cp in loads:
        cp.start()
    barrier = pltpu.get_barrier_semaphore()
    total = 0
    for a in range(sizes[0]):
        for b in range(sizes[1]):
            for c in range(sizes[2]):
                move = (a, b, c)
                if not any(move):
                    continue
                target = {}
                for axis in range(3):
                    if move[axis]:
                        target.update(at(axis, move[axis]))
                pl.semaphore_signal(barrier, inc=1, device_id=target, device_id_type=MESH)
                total += 1

    def copy(src, dst, ss, sr, axis, by):
        return pltpu.make_async_remote_copy(
            src_ref=src, dst_ref=dst, send_sem=ss, recv_sem=sr,
            device_id=at(axis, by), device_id_type=MESH,
        )

    GX, GY = sizes[0], sizes[1]
    XG, YG, NS, EDGE = GX * X, GY * Y, GX * X // 2, 2 * SUBSTEPS
    HALF, FIELDS, SLOTS = Z // 2, 30, Z // EDGE

    def moved(move):
        target = {}
        for axis in range(3):
            if move[axis] % sizes[axis]:
                target.update(at(axis, move[axis] % sizes[axis] ))
        return target

    def remote(src, dst, ss, sr, move):
        return pltpu.make_async_remote_copy(
            src_ref=src, dst_ref=dst, send_sem=ss, recv_sem=sr,
            device_id=moved(move), device_id_type=MESH,
        )

    def plane_copy(ry):
        return remote(GU.at[0, 0], GU.at[0, ry], g1s.at[ry], g1r.at[ry], (0, -ry, 0))

    def core_copies(ry):
        return [
            remote(GU.at[0, ry], GU.at[rx, ry], g2s.at[rx, ry], g2r.at[rx, ry], (-rx, 0, 0))
            for rx in range(1, GX)
        ]

    def edge_copies():
        return [
            remote(ZP.at[side], ZR.at[0, ry, side], zs.at[side, ry], zr.at[side, ry], (0, -ry, 2 * side - 1))
            for side in range(2) for ry in range(GY)
        ]

    def edge_core_copies():
        return [
            remote(ZR.at[0], ZR.at[rx], y2s.at[rx], y2r.at[rx], (-rx, 0, 0)) for rx in range(1, GX)
        ]

    slot2 = lax.broadcasted_iota(jnp.int32, (Y, Z), 1) // EDGE
    packs = -(-FIELDS * X // SLOTS)

    def pack_edges():
        acc = [[jnp.zeros((Y, Z), f32) for _ in range(packs)] for _ in range(2)]
        for m in range(FIELDS):
            for ix in range(X):
                t = m * X + ix
                v, p = t // SLOTS, EDGE * (t % SLOTS)
                x = GU[0, 0, m, ix]
                low = pltpu.roll(x, p, 1) if p else x
                high = pltpu.roll(x, (p + EDGE) % Z, 1) if (p + EDGE) % Z else x
                acc[0][v] = jnp.where(slot2 == t % SLOTS, low, acc[0][v])
                acc[1][v] = jnp.where(slot2 == t % SLOTS, high, acc[1][v])
        for side in range(2):
            for v in range(packs):
                ZP[side, v] = acc[side][v]

    for cp in loads[:2]:
        cp.wait()
    speed = None
    for ix in range(X):
        here = jnp.abs(GU[0, 0, 27, ix]) + jnp.abs(GU[0, 0, 28, ix]) + jnp.abs(GU[0, 0, 29, ix])
        speed = here if speed is None else jnp.maximum(speed, here)
    ROWS[0, 0] = jnp.broadcast_to(jnp.max(speed, axis=0, keepdims=True), (2, Z))
    pack_edges()

    def unweave():
        a_i = lax.broadcasted_iota(jnp.int32, (3 * Z, 3 * Z), 0)
        b_i = lax.broadcasted_iota(jnp.int32, (3 * Z, 3 * Z), 1)
        b_k = (b_i >= Z).astype(jnp.int32) + (b_i >= 2 * Z).astype(jnp.int32)
        perm[...] = (a_i == 3 * (b_i - b_k * Z) + b_k).astype(f32)
        slab[...] = jnp.zeros_like(slab)
        for c in range(3):
            for i in range(NX):
                slab[c * NX + i, 0:NY, :] = disp[c, i]
        spread = jnp.dot(
            slab[...].reshape(3 * NX * ROWS_Y, 3 * Z), perm[...],
            precision=lax.Precision.HIGHEST, preferred_element_type=f32,
        ).reshape(3, NX, ROWS_Y, 3 * Z)
        for c in range(3):
            for k in range(3):
                N[c, 0:NX, k] = spread[c, :, :, k * Z : (k + 1) * Z]

    loads[2].wait()
    unweave()
    pl.semaphore_wait(barrier, total)
    for cp in core_copies(0):
        cp.start()
    for ry in range(1, GY):
        plane_copy(ry).start()
    for cp in edge_copies():
        cp.start()

    devices = sizes[0] * sizes[1] * sizes[2]
    stages = [(0, 1, 2)] if devices <= 64 else [(0,), (1, 2)]

    def row_stage(r, stage):
        block = 1
        for axes in stages[:stage]:
            for axis in axes:
                block *= sizes[axis]
        moves = [()]
        for axis in range(3):
            moves = [m + (b,) for m in moves for b in range(sizes[axis] if axis in stages[stage] else 1)]
        src = ROWS.at[r, 0:block]
        copies = [
            remote(src, ROWS.at[r, n * block : (n + 1) * block], rs.at[r, stage], rr.at[r, stage], m)
            for n, m in enumerate(moves) if n
        ]
        rest = ROWS.at[r, block : len(moves) * block]
        return copies, remote(rest, rest, rs.at[r, stage], rr.at[r, stage], moves[1])

    def rows_start(r, stage):
        for cp in row_stage(r, stage)[0]:
            cp.start()

    def rows_finish(r):
        for stage in range(len(stages)):
            row_stage(r, stage)[1].wait_recv()
            if stage + 1 < len(stages):
                rows_start(r, stage + 1)

    def rows_sent(r):
        for stage in range(len(stages)):
            row_stage(r, stage)[1].wait_send()

    in_lane = lambda n: functools.reduce(jnp.logical_or, [lane == c * (NX + 1) + n for c in range(3)])

    def rim_copies():
        out = [
            remote(N.at[:, 0, 0:3], NXR, ns.at[0], nr.at[0], (-1, 0, 0)),
            remote(NYS, NYR, ns.at[1], nr.at[1], (0, -1, 0)),
            remote(NYS.at[:, 0], NXYR, ns.at[2], nr.at[2], (-1, -1, 0)),
        ]
        for n, move in enumerate(((0, 0, -1), (-1, 0, -1), (0, -1, -1), (-1, -1, -1))):
            out.append(remote(NZS, NZR.at[n], ns.at[3 + n], nr.at[3 + n], move))
        return out

    def rim_pack():
        packed = jnp.zeros((ROWS_Y, Z), f32)
        for c in range(3):
            for i in range(NX):
                for k in range(3):
                    NYS[c, i, k : k + 1, :] = N[c, i, k, 0:1, :]
                packed = jnp.where(lane == c * (NX + 1) + i, N[c, i, 0][:, 0:1], packed)
        NZS[...] = packed

    def rim_unpack():
        for c in range(3):
            for k in range(3):
                N[c, NX, k] = NXR[c, k]
                N[c, NX, k, NY : NY + 1, :] = NXYR[c, k : k + 1, :]
                for i in range(NX):
                    N[c, i, k, NY : NY + 1, :] = NYR[c, i, k : k + 1, :]
        last = in_lane(NX)
        packed = jnp.where(last, pltpu.roll(NZR[1], NX, 1), NZR[0])
        below = jnp.where(last[0:1], pltpu.roll(NZR[3], NX, 1)[0:1], NZR[2][0:1])
        packed = jnp.where(row == NY, jnp.broadcast_to(below, (ROWS_Y, Z)), packed)
        for c in range(3):
            for i in range(NX + 1):
                at_ = c * (NX + 1) + i
                N[c, i, 3] = jnp.where(lane == Z - 1, packed[:, at_ : at_ + 1], pltpu.roll(N[c, i, 0], Z - 1, 1))

    scale = [plus_values[m // 9] * plus_values[m // 3 % 3] * plus_values[m % 3] for m in range(27)]

    def assemble():
        def plane(x, carry):
            rx, ix = x // X, x % X
            for ry in range(GY):
                for m in range(FIELDS):
                    v = GU[rx, ry, m, ix]
                    if m < 27:
                        UM[m, x, ry * Y : ry * Y + Y, :] = scale[m] * v
                    else:
                        VM[m - 27, x, ry * Y : ry * Y + Y, :] = v
            return carry

        lax.fori_loop(0, XG, plane, 0)

    lanes = lax.broadcasted_iota(jnp.int32, (YG, Z), 1)
    W2, W3 = 2 * EDGE, 3 * EDGE

    def within(lo, hi):
        return (lanes >= lo) & (lanes < hi)

    def strip_own():
        def one(q, carry):
            for m in range(FIELDS):
                out = jnp.zeros((YG, Z), f32)
                for h in range(2):
                    t = UM[m, q + h * NS] if m < 27 else VM[m - 27, q + h * NS]
                    o = h * HALF
                    out = jnp.where(within(o, o + W2), pltpu.roll(t, o + W2, 1), out)
                    out = jnp.where(within(o + 2 * W2, o + 3 * W2), pltpu.roll(t, o + 2 * W2, 1), out)
                if m < 27:
                    US[m, q] = out
                else:
                    VS[m - 27, q] = out
            return carry

        lax.fori_loop(0, NS, one, 0)

    def strip_halo():
        for rx in range(GX):
            for ry in range(GY):
                ZA[rx, :, :, ry * Y : ry * Y + Y, :] = ZR[rx, ry]
        for q in range(NS):
            for m in range(FIELDS):
                out = US[m, q] if m < 27 else VS[m - 27, q]
                for h in range(2):
                    x = q + h * NS
                    rx, ix = x // X, x % X
                    t = m * X + ix
                    v, p = t // SLOTS, EDGE * (t % SLOTS)
                    for side in range(2):
                        o = h * HALF + W2 + side * EDGE
                        piece = ZA[rx, side, v]
                        by = (o - p) % Z
                        piece = pltpu.roll(piece, by, 1) if by else piece
                        if m < 27:
                            piece = scale[m] * piece
                        out = jnp.where(within(o, o + EDGE), piece, out)
                if m < 27:
                    US[m, q] = out
                else:
                    VS[m - 27, q] = out

    def ynext(t):
        return pltpu.roll(t, YG - 1, 0)

    def yprev(t):
        return pltpu.roll(t, 1, 0)

    def znext(t):
        return pltpu.roll(t, Z - 1, 1)

    def zprev(t):
        return pltpu.roll(t, 1, 1)

    def coefficients(V, C, nx, wrap):
        dt = DT[...]
        for q in range(nx):
            nxt = V[0, q + 1] if q < nx - 1 else wrap(V[0, 0])
            for d in range(3):
                v = V[d, q]
                ahead = nxt if d == 0 else ynext(v) if d == 1 else znext(v)
                face = (0.5 * dt) * (v + ahead)
                C[q, 3 * d] = jnp.maximum(face, 0.0)
                C[q, 3 * d + 1] = jnp.minimum(face, 0.0)
                C[q, 3 * d + 2] = (2.0 * dt) * v

    def line(u, hp, hm, v2, ahead, behind):
        e = u[0] + u[2]
        up = hp * (e + u[1]) + hm * ahead(e - u[1])
        low = behind(up)
        diff = low - up
        return diff, 3.0 * (v2 * u[0] - (low + up)), 5.0 * (v2 * u[1] + diff)

    def rate(src, C, F, nx, wrap, write):
        for n in range(9):
            tp, tm = [], []
            for q in range(nx):
                u0, u1, u2 = src[n, q], src[9 + n, q], src[18 + n, q]
                e = u0 + u2
                tp.append(e + u1)
                tm.append(e - u1)
            for q in range(nx):
                nxt = tm[q + 1] if q < nx - 1 else wrap(tm[0])
                f = C[q, 0] * tp[q] + C[q, 1] * nxt
                F[q + 1, n] = f
                if q == nx - 1:
                    F[0, n] = wrap(f)

        def block(q, carry):
            vx = C[q, 2]
            for a in range(3):
                u = [src[9 * a + n, q] for n in range(9)]
                acc = []
                for n in range(9):
                    up, low = F[q + 1, n], F[q, n]
                    if a == 0:
                        acc.append(low - up)
                    elif a == 1:
                        acc.append(3.0 * (vx * src[n, q] - (low + up)))
                    else:
                        acc.append(5.0 * (vx * src[9 + n, q] + (low - up)))
                for d, st, ot, ahead, behind in ((1, 3, 1, ynext, yprev), (2, 1, 3, znext, zprev)):
                    hp, hm, v2 = C[q, 3 * d], C[q, 3 * d + 1], C[q, 3 * d + 2]
                    for o in range(3):
                        at_ = [ot * o + st * t for t in range(3)]
                        out = line([u[t] for t in at_], hp, hm, v2, ahead, behind)
                        for t in range(3):
                            acc[at_[t]] = acc[at_[t]] + out[t]
                for n in range(9):
                    write(9 * a + n, q, acc[n])
            return carry

        if nx <= 4:
            for q in range(nx):
                block(q, 0)
        else:
            lax.fori_loop(0, nx, block, 0)

    def advance(Ur, Wr, C, F, nx, wrap):
        def put(m, q, value):
            Wr[m, q] = value

        def step(m, q, value):
            Ur[m, q] = (Ur[m, q] + Wr[m, q]) + 0.5 * value

        def substep(t, carry):
            rate(Ur, C, F, nx, wrap, put)
            rate(Wr, C, F, nx, wrap, step)
            return carry

        lax.fori_loop(0, SUBSTEPS, substep, 0)

    def same(t):
        return t

    def half_turn(t):
        return pltpu.roll(t, HALF, 1)

    def finish_field():
        U[...] = jnp.zeros_like(U)
        for m in range(27):
            for ix in range(X):
                t = UM[m, ix]
                h, q = ix // NS, ix % NS
                s = US[m, q]
                o = h * HALF
                left = pltpu.roll(s, (Z - o - 2 * W2) % Z, 1)
                right = pltpu.roll(s, (Z - W2 - o) % Z, 1)
                t = jnp.where(lanes < EDGE, left, jnp.where(lanes >= Z - EDGE, right, t))
                U[m, ix * Y : ix * Y + Y, :] = (1.0 / scale[m]) * t[0:Y]

    def yz_of(src):
        def yz(i, carry):
            for c in range(3):
                yv, yd = [], []
                for k in range(4):
                    sv = sd = None
                    for j in range(NY + 1):
                        x = src[c, i, k, j : j + 1, :]
                        tv, td = tab[oTV + j] * x, tab[oTD + j] * x
                        sv = tv if sv is None else sv + tv
                        sd = td if sd is None else sd + td
                    yv.append(sv)
                    yd.append(sd)
                for r in range(4):
                    A[0, c, i, r] = sum(float(value[r, k]) * yv[k] for k in range(4))
                    A[1, c, i, r] = sum(float(value[r, k]) * yd[k] for k in range(4))
                    A[2, c, i, r] = sum(float(slope[r, k]) * yv[k] for k in range(4))
            return carry

        lax.fori_loop(0, NX + 1, yz, 0)

    def slope_at(ix, p, r, c, d):
        tb = slope if d == 0 else value
        return sum(float(tb[p, m]) * A[d, c, 3 * ix + m, r] for m in range(4))

    def jacobians(t):
        ix, r = t // 4, t % 4
        for p in range(4):
            for c in range(3):
                for d in range(3):
                    jac = slope_at(ix, p, r, c, d)
                    J[d, c, ix, p, r] = jac + 1.0 if c == d else jac

    rows_start(0, 0)
    rim_pack()
    for cp in rim_copies():
        cp.start()
    for ry in range(1, GY):
        plane_copy(ry).wait_recv()
        for cp in core_copies(ry):
            cp.start()
    for cp in edge_copies():
        cp.wait_recv()
    for cp in edge_core_copies():
        cp.start()
    for cp in rim_copies():
        cp.wait()
    rim_unpack()
    yz_of(N)

    def all_jacobians(t, carry):
        jacobians(t)
        return carry

    lax.fori_loop(0, 4 * X, all_jacobians, 0)
    rows_finish(0)
    fastest = functools.reduce(jnp.maximum, [ROWS[0, n] for n in range(devices)])
    fastest = jnp.max(fastest, axis=(0, 1), keepdims=True)
    DT[...] = jnp.broadcast_to(courant / jnp.maximum(fastest, 0.25), (YG, Z))
    for ry in range(GY):
        for cp in core_copies(ry):
            cp.wait_recv()
    assemble()
    strip_own()
    coefficients(VM, CM, XG, same)
    advance(UM, WM, CM, FM, XG, same)
    for cp in edge_core_copies():
        cp.wait_recv()
    strip_halo()
    coefficients(VS, CS, NS, half_turn)
    advance(US, WS, CS, FT, NS, half_turn)
    finish_field()
    def size_of(ix, carry):
        mid = {}
        for a in range(3):
            for r in range(4):
                mid[a, r] = None
            for c in range(3):
                t = None
                for b in range(3):
                    for e in range(Y):
                        term = tab[oL + b * Y + e] * U[a * 9 + b * 3 + c, pl.ds(ix * Y + e, 1), :]
                        t = term if t is None else t + term
                for r in range(4):
                    term = float(legendre[r, c]) * t
                    mid[a, r] = term if mid[a, r] is None else mid[a, r] + term
        for p in range(4):
            for r in range(4):
                s = sum(float(legendre[p, a]) * mid[a, r] for a in range(3))
                SIZ[ix, p, r] = jnp.exp(theta_size * s)
        return carry

    lax.fori_loop(0, X, size_of, 0)

    wrow = tab[oW]
    pairs = [(d, e) for d in range(3) for e in range(d, 3)]

    def dot3(p, q, d, e):
        return p[0][d] * q[0][e] + p[1][d] * q[1][e] + p[2][d] * q[2][e]

    def gauss_weight(r):
        return jnp.where((r == 0) | (r == 3), float(weights[0]), float(weights[1]))

    def gauss(t, esum):
        ix, r = t // 4, t % 4
        for p in range(4):
            size = SIZ[ix, p, r]
            inv = 1.0 / size
            M = [[J[d, c, ix, p, r] * inv for d in range(3)] for c in range(3)]
            D = [[None] * 3 for _ in range(3)]
            metric = None
            for d, e in pairs:
                dev = dot3(M, M, d, e)
                if d == e:
                    dev = dev - 1.0
                D[d][e] = D[e][d] = dev
                sq = dev * dev if d == e else 2.0 * (dev * dev)
                metric = sq if metric is None else metric + sq
            w = wrow * (gauss_weight(r) * float(weights[p]))
            size2 = size * size
            esum = esum + w * (size2 * size) * metric
            scale = (4.0 * w) * size2
            for c in range(3):
                for d in range(3):
                    g = M[c][0] * D[0][d] + M[c][1] * D[1][d] + M[c][2] * D[2][d]
                    G[d, c, ix, p, r] = scale * g
        return esum

    zero = jnp.zeros((ROWS_Y, Z), f32)
    esum = lax.fori_loop(0, 4 * X, gauss, zero)

    def back_c(c, carry):
        for i in range(NX + 1):
            bv = [None] * 4
            bd = [None] * 4
            for r in range(4):
                ga = []
                for d in range(3):
                    tb = slope if d == 0 else value
                    acc = None
                    for ix in range(X):
                        m = i - 3 * ix
                        if 0 <= m <= 3:
                            for p in range(4):
                                term = float(tb[p, m]) * G[d, c, ix, p, r]
                                acc = term if acc is None else acc + term
                    ga.append(acc)
                for k in range(4):
                    tv = float(value[r, k]) * ga[0] + float(slope[r, k]) * ga[2]
                    td = float(value[r, k]) * ga[1]
                    bv[k] = tv if bv[k] is None else bv[k] + tv
                    bd[k] = td if bd[k] is None else bd[k] + td
            for k in range(4):
                B[0, i, k] = bv[k]
                B[1, i, k] = bd[k]
        for i in range(NX + 1):
            for k in range(4):
                acc = None
                for s in range(ROWS_Y):
                    term = tab[oGV + s] * B[0, i, k, s : s + 1, :] + tab[oGD + s] * B[1, i, k, s : s + 1, :]
                    acc = term if acc is None else acc + term
                GN[c, i, k] = acc
        return carry

    lax.fori_loop(0, 3, back_c, 0)

    def row_of(column_of):
        out = zero
        for c in range(3):
            out = jnp.where(lane == c * ROWS_Y + row, column_of(c), out)
        return jnp.sum(out, axis=0, keepdims=True)

    far, near = zero, zero
    for c in range(3):
        for i in range(NX + 1):
            here = lane == c * (NX + 1) + i
            far = jnp.where(here, GN[c, i, 3][:, Z - 1 : Z], far)
            near = jnp.where(here, GN[c, i, 0][:, 0:1], near)
    FZS[0] = far
    FZS[1] = near
    for zs_, (k, at_) in enumerate(((3, Z - 1), (0, 0))):
        for xs_, i in enumerate((NX, 0)):
            FES[zs_, xs_] = row_of(lambda c: GN[c, i, k][:, at_ : at_ + 1])
        for ys_, j in enumerate((NY, 0)):
            FES[zs_, 2 + ys_] = FZS[zs_][j : j + 1]
    for c in range(3):
        for i in range(NX + 1):
            GN[c, i, 0] = GN[c, i, 0] + jnp.where(lane == 0, 0.0, pltpu.roll(GN[c, i, 3], 1, 1))
            for k in range(4):
                FYS[0, c, i, k : k + 1, :] = GN[c, i, k, NY : NY + 1, :]
                FYS[1, c, i, k : k + 1, :] = GN[c, i, k, 0:1, :]
    ways = (1, -1)

    def fold_copies():
        out = []

        def add(src, dst, move):
            n = len(out)
            out.append(remote(src, dst, fs.at[n], fr.at[n], move))

        for zs_ in range(2):
            for xs_ in range(2):
                for ys_ in range(2):
                    add(FES.at[zs_, xs_], FER.at[zs_, 4 + 2 * xs_ + ys_], (ways[xs_], ways[ys_], ways[zs_]))
            for ys_ in range(2):
                add(FES.at[zs_, 2 + ys_], FER.at[zs_, 2 + ys_], (0, ways[ys_], ways[zs_]))
            for xs_ in range(2):
                add(FES.at[zs_, xs_], FER.at[zs_, xs_], (ways[xs_], 0, ways[zs_]))
            add(FZS.at[zs_], FZR.at[zs_], (0, 0, ways[zs_]))
        for ys_ in range(2):
            for xs_ in range(2):
                add(FYS.at[ys_, :, (NX, 0)[xs_]], FXYR.at[xs_, ys_], (ways[xs_], ways[ys_], 0))
            add(FYS.at[ys_], FYR.at[ys_], (0, ways[ys_], 0))
        for xs_ in range(2):
            add(GN.at[:, (NX, 0)[xs_]], FXR.at[xs_], (ways[xs_], 0, 0))
        return out

    for cp in fold_copies():
        cp.start()
    for cp in fold_copies():
        cp.wait()

    lane1, row_j = lane[0:1], lane[0:1] % ROWS_Y
    planes = []
    for zs_ in range(2):
        p = FZR[zs_]
        p = p + jnp.where(row == 0, FER[zs_, 2], 0.0) + jnp.where(row == NY, FER[zs_, 3], 0.0)
        for xs_, i in enumerate((0, NX)):
            edge = FER[zs_, xs_]
            edge = edge + jnp.where(row_j == 0, pltpu.roll(FER[zs_, 4 + 2 * xs_], Z - NY, 1), 0.0)
            edge = edge + jnp.where(row_j == NY, pltpu.roll(FER[zs_, 5 + 2 * xs_], NY, 1), 0.0)
            for c in range(3):
                col = jnp.sum(jnp.where(lane == c * ROWS_Y + row, edge, 0.0), axis=1, keepdims=True)
                p = p + jnp.where(lane == c * (NX + 1) + i, col, 0.0)
        planes.append(p)
    for c in range(3):
        for k in range(4):
            for xs_, i in enumerate((0, NX)):
                GN[c, i, k] = GN[c, i, k] + FXR[xs_, c, k]
                for ys_, j in enumerate((0, NY)):
                    GN[c, i, k, j : j + 1, :] = GN[c, i, k, j : j + 1, :] + FXYR[xs_, ys_, c, k : k + 1, :]
            for i in range(NX + 1):
                for ys_, j in enumerate((0, NY)):
                    GN[c, i, k, j : j + 1, :] = GN[c, i, k, j : j + 1, :] + FYR[ys_, c, i, k : k + 1, :]
        for i in range(NX + 1):
            n = c * (NX + 1) + i
            full = GN[c, i, 0] + jnp.where(lane == 0, planes[0][:, n : n + 1], 0.0)
            GN[c, i, 0] = full
            GN[c, i, 3] = jnp.where(lane == Z - 1, GN[c, i, 3] + planes[1][:, n : n + 1], pltpu.roll(full, Z - 1, 1))
    ssum = zero
    for c in range(3):
        for i in range(NX):
            for k in range(3):
                g = GN[c, i, k]
                ssum = ssum + g * g
    ssum = jnp.where(row < NY, ssum, 0.0)
    elements = float(EL * Z * devices)
    entries = 81.0 * elements
    mine = jnp.sum(ssum, axis=(0, 1), keepdims=True)
    bound = trial_step / jnp.sqrt(1.0 + mine / entries)
    bound = jnp.broadcast_to(bound, (ROWS_Y, Z))
    yz_of(GN)

    def trial(t, sums):
        ix, r = t // 4, t % 4
        s2, s3, s4 = sums
        for p in range(4):
            size = SIZ[ix, p, r]
            inv = 1.0 / size
            move = -(inv * bound)
            M = [[J[d, c, ix, p, r] * inv for d in range(3)] for c in range(3)]
            K = [[slope_at(ix, p, r, c, d) * move for d in range(3)] for c in range(3)]
            w = wrow * (gauss_weight(r) * float(weights[p])) * (size * size * size)
            q = [None] * 3
            for d, e in pairs:
                d0 = dot3(M, M, d, e)
                d2 = dot3(K, K, d, e)
                if d == e:
                    d0 = d0 - 1.0
                    d1 = 2.0 * dot3(M, K, d, d)
                else:
                    d1 = dot3(M, K, d, e) + dot3(K, M, d, e)
                terms = [d1 * d1 + 2.0 * (d0 * d2), 2.0 * (d1 * d2), d2 * d2]
                for n in range(3):
                    term = terms[n] if d == e else 2.0 * terms[n]
                    q[n] = term if q[n] is None else q[n] + term
            s2, s3, s4 = s2 + w * q[0], s3 + w * q[1], s4 + w * q[2]
        return s2, s3, s4

    sums = lax.fori_loop(0, 4 * X, trial, (zero,) * 3)
    block = zero
    for n, part in enumerate((esum, ssum) + tuple(sums)):
        block = jnp.where(row == n, jnp.sum(part, axis=0, keepdims=True), block)
    column = jnp.sum(block, axis=1, keepdims=True)
    ROWS[1, 0, 0:1] = jnp.sum(jnp.where(lane == row, column, 0.0), axis=0, keepdims=True)
    ROWS[1, 0, 1:2] = 1.0 / bound[0:1]
    rows_start(1, 0)
    for c in range(3):
        for k in range(3):
            slab[c * NX : (c + 1) * NX, :, k * Z : (k + 1) * Z] = GN[c, 0:NX, k]
    woven = lax.dot_general(
        slab[...].reshape(3 * NX * ROWS_Y, 3 * Z), perm[...], (((1,), (1,)), ((), ())),
        precision=lax.Precision.HIGHEST, preferred_element_type=f32,
    ).reshape(3, NX, ROWS_Y, 3 * Z)
    grad[...] = woven[:, :, 0:NY, :]
    for ix in range(X):
        adv[:, ix] = U[:, ix * Y : ix * Y + Y, :]
    rows_finish(1)
    every = [ROWS[1, n] for n in range(devices)]
    l1 = lax.broadcasted_iota(jnp.int32, (1, Z), 1)

    def lane_sum(x, n):
        return jnp.sum(jnp.where(l1 == n, x, 0.0), axis=1, keepdims=True)

    sums = sum(x[0:1] for x in every)
    etot, stot = lane_sum(sums, 0), lane_sum(sums, 1)
    step = trial_step / jnp.sqrt(1.0 + stot / entries)
    higher = jnp.zeros((1, Z), f32)
    for x in every:
        h = step * x[1:2]
        h2 = h * h
        power = jnp.where(l1 == 2, h2, jnp.where(l1 == 3, h2 * h, h2 * h2))
        higher = higher + x[0:1] * power
    higher = jnp.sum(jnp.where((l1 >= 2) & (l1 < 5), higher, 0.0), axis=1, keepdims=True)
    ttot = (etot - step * stot) + higher
    for ry in range(GY):
        if ry:
            plane_copy(ry).wait_send()
        for cp in core_copies(ry):
            cp.wait_send()
    for cp in edge_copies() + edge_core_copies():
        cp.wait_send()
    rows_sent(0)
    rows_sent(1)
    checks[...] = jnp.where(
        l1 == 0, etot / elements, jnp.where(l1 == 1, stot / entries, ttot / elements)
    )


def publish(adv, grad, checks, adv_out, grad_out, checks_out, sem):
    copies = [
        pltpu.make_async_copy(grad, grad_out, sem.at[0]),
        pltpu.make_async_copy(adv, adv_out, sem.at[1]),
    ]
    for cp in copies:
        cp.start()
    row = checks[...]
    lane = lax.broadcasted_iota(jnp.int32, row.shape, 1)
    for n in range(3):
        checks_out[n] = jnp.sum(jnp.where(lane == n, row, 0.0))
    for cp in copies:
        cp.wait()


def solution(mesh):
    sizes = tuple(mesh.shape[a] for a in AXES)

    def on_device(displacement, size_field_modes, velocity):
        modes, X, Y, Z = size_field_modes.shape
        assert Y == 2 and displacement.shape == (3, 3 * X, 3 * Y, 3 * Z)
        R, NX, NY = 4 * Y, 3 * X, 3 * Y
        tab = jnp.asarray(row_tables(Y, Z))
        devices = sizes[0] * sizes[1] * sizes[2]
        GX, GY = sizes[0], sizes[1]
        XG, YG, NS = GX * X, GY * Y, GX * X // 2
        packs = -(-30 * X // (Z // (2 * SUBSTEPS)))
        assert YG == 8 and XG % 2 == 0 and min(sizes) > 1
        vm = lambda *shape: pltpu.VMEM(shape, jnp.float32)
        dma = lambda *shape: pltpu.SemaphoreType.DMA(shape)
        spec = pl.BlockSpec(memory_space=pltpu.VMEM)
        adv, grad, checks = pl.pallas_call(
            functools.partial(kernel, sizes, X, Y, Z),
            out_shape=(
                pltpu.VMEM(size_field_modes.shape, jnp.float32),
                pltpu.VMEM(displacement.shape, jnp.float32),
                pltpu.VMEM((1, Z), jnp.float32),
            ),
            in_specs=[pl.BlockSpec(memory_space=pl.ANY)] * 3 + [spec],
            out_specs=(spec,) * 3,
            scratch_shapes=[
                vm(3, NX, NY, 3 * Z), vm(GX, GY, 30, X, Y, Z), vm(2, packs, Y, Z), vm(GX, GY, 2, packs, Y, Z), vm(GX, 2, packs, YG, Z),
                vm(27, XG, YG, Z), vm(27, XG, YG, Z), vm(3, XG, YG, Z), vm(XG, 9, YG, Z), vm(XG + 1, 9, YG, Z),
                vm(27, NS, YG, Z), vm(27, NS, YG, Z), vm(3, NS, YG, Z), vm(NS, 9, YG, Z), vm(NS + 1, 9, YG, Z),
                vm(3 * Z, 3 * Z), vm(3 * NX, R, 3 * Z), vm(27, R, Z),
                vm(2, devices, 2, Z),
                vm(3, NX + 1, 4, R, Z), vm(3, NX + 1, 4, R, Z),
                vm(3, 3, NX + 1, 4, R, Z), vm(3, 3, X, 4, 4, R, Z), vm(3, 3, X, 4, 4, R, Z), vm(2, NX + 1, 4, R, Z), vm(X, 4, 4, R, Z), vm(R, Z),
                vm(3, 3, R, Z), vm(3, NX, 3, Z), vm(3, NX, 3, Z), vm(3, 3, Z), vm(R, Z), vm(4, R, Z),
                vm(2, 3, 4, R, Z), vm(2, 3, NX + 1, 4, Z), vm(2, 3, NX + 1, 4, Z), vm(2, 2, 3, 4, Z), vm(2, R, Z), vm(2, R, Z), vm(2, 4, 1, Z), vm(2, 8, 1, Z),
                dma(3), dma(GY), dma(GY), dma(GX, GY), dma(GX, GY), dma(2, GY), dma(2, GY), dma(GX), dma(GX), dma(2, 2), dma(2, 2), dma(7), dma(7), dma(26), dma(26),
            ],
            compiler_params=pltpu.CompilerParams(collective_id=0, has_side_effects=True),
        )(displacement, size_field_modes, velocity, tab)
        return tuple(
            pl.pallas_call(
                publish,
                out_shape=(
                    jax.ShapeDtypeStruct(size_field_modes.shape, jnp.float32),
                    jax.ShapeDtypeStruct(displacement.shape, jnp.float32),
                    jax.ShapeDtypeStruct((3,), jnp.float32),
                ),
                in_specs=[spec] * 3,
                out_specs=(pl.BlockSpec(memory_space=pl.ANY),) * 2 + (pl.BlockSpec(memory_space=pltpu.SMEM),),
                scratch_shapes=[dma(2)],
            )(*(pltpu.with_memory_space_constraint(a, pltpu.VMEM) for a in (adv, grad, checks)))
        )

    return jax.shard_map(
        on_device,
        mesh=mesh,
        in_specs=(P(None, "gx", "gy", "gz"),) * 3,
        out_specs=(P(None, "gx", "gy", "gz"), P(None, "gx", "gy", "gz"), P()),
        check_vma=False,
    )
```

```python
import functools

import jax
import jax.numpy as jnp
import numpy as np
from jax import lax
from jax.experimental import pallas as pl
from jax.experimental.pallas import tpu as pltpu
from jax.sharding import PartitionSpec as P

SUBSTEPS = 4
MESH = pl.DeviceIdType.MESH
AXES = ("gx", "gy", "gz")

plus_values = (0.7071067811865476, 1.224744871391589, 1.5811388300841898)
g10 = 1.7320508075688772
g21 = 3.872983346207417
courant = 0.1
theta_size = 0.3
trial_step = 0.05


def tables_1d():
    points = np.array(
        [-0.8611363115940526, -0.3399810435848563, 0.3399810435848563, 0.8611363115940526]
    )
    weights = np.array(
        [0.3478548451374538, 0.6521451548625461, 0.6521451548625461, 0.3478548451374538]
    )
    points = 0.5 * (points + 1.0)
    weights = 0.5 * weights
    nodes = np.array([0.0, 1.0 / 3.0, 2.0 / 3.0, 1.0])
    value = np.zeros((4, 4))
    slope = np.zeros((4, 4))
    for m in range(4):
        others = [nodes[o] for o in range(4) if o != m]
        den = np.prod([nodes[m] - o for o in others])
        for q in range(4):
            g = points[q]
            value[q, m] = np.prod([g - o for o in others]) / den
            slope[q, m] = (
                sum(np.prod([g - others[t] for t in range(3) if t != s]) for s in range(3)) / den
            )
    c = 2.0 * points - 1.0
    legendre = np.stack(
        [
            np.full(4, plus_values[0]),
            plus_values[1] * c,
            plus_values[2] * 0.5 * (3.0 * c**2 - 1.0),
        ],
        axis=1,
    )
    return value, slope, legendre, weights


def row_tables(Y, Z):
    value, slope, legendre, weights = tables_1d()
    rows, nodes = 4 * Y, 3 * Y + 1
    tv = np.zeros((rows, rows))
    td = np.zeros((rows, rows))
    for e in range(Y):
        tv[4 * e : 4 * e + 4, 3 * e : 3 * e + 4] = value
        td[4 * e : 4 * e + 4, 3 * e : 3 * e + 4] = slope
    blocks = [tv[:, j] for j in range(nodes)] + [td[:, j] for j in range(nodes)]
    blocks += [tv[s, :] for s in range(rows)] + [td[s, :] for s in range(rows)]
    for b in range(3):
        for e in range(Y):
            col = np.zeros(rows)
            col[4 * e : 4 * e + 4] = legendre[:, b]
            blocks.append(col)
    blocks.append(np.tile(weights, Y))
    stacked = np.stack(blocks).astype(np.float32)
    return np.ascontiguousarray(np.broadcast_to(stacked[:, :, None], stacked.shape + (Z,)))


def kernel(sizes, X, Y, Z, disp_in, modes_in, vel_in, tab_in, adv, grad, checks,
           disp, tab, GU, ZP, ZR, ZA, UM, VM, CM, FM, US, VS, CS, FT,
           perm, slab, U, ROWS, N, GN, A, G, J, B, SIZ, DT,
           NXR, NYS, NYR, NXYR, NZS, NZR, FXR, FYS, FYR, FXYR, FZS, FZR, FES, FER,
           ls, g1s, g1r, g2s, g2r, zs, zr, y2s, y2r, rs, rr, ns, nr, fs, fr):
    value, slope, legendre, weights = tables_1d()
    NX, NY = 3 * X, 3 * Y
    ROWS_Y = 4 * Y
    EL = X * Y
    f32 = jnp.float32
    index = [lax.axis_index(a) for a in AXES]
    lane = lax.broadcasted_iota(jnp.int32, (ROWS_Y, Z), 1)
    row = lax.broadcasted_iota(jnp.int32, (ROWS_Y, Z), 0)
    oTV, oTD, oGV, oGD, oL, oW = 0, NY + 1, 2 * NY + 2, 2 * NY + 2 + ROWS_Y, 2 * NY + 2 + 2 * ROWS_Y, 2 * NY + 2 + 2 * ROWS_Y + 3 * Y

    def at(axis, by):
        n = sizes[axis]
        return {AXES[axis]: lax.rem(index[axis] + (by + n), n)}

    barrier = pltpu.get_barrier_semaphore()
    total = 0
    for a in range(sizes[0]):
        for b in range(sizes[1]):
            for c in range(sizes[2]):
                move = (a, b, c)
                if not any(move) or (c and (a or b)):
                    continue
                target = {}
                for axis in range(3):
                    if move[axis]:
                        target.update(at(axis, move[axis]))
                pl.semaphore_signal(barrier, inc=1, device_id=target, device_id_type=MESH)
                total += 1

    loads = [
        pltpu.make_async_copy(modes_in, GU.at[0, 0, 0:27], ls.at[0]),
        pltpu.make_async_copy(vel_in, GU.at[0, 0, 27:30], ls.at[1]),
        pltpu.make_async_copy(disp_in, disp, ls.at[2]),
        pltpu.make_async_copy(tab_in, tab, ls.at[3]),
    ]
    for cp in loads:
        cp.start()

    def copy(src, dst, ss, sr, axis, by):
        return pltpu.make_async_remote_copy(
            src_ref=src, dst_ref=dst, send_sem=ss, recv_sem=sr,
            device_id=at(axis, by), device_id_type=MESH,
        )

    GX, GY = sizes[0], sizes[1]
    XG, YG, NS, EDGE = GX * X, GY * Y, GX * X // 2, 2 * SUBSTEPS
    HALF, FIELDS, SLOTS = Z // 2, 30, Z // EDGE

    def moved(move):
        target = {}
        for axis in range(3):
            if move[axis] % sizes[axis]:
                target.update(at(axis, move[axis] % sizes[axis] ))
        return target

    def remote(src, dst, ss, sr, move):
        return pltpu.make_async_remote_copy(
            src_ref=src, dst_ref=dst, send_sem=ss, recv_sem=sr,
            device_id=moved(move), device_id_type=MESH,
        )

    def plane_copy(ry):
        return remote(GU.at[0, 0], GU.at[0, ry], g1s.at[ry], g1r.at[ry], (0, -ry, 0))

    def core_copies(ry):
        return [
            remote(GU.at[0, ry], GU.at[rx, ry], g2s.at[rx, ry], g2r.at[rx, ry], (-rx, 0, 0))
            for rx in range(1, GX)
        ]

    def edge_copies():
        return [
            remote(ZP.at[side], ZR.at[0, 0, side], zs.at[side, 0], zr.at[side, 0], (0, 0, 2 * side - 1))
            for side in range(2)
        ]

    def edge_plane_copies():
        return [
            remote(ZR.at[0, 0], ZR.at[0, ry], zs.at[0, ry], zr.at[0, ry], (0, -ry, 0)) for ry in range(1, GY)
        ]

    def edge_core_copies():
        return [
            remote(ZR.at[0], ZR.at[rx], y2s.at[rx], y2r.at[rx], (-rx, 0, 0)) for rx in range(1, GX)
        ]

    slot2 = lax.broadcasted_iota(jnp.int32, (Y, Z), 1) // EDGE
    packs = -(-FIELDS * X // SLOTS)

    def pack_edges():
        acc = [[jnp.zeros((Y, Z), f32) for _ in range(packs)] for _ in range(2)]
        for m in range(FIELDS):
            for ix in range(X):
                t = m * X + ix
                v, p = t // SLOTS, EDGE * (t % SLOTS)
                x = GU[0, 0, m, ix]
                low = pltpu.roll(x, p, 1) if p else x
                high = pltpu.roll(x, (p + EDGE) % Z, 1) if (p + EDGE) % Z else x
                acc[0][v] = jnp.where(slot2 == t % SLOTS, low, acc[0][v])
                acc[1][v] = jnp.where(slot2 == t % SLOTS, high, acc[1][v])
        for side in range(2):
            for v in range(packs):
                ZP[side, v] = acc[side][v]

    def unweave():
        a_i = lax.broadcasted_iota(jnp.int32, (3 * Z, 3 * Z), 0)
        b_i = lax.broadcasted_iota(jnp.int32, (3 * Z, 3 * Z), 1)
        b_k = (b_i >= Z).astype(jnp.int32) + (b_i >= 2 * Z).astype(jnp.int32)
        perm[...] = (a_i == 3 * (b_i - b_k * Z) + b_k).astype(f32)
        slab[...] = jnp.zeros_like(slab)
        for c in range(3):
            for i in range(NX):
                slab[c * NX + i, 0:NY, :] = disp[c, i]
        spread = jnp.dot(
            slab[...].reshape(3 * NX * ROWS_Y, 3 * Z), perm[...],
            precision=lax.Precision.HIGHEST, preferred_element_type=f32,
        ).reshape(3, NX, ROWS_Y, 3 * Z)
        for c in range(3):
            for k in range(3):
                N[c, 0:NX, k] = spread[c, :, :, k * Z : (k + 1) * Z]

    devices = sizes[0] * sizes[1] * sizes[2]
    by_column = [(2,), (0, 1)]
    plans = [by_column, [(0, 1, 2)] if devices <= 64 else by_column]

    def row_stage(r, stage):
        block = 1
        stages = plans[r]
        for axes in stages[:stage]:
            for axis in axes:
                block *= sizes[axis]
        moves = [()]
        for axis in range(3):
            moves = [m + (b,) for m in moves for b in range(sizes[axis] if axis in stages[stage] else 1)]
        src = ROWS.at[r, 0:block]
        copies = [
            remote(src, ROWS.at[r, n * block : (n + 1) * block], rs.at[r, stage], rr.at[r, stage], m)
            for n, m in enumerate(moves) if n
        ]
        rest = ROWS.at[r, block : len(moves) * block]
        return copies, remote(rest, rest, rs.at[r, stage], rr.at[r, stage], moves[1])

    def rows_start(r, stage):
        for cp in row_stage(r, stage)[0]:
            cp.start()

    def rows_relay(r):
        for stage in range(len(plans[r]) - 1):
            row_stage(r, stage)[1].wait_recv()
            rows_start(r, stage + 1)

    def rows_finish(r):
        row_stage(r, len(plans[r]) - 1)[1].wait_recv()

    def rows_sent(r):
        for stage in range(len(plans[r])):
            row_stage(r, stage)[1].wait_send()

    in_lane = lambda n: functools.reduce(jnp.logical_or, [lane == c * (NX + 1) + n for c in range(3)])

    def rim_copies():
        out = [
            remote(N.at[:, 0, 0:3], NXR, ns.at[0], nr.at[0], (-1, 0, 0)),
            remote(NYS, NYR, ns.at[1], nr.at[1], (0, -1, 0)),
            remote(NYS.at[:, 0], NXYR, ns.at[2], nr.at[2], (-1, -1, 0)),
        ]
        return out

    def rim_column():
        return remote(NZS, NZR.at[0], ns.at[3], nr.at[3], (0, 0, -1))

    def rim_relays():
        return [
            remote(NZR.at[0], NZR.at[n], ns.at[3 + n], nr.at[3 + n], move)
            for n, move in ((1, (-1, 0, 0)), (2, (0, -1, 0)), (3, (-1, -1, 0)))
        ]

    def rim_pack():
        packed = jnp.zeros((ROWS_Y, Z), f32)
        for c in range(3):
            for i in range(NX):
                for k in range(3):
                    NYS[c, i, k : k + 1, :] = N[c, i, k, 0:1, :]
                packed = jnp.where(lane == c * (NX + 1) + i, N[c, i, 0][:, 0:1], packed)
        NZS[...] = packed

    def rim_unpack():
        for c in range(3):
            for k in range(3):
                N[c, NX, k] = NXR[c, k]
                N[c, NX, k, NY : NY + 1, :] = NXYR[c, k : k + 1, :]
                for i in range(NX):
                    N[c, i, k, NY : NY + 1, :] = NYR[c, i, k : k + 1, :]
        for c in range(3):
            for i in range(NX + 1):
                N[c, i, 3] = jnp.where(lane == Z - 1, 0.0, pltpu.roll(N[c, i, 0], Z - 1, 1))

    def rim_last():
        last = in_lane(NX)
        packed = jnp.where(last, pltpu.roll(NZR[1], NX, 1), NZR[0])
        below = jnp.where(last[0:1], pltpu.roll(NZR[3], NX, 1)[0:1], NZR[2][0:1])
        rows = [packed[j : j + 1] for j in range(NY)] + [below]
        pv = sum(tab[oTV + j] * rows[j] for j in range(NY + 1))
        pd = sum(tab[oTD + j] * rows[j] for j in range(NY + 1))
        end = lane == Z - 1
        for c in range(3):
            for i in range(NX + 1):
                n = c * (NX + 1) + i
                mv = jnp.where(end, pv[:, n : n + 1], 0.0)
                md = jnp.where(end, pd[:, n : n + 1], 0.0)
                for r in range(4):
                    A[0, c, i, r] = A[0, c, i, r] + float(value[r, 3]) * mv
                    A[1, c, i, r] = A[1, c, i, r] + float(value[r, 3]) * md
                    A[2, c, i, r] = A[2, c, i, r] + float(slope[r, 3]) * mv

    scale = [plus_values[m // 9] * plus_values[m // 3 % 3] * plus_values[m % 3] for m in range(27)]

    def assemble():
        def plane(x, carry):
            rx, ix = x // X, x % X
            for ry in range(GY):
                for m in range(FIELDS):
                    v = GU[rx, ry, m, ix]
                    if m < 27:
                        UM[0, m, x, ry * Y : ry * Y + Y, :] = scale[m] * v
                    else:
                        VM[m - 27, x, ry * Y : ry * Y + Y, :] = v
            return carry

        lax.fori_loop(0, XG, plane, 0)

    lanes = lax.broadcasted_iota(jnp.int32, (YG, Z), 1)
    W2, W3 = 2 * EDGE, 3 * EDGE

    def within(lo, hi):
        return (lanes >= lo) & (lanes < hi)

    def strip_own():
        def one(q, carry):
            for m in range(FIELDS):
                out = jnp.zeros((YG, Z), f32)
                for h in range(2):
                    t = UM[0, m, q + h * NS] if m < 27 else VM[m - 27, q + h * NS]
                    o = h * HALF
                    out = jnp.where(within(o, o + W2), pltpu.roll(t, o + W2, 1), out)
                    out = jnp.where(within(o + 2 * W2, o + 3 * W2), pltpu.roll(t, o + 2 * W2, 1), out)
                if m < 27:
                    US[0, m, q] = out
                else:
                    VS[m - 27, q] = out
            return carry

        lax.fori_loop(0, NS, one, 0)

    def strip_halo():
        for rx in range(GX):
            for ry in range(GY):
                ZA[rx, :, :, ry * Y : ry * Y + Y, :] = ZR[rx, ry]
        for q in range(NS):
            for m in range(FIELDS):
                out = US[0, m, q] if m < 27 else VS[m - 27, q]
                for h in range(2):
                    x = q + h * NS
                    rx, ix = x // X, x % X
                    t = m * X + ix
                    v, p = t // SLOTS, EDGE * (t % SLOTS)
                    for side in range(2):
                        o = h * HALF + W2 + side * EDGE
                        piece = ZA[rx, side, v]
                        by = (o - p) % Z
                        piece = pltpu.roll(piece, by, 1) if by else piece
                        if m < 27:
                            piece = scale[m] * piece
                        out = jnp.where(within(o, o + EDGE), piece, out)
                if m < 27:
                    US[0, m, q] = out
                else:
                    VS[m - 27, q] = out

    def ynext(t):
        return pltpu.roll(t, YG - 1, 0)

    def yprev(t):
        return pltpu.roll(t, 1, 0)

    def znext(t):
        return pltpu.roll(t, Z - 1, 1)

    def zprev(t):
        return pltpu.roll(t, 1, 1)

    def coefficients(V, C, nx, wrap):
        for q in range(nx):
            nxt = V[0, q + 1] if q < nx - 1 else wrap(V[0, 0])
            for d in range(3):
                v = V[d, q]
                ahead = nxt if d == 0 else ynext(v) if d == 1 else znext(v)
                face = 0.5 * (v + ahead)
                C[q, 3 * d] = jnp.maximum(face, 0.0)
                C[q, 3 * d + 1] = jnp.minimum(face, 0.0)
                C[q, 3 * d + 2] = 2.0 * v

    def line(u, hp, hm, v2, ahead, behind):
        e = u[0] + u[2]
        up = hp * (e + u[1]) + hm * ahead(e - u[1])
        low = behind(up)
        diff = low - up
        return diff, 3.0 * (v2 * u[0] - (low + up)), 5.0 * (v2 * u[1] + diff)

    def rate(src, dst, C, F, nx, wrap):
        for n in range(9):
            tp, tm = [], []
            for q in range(nx):
                u0, u1, u2 = src[n, q], src[9 + n, q], src[18 + n, q]
                e = u0 + u2
                tp.append(e + u1)
                tm.append(e - u1)
            for q in range(nx):
                nxt = tm[q + 1] if q < nx - 1 else wrap(tm[0])
                f = C[q, 0] * tp[q] + C[q, 1] * nxt
                F[q + 1, n] = f
                if q == nx - 1:
                    F[0, n] = wrap(f)

        def block(q, carry):
            vx = C[q, 2]
            for a in range(3):
                u = [src[9 * a + n, q] for n in range(9)]
                acc = []
                for n in range(9):
                    up, low = F[q + 1, n], F[q, n]
                    if a == 0:
                        acc.append(low - up)
                    elif a == 1:
                        acc.append(3.0 * (vx * src[n, q] - (low + up)))
                    else:
                        acc.append(5.0 * (vx * src[9 + n, q] + (low - up)))
                for d, st, ot, ahead, behind in ((1, 3, 1, ynext, yprev), (2, 1, 3, znext, zprev)):
                    hp, hm, v2 = C[q, 3 * d], C[q, 3 * d + 1], C[q, 3 * d + 2]
                    for o in range(3):
                        at_ = [ot * o + st * t for t in range(3)]
                        out = line([u[t] for t in at_], hp, hm, v2, ahead, behind)
                        for t in range(3):
                            acc[at_[t]] = acc[at_[t]] + out[t]
                for n in range(9):
                    dst[9 * a + n, q] = acc[n]
            return carry

        if nx <= 4:
            for q in range(nx):
                block(q, 0)
        else:
            lax.fori_loop(0, nx, block, 0)

    def powers(P, C, F, nx, wrap, first, last):
        def one(k, carry):
            rate(P.at[k], P.at[k + 1], C, F, nx, wrap)
            return carry

        lax.fori_loop(first, last, one, 0)

    def same(t):
        return t

    def half_turn(t):
        return pltpu.roll(t, HALF, 1)

    taylor = np.polynomial.polynomial.polypow([1.0, 1.0, 0.5], SUBSTEPS)

    def finish_field():
        U[...] = jnp.zeros_like(U)
        dt = DT[...]
        weight, power = [], None
        for k in range(1, 2 * SUBSTEPS + 1):
            power = dt if power is None else power * dt
            weight.append(float(taylor[k]) * power)

        def summed(P, m, q):
            out = P[0, m, q]
            for k in range(1, 2 * SUBSTEPS + 1):
                out = out + weight[k - 1] * P[k, m, q]
            return out

        for m in range(27):
            for ix in range(X):
                h, q = ix // NS, ix % NS
                t, s = summed(UM, m, ix), summed(US, m, q)
                o = h * HALF
                left = pltpu.roll(s, (Z - o - 2 * W2) % Z, 1)
                right = pltpu.roll(s, (Z - W2 - o) % Z, 1)
                t = jnp.where(lanes < EDGE, left, jnp.where(lanes >= Z - EDGE, right, t))
                U[m, ix * Y : ix * Y + Y, :] = (1.0 / scale[m]) * t[0:Y]

    def yz_of(src):
        def yz(i, carry):
            for c in range(3):
                yv, yd = [], []
                for k in range(4):
                    sv = sd = None
                    for j in range(NY + 1):
                        x = src[c, i, k, j : j + 1, :]
                        tv, td = tab[oTV + j] * x, tab[oTD + j] * x
                        sv = tv if sv is None else sv + tv
                        sd = td if sd is None else sd + td
                    yv.append(sv)
                    yd.append(sd)
                for r in range(4):
                    A[0, c, i, r] = sum(float(value[r, k]) * yv[k] for k in range(4))
                    A[1, c, i, r] = sum(float(value[r, k]) * yd[k] for k in range(4))
                    A[2, c, i, r] = sum(float(slope[r, k]) * yv[k] for k in range(4))
            return carry

        lax.fori_loop(0, NX + 1, yz, 0)

    def slope_at(ix, p, r, c, d):
        tb = slope if d == 0 else value
        return sum(float(tb[p, m]) * A[d, c, 3 * ix + m, r] for m in range(4))

    def jacobians(t):
        ix, r = t // 4, t % 4
        for p in range(4):
            for c in range(3):
                for d in range(3):
                    jac = slope_at(ix, p, r, c, d)
                    J[d, c, ix, p, r] = jac + 1.0 if c == d else jac

    for cp in loads[:2]:
        cp.wait()
    pl.semaphore_wait(barrier, total)
    for cp in core_copies(0):
        cp.start()
    for ry in range(1, GY):
        plane_copy(ry).start()
    speed = None
    for ix in range(X):
        here = jnp.abs(GU[0, 0, 27, ix]) + jnp.abs(GU[0, 0, 28, ix]) + jnp.abs(GU[0, 0, 29, ix])
        speed = here if speed is None else jnp.maximum(speed, here)
    ROWS[0, 0] = jnp.broadcast_to(jnp.max(speed, axis=0, keepdims=True), (2, Z))
    rows_start(0, 0)
    pack_edges()
    for cp in edge_copies():
        cp.start()
    loads[2].wait()
    unweave()
    rim_pack()
    rim_column().start()
    for cp in rim_copies():
        cp.start()
    loads[3].wait()
    for cp in edge_copies():
        cp.wait_recv()
    for cp in edge_plane_copies():
        cp.start()
    for ry in range(1, GY):
        plane_copy(ry).wait_recv()
        for cp in core_copies(ry):
            cp.start()
    rows_relay(0)
    rim_column().wait_recv()
    for cp in rim_relays():
        cp.start()
    for cp in rim_copies():
        cp.wait()
    rim_unpack()
    yz_of(N)
    for ry in range(GY):
        for cp in core_copies(ry):
            cp.wait_recv()
    assemble()
    strip_own()
    coefficients(VM, CM, XG, same)
    for cp in edge_plane_copies():
        cp.wait_recv()
    for cp in edge_core_copies():
        cp.start()
    powers(UM, CM, FM, XG, same, 0, 2 * SUBSTEPS)
    for cp in rim_relays():
        cp.wait_recv()
    rim_last()

    def all_jacobians(t, carry):
        jacobians(t)
        return carry

    lax.fori_loop(0, 4 * X, all_jacobians, 0)
    for cp in edge_core_copies():
        cp.wait_recv()
    strip_halo()
    coefficients(VS, CS, NS, half_turn)
    powers(US, CS, FT, NS, half_turn, 0, 2 * SUBSTEPS)
    rows_finish(0)
    fastest = functools.reduce(jnp.maximum, [ROWS[0, n] for n in range(devices)])
    fastest = jnp.max(fastest, axis=(0, 1), keepdims=True)
    DT[...] = jnp.broadcast_to(courant / jnp.maximum(fastest, 0.25), (YG, Z))
    finish_field()
    def size_of(ix, carry):
        mid = {}
        for a in range(3):
            for r in range(4):
                mid[a, r] = None
            for c in range(3):
                t = None
                for b in range(3):
                    for e in range(Y):
                        term = tab[oL + b * Y + e] * U[a * 9 + b * 3 + c, pl.ds(ix * Y + e, 1), :]
                        t = term if t is None else t + term
                for r in range(4):
                    term = float(legendre[r, c]) * t
                    mid[a, r] = term if mid[a, r] is None else mid[a, r] + term
        for p in range(4):
            for r in range(4):
                s = sum(float(legendre[p, a]) * mid[a, r] for a in range(3))
                SIZ[ix, p, r] = jnp.exp(theta_size * s)
        return carry

    lax.fori_loop(0, X, size_of, 0)

    wrow = tab[oW]
    pairs = [(d, e) for d in range(3) for e in range(d, 3)]

    def dot3(p, q, d, e):
        return p[0][d] * q[0][e] + p[1][d] * q[1][e] + p[2][d] * q[2][e]

    def gauss_weight(r):
        return jnp.where((r == 0) | (r == 3), float(weights[0]), float(weights[1]))

    def gauss(t, esum):
        ix, r = t // 4, t % 4
        for p in range(4):
            size = SIZ[ix, p, r]
            inv = 1.0 / size
            M = [[J[d, c, ix, p, r] * inv for d in range(3)] for c in range(3)]
            D = [[None] * 3 for _ in range(3)]
            metric = None
            for d, e in pairs:
                dev = dot3(M, M, d, e)
                if d == e:
                    dev = dev - 1.0
                D[d][e] = D[e][d] = dev
                sq = dev * dev if d == e else 2.0 * (dev * dev)
                metric = sq if metric is None else metric + sq
            w = wrow * (gauss_weight(r) * float(weights[p]))
            size2 = size * size
            esum = esum + w * (size2 * size) * metric
            scale = (4.0 * w) * size2
            for c in range(3):
                for d in range(3):
                    g = M[c][0] * D[0][d] + M[c][1] * D[1][d] + M[c][2] * D[2][d]
                    G[d, c, ix, p, r] = scale * g
        return esum

    zero = jnp.zeros((ROWS_Y, Z), f32)
    esum = lax.fori_loop(0, 4 * X, gauss, zero)

    def back_c(c, carry):
        for i in range(NX + 1):
            bv = [None] * 4
            bd = [None] * 4
            for r in range(4):
                ga = []
                for d in range(3):
                    tb = slope if d == 0 else value
                    acc = None
                    for ix in range(X):
                        m = i - 3 * ix
                        if 0 <= m <= 3:
                            for p in range(4):
                                term = float(tb[p, m]) * G[d, c, ix, p, r]
                                acc = term if acc is None else acc + term
                    ga.append(acc)
                for k in range(4):
                    tv = float(value[r, k]) * ga[0] + float(slope[r, k]) * ga[2]
                    td = float(value[r, k]) * ga[1]
                    bv[k] = tv if bv[k] is None else bv[k] + tv
                    bd[k] = td if bd[k] is None else bd[k] + td
            for k in range(4):
                B[0, i, k] = bv[k]
                B[1, i, k] = bd[k]
        for i in range(NX + 1):
            for k in range(4):
                acc = None
                for s in range(ROWS_Y):
                    term = tab[oGV + s] * B[0, i, k, s : s + 1, :] + tab[oGD + s] * B[1, i, k, s : s + 1, :]
                    acc = term if acc is None else acc + term
                GN[c, i, k] = acc
        return carry

    lax.fori_loop(0, 3, back_c, 0)

    def row_of(column_of):
        out = zero
        for c in range(3):
            out = jnp.where(lane == c * ROWS_Y + row, column_of(c), out)
        return jnp.sum(out, axis=0, keepdims=True)

    far, near = zero, zero
    for c in range(3):
        for i in range(NX + 1):
            here = lane == c * (NX + 1) + i
            far = jnp.where(here, GN[c, i, 3][:, Z - 1 : Z], far)
            near = jnp.where(here, GN[c, i, 0][:, 0:1], near)
    FZS[0] = far
    FZS[1] = near
    for zs_, (k, at_) in enumerate(((3, Z - 1), (0, 0))):
        for xs_, i in enumerate((NX, 0)):
            FES[zs_, xs_] = row_of(lambda c: GN[c, i, k][:, at_ : at_ + 1])
        for ys_, j in enumerate((NY, 0)):
            FES[zs_, 2 + ys_] = FZS[zs_][j : j + 1]
    for c in range(3):
        for i in range(NX + 1):
            GN[c, i, 0] = GN[c, i, 0] + jnp.where(lane == 0, 0.0, pltpu.roll(GN[c, i, 3], 1, 1))
            for k in range(4):
                FYS[0, c, i, k : k + 1, :] = GN[c, i, k, NY : NY + 1, :]
                FYS[1, c, i, k : k + 1, :] = GN[c, i, k, 0:1, :]
    ways = (1, -1)

    def fold_copies():
        out = []

        def add(src, dst, move):
            n = len(out)
            out.append(remote(src, dst, fs.at[n], fr.at[n], move))

        for zs_ in range(2):
            for xs_ in range(2):
                for ys_ in range(2):
                    add(FES.at[zs_, xs_], FER.at[zs_, 4 + 2 * xs_ + ys_], (ways[xs_], ways[ys_], ways[zs_]))
            for ys_ in range(2):
                add(FES.at[zs_, 2 + ys_], FER.at[zs_, 2 + ys_], (0, ways[ys_], ways[zs_]))
            for xs_ in range(2):
                add(FES.at[zs_, xs_], FER.at[zs_, xs_], (ways[xs_], 0, ways[zs_]))
            add(FZS.at[zs_], FZR.at[zs_], (0, 0, ways[zs_]))
        for ys_ in range(2):
            for xs_ in range(2):
                add(FYS.at[ys_, :, (NX, 0)[xs_]], FXYR.at[xs_, ys_], (ways[xs_], ways[ys_], 0))
            add(FYS.at[ys_], FYR.at[ys_], (0, ways[ys_], 0))
        for xs_ in range(2):
            add(GN.at[:, (NX, 0)[xs_]], FXR.at[xs_], (ways[xs_], 0, 0))
        return out

    for cp in fold_copies():
        cp.start()
    for cp in fold_copies():
        cp.wait()

    lane1, row_j = lane[0:1], lane[0:1] % ROWS_Y
    planes = []
    for zs_ in range(2):
        p = FZR[zs_]
        p = p + jnp.where(row == 0, FER[zs_, 2], 0.0) + jnp.where(row == NY, FER[zs_, 3], 0.0)
        for xs_, i in enumerate((0, NX)):
            edge = FER[zs_, xs_]
            edge = edge + jnp.where(row_j == 0, pltpu.roll(FER[zs_, 4 + 2 * xs_], Z - NY, 1), 0.0)
            edge = edge + jnp.where(row_j == NY, pltpu.roll(FER[zs_, 5 + 2 * xs_], NY, 1), 0.0)
            for c in range(3):
                col = jnp.sum(jnp.where(lane == c * ROWS_Y + row, edge, 0.0), axis=1, keepdims=True)
                p = p + jnp.where(lane == c * (NX + 1) + i, col, 0.0)
        planes.append(p)
    for c in range(3):
        for k in range(4):
            for xs_, i in enumerate((0, NX)):
                GN[c, i, k] = GN[c, i, k] + FXR[xs_, c, k]
                for ys_, j in enumerate((0, NY)):
                    GN[c, i, k, j : j + 1, :] = GN[c, i, k, j : j + 1, :] + FXYR[xs_, ys_, c, k : k + 1, :]
            for i in range(NX + 1):
                for ys_, j in enumerate((0, NY)):
                    GN[c, i, k, j : j + 1, :] = GN[c, i, k, j : j + 1, :] + FYR[ys_, c, i, k : k + 1, :]
        for i in range(NX + 1):
            n = c * (NX + 1) + i
            full = GN[c, i, 0] + jnp.where(lane == 0, planes[0][:, n : n + 1], 0.0)
            GN[c, i, 0] = full
            GN[c, i, 3] = jnp.where(lane == Z - 1, GN[c, i, 3] + planes[1][:, n : n + 1], pltpu.roll(full, Z - 1, 1))
    ssum = zero
    for c in range(3):
        for i in range(NX):
            for k in range(3):
                g = GN[c, i, k]
                ssum = ssum + g * g
    ssum = jnp.where(row < NY, ssum, 0.0)
    elements = float(EL * Z * devices)
    entries = 81.0 * elements
    mine = jnp.sum(ssum, axis=(0, 1), keepdims=True)
    bound = trial_step / jnp.sqrt(1.0 + mine / entries)
    bound = jnp.broadcast_to(bound, (ROWS_Y, Z))
    yz_of(GN)

    def trial(t, sums):
        ix, r = t // 4, t % 4
        s2, s3, s4 = sums
        for p in range(4):
            size = SIZ[ix, p, r]
            inv = 1.0 / size
            move = -(inv * bound)
            M = [[J[d, c, ix, p, r] * inv for d in range(3)] for c in range(3)]
            K = [[slope_at(ix, p, r, c, d) * move for d in range(3)] for c in range(3)]
            w = wrow * (gauss_weight(r) * float(weights[p])) * (size * size * size)
            q = [None] * 3
            for d, e in pairs:
                d0 = dot3(M, M, d, e)
                d2 = dot3(K, K, d, e)
                if d == e:
                    d0 = d0 - 1.0
                    d1 = 2.0 * dot3(M, K, d, d)
                else:
                    d1 = dot3(M, K, d, e) + dot3(K, M, d, e)
                terms = [d1 * d1 + 2.0 * (d0 * d2), 2.0 * (d1 * d2), d2 * d2]
                for n in range(3):
                    term = terms[n] if d == e else 2.0 * terms[n]
                    q[n] = term if q[n] is None else q[n] + term
            s2, s3, s4 = s2 + w * q[0], s3 + w * q[1], s4 + w * q[2]
        return s2, s3, s4

    sums = lax.fori_loop(0, 4 * X, trial, (zero,) * 3)
    block = zero
    for n, part in enumerate((esum, ssum) + tuple(sums)):
        block = jnp.where(row == n, jnp.sum(part, axis=0, keepdims=True), block)
    column = jnp.sum(block, axis=1, keepdims=True)
    ROWS[1, 0, 0:1] = jnp.sum(jnp.where(lane == row, column, 0.0), axis=0, keepdims=True)
    ROWS[1, 0, 1:2] = 1.0 / bound[0:1]
    rows_start(1, 0)
    for c in range(3):
        for k in range(3):
            slab[c * NX : (c + 1) * NX, :, k * Z : (k + 1) * Z] = GN[c, 0:NX, k]
    woven = lax.dot_general(
        slab[...].reshape(3 * NX * ROWS_Y, 3 * Z), perm[...], (((1,), (1,)), ((), ())),
        precision=lax.Precision.HIGHEST, preferred_element_type=f32,
    ).reshape(3, NX, ROWS_Y, 3 * Z)
    grad[...] = woven[:, :, 0:NY, :]
    for ix in range(X):
        adv[:, ix] = U[:, ix * Y : ix * Y + Y, :]
    rows_relay(1)
    rows_finish(1)
    every = [ROWS[1, n] for n in range(devices)]
    l1 = lax.broadcasted_iota(jnp.int32, (1, Z), 1)

    def lane_sum(x, n):
        return jnp.sum(jnp.where(l1 == n, x, 0.0), axis=1, keepdims=True)

    sums = sum(x[0:1] for x in every)
    etot, stot = lane_sum(sums, 0), lane_sum(sums, 1)
    step = trial_step / jnp.sqrt(1.0 + stot / entries)
    higher = jnp.zeros((1, Z), f32)
    for x in every:
        h = step * x[1:2]
        h2 = h * h
        power = jnp.where(l1 == 2, h2, jnp.where(l1 == 3, h2 * h, h2 * h2))
        higher = higher + x[0:1] * power
    higher = jnp.sum(jnp.where((l1 >= 2) & (l1 < 5), higher, 0.0), axis=1, keepdims=True)
    ttot = (etot - step * stot) + higher
    for ry in range(GY):
        if ry:
            plane_copy(ry).wait_send()
        for cp in core_copies(ry):
            cp.wait_send()
    for cp in edge_copies() + edge_plane_copies() + edge_core_copies() + [rim_column()] + rim_relays():
        cp.wait_send()
    rows_sent(0)
    rows_sent(1)
    checks[...] = jnp.where(
        l1 == 0, etot / elements, jnp.where(l1 == 1, stot / entries, ttot / elements)
    )


def publish(adv, grad, checks, adv_out, grad_out, checks_out, sem):
    copies = [
        pltpu.make_async_copy(grad, grad_out, sem.at[0]),
        pltpu.make_async_copy(adv, adv_out, sem.at[1]),
    ]
    for cp in copies:
        cp.start()
    row = checks[...]
    lane = lax.broadcasted_iota(jnp.int32, row.shape, 1)
    for n in range(3):
        checks_out[n] = jnp.sum(jnp.where(lane == n, row, 0.0))
    for cp in copies:
        cp.wait()


def solution(mesh):
    sizes = tuple(mesh.shape[a] for a in AXES)

    def on_device(displacement, size_field_modes, velocity):
        modes, X, Y, Z = size_field_modes.shape
        assert Y == 2 and displacement.shape == (3, 3 * X, 3 * Y, 3 * Z)
        R, NX, NY = 4 * Y, 3 * X, 3 * Y
        tab = jnp.asarray(row_tables(Y, Z))
        devices = sizes[0] * sizes[1] * sizes[2]
        GX, GY = sizes[0], sizes[1]
        XG, YG, NS = GX * X, GY * Y, GX * X // 2
        packs = -(-30 * X // (Z // (2 * SUBSTEPS)))
        assert YG == 8 and XG % 2 == 0 and min(sizes) > 1
        vm = lambda *shape: pltpu.VMEM(shape, jnp.float32)
        dma = lambda *shape: pltpu.SemaphoreType.DMA(shape)
        spec = pl.BlockSpec(memory_space=pltpu.VMEM)
        adv, grad, checks = pl.pallas_call(
            functools.partial(kernel, sizes, X, Y, Z),
            out_shape=(
                pltpu.VMEM(size_field_modes.shape, jnp.float32),
                pltpu.VMEM(displacement.shape, jnp.float32),
                pltpu.VMEM((1, Z), jnp.float32),
            ),
            in_specs=[pl.BlockSpec(memory_space=pl.ANY)] * 4,
            out_specs=(spec,) * 3,
            scratch_shapes=[
                vm(3, NX, NY, 3 * Z), vm(*tab.shape), vm(GX, GY, 30, X, Y, Z), vm(2, packs, Y, Z), vm(GX, GY, 2, packs, Y, Z), vm(GX, 2, packs, YG, Z),
                vm(2 * SUBSTEPS + 1, 27, XG, YG, Z), vm(3, XG, YG, Z), vm(XG, 9, YG, Z), vm(XG + 1, 9, YG, Z),
                vm(2 * SUBSTEPS + 1, 27, NS, YG, Z), vm(3, NS, YG, Z), vm(NS, 9, YG, Z), vm(NS + 1, 9, YG, Z),
                vm(3 * Z, 3 * Z), vm(3 * NX, R, 3 * Z), vm(27, R, Z),
                vm(2, devices, 2, Z),
                vm(3, NX + 1, 4, R, Z), vm(3, NX + 1, 4, R, Z),
                vm(3, 3, NX + 1, 4, R, Z), vm(3, 3, X, 4, 4, R, Z), vm(3, 3, X, 4, 4, R, Z), vm(2, NX + 1, 4, R, Z), vm(X, 4, 4, R, Z), vm(R, Z),
                vm(3, 3, R, Z), vm(3, NX, 3, Z), vm(3, NX, 3, Z), vm(3, 3, Z), vm(R, Z), vm(4, R, Z),
                vm(2, 3, 4, R, Z), vm(2, 3, NX + 1, 4, Z), vm(2, 3, NX + 1, 4, Z), vm(2, 2, 3, 4, Z), vm(2, R, Z), vm(2, R, Z), vm(2, 4, 1, Z), vm(2, 8, 1, Z),
                dma(4), dma(GY), dma(GY), dma(GX, GY), dma(GX, GY), dma(2, GY), dma(2, GY), dma(GX), dma(GX), dma(2, 2), dma(2, 2), dma(7), dma(7), dma(26), dma(26),
            ],
            compiler_params=pltpu.CompilerParams(collective_id=0, has_side_effects=True),
        )(displacement, size_field_modes, velocity, tab)
        return tuple(
            pl.pallas_call(
                publish,
                out_shape=(
                    jax.ShapeDtypeStruct(size_field_modes.shape, jnp.float32),
                    jax.ShapeDtypeStruct(displacement.shape, jnp.float32),
                    jax.ShapeDtypeStruct((3,), jnp.float32),
                ),
                in_specs=[spec] * 3,
                out_specs=(pl.BlockSpec(memory_space=pl.ANY),) * 2 + (pl.BlockSpec(memory_space=pltpu.SMEM),),
                scratch_shapes=[dma(2)],
            )(*(pltpu.with_memory_space_constraint(a, pltpu.VMEM) for a in (adv, grad, checks)))
        )

    return jax.shard_map(
        on_device,
        mesh=mesh,
        in_specs=(P(None, "gx", "gy", "gz"),) * 3,
        out_specs=(P(None, "gx", "gy", "gz"), P(None, "gx", "gy", "gz"), P()),
        check_vma=False,
    )
```

```python
import functools

import jax
import jax.numpy as jnp
import numpy as np
from jax import lax
from jax.experimental import pallas as pl
from jax.experimental.pallas import tpu as pltpu
from jax.sharding import PartitionSpec as P

SUBSTEPS = 4
MESH = pl.DeviceIdType.MESH
AXES = ("gx", "gy", "gz")

plus_values = (0.7071067811865476, 1.224744871391589, 1.5811388300841898)
g10 = 1.7320508075688772
g21 = 3.872983346207417
courant = 0.1
theta_size = 0.3
trial_step = 0.05


def tables_1d():
    points = np.array(
        [-0.8611363115940526, -0.3399810435848563, 0.3399810435848563, 0.8611363115940526]
    )
    weights = np.array(
        [0.3478548451374538, 0.6521451548625461, 0.6521451548625461, 0.3478548451374538]
    )
    points = 0.5 * (points + 1.0)
    weights = 0.5 * weights
    nodes = np.array([0.0, 1.0 / 3.0, 2.0 / 3.0, 1.0])
    value = np.zeros((4, 4))
    slope = np.zeros((4, 4))
    for m in range(4):
        others = [nodes[o] for o in range(4) if o != m]
        den = np.prod([nodes[m] - o for o in others])
        for q in range(4):
            g = points[q]
            value[q, m] = np.prod([g - o for o in others]) / den
            slope[q, m] = (
                sum(np.prod([g - others[t] for t in range(3) if t != s]) for s in range(3)) / den
            )
    c = 2.0 * points - 1.0
    legendre = np.stack(
        [
            np.full(4, plus_values[0]),
            plus_values[1] * c,
            plus_values[2] * 0.5 * (3.0 * c**2 - 1.0),
        ],
        axis=1,
    )
    return value, slope, legendre, weights


def row_tables(Y, Z):
    value, slope, legendre, weights = tables_1d()
    rows, nodes = 4 * Y, 3 * Y + 1
    tv = np.zeros((rows, rows))
    td = np.zeros((rows, rows))
    for e in range(Y):
        tv[4 * e : 4 * e + 4, 3 * e : 3 * e + 4] = value
        td[4 * e : 4 * e + 4, 3 * e : 3 * e + 4] = slope
    blocks = [tv[:, j] for j in range(nodes)] + [td[:, j] for j in range(nodes)]
    blocks += [tv[s, :] for s in range(rows)] + [td[s, :] for s in range(rows)]
    for b in range(3):
        for e in range(Y):
            col = np.zeros(rows)
            col[4 * e : 4 * e + 4] = legendre[:, b]
            blocks.append(col)
    blocks.append(np.tile(weights, Y))
    stacked = np.stack(blocks).astype(np.float32)
    return np.ascontiguousarray(np.broadcast_to(stacked[:, :, None], stacked.shape + (Z,)))


def kernel(sizes, X, Y, Z, disp_in, modes_in, vel_in, tab_in, adv, grad, checks,
           disp, tab, GU, ZP, ZR, ZA, UM, VM, CM, FM, US, VS, CS, FT,
           perm, slab, U, ROWS, N, GN, A, G, J, B, SIZ, DT,
           NXR, NYS, NYR, NXYR, NZS, NZR, FXR, FYS, FYR, FXYR, FZS, FZR, FES, FER,
           ls, g1s, g1r, g2s, g2r, zs, zr, y2s, y2r, rs, rr, ns, nr, fs, fr):
    value, slope, legendre, weights = tables_1d()
    NX, NY = 3 * X, 3 * Y
    ROWS_Y = 4 * Y
    EL = X * Y
    f32 = jnp.float32
    index = [lax.axis_index(a) for a in AXES]
    lane = lax.broadcasted_iota(jnp.int32, (ROWS_Y, Z), 1)
    row = lax.broadcasted_iota(jnp.int32, (ROWS_Y, Z), 0)
    oTV, oTD, oGV, oGD, oL, oW = 0, NY + 1, 2 * NY + 2, 2 * NY + 2 + ROWS_Y, 2 * NY + 2 + 2 * ROWS_Y, 2 * NY + 2 + 2 * ROWS_Y + 3 * Y

    def at(axis, by):
        n = sizes[axis]
        return {AXES[axis]: lax.rem(index[axis] + (by + n), n)}

    barrier = pltpu.get_barrier_semaphore()
    total = 0
    for a in range(sizes[0]):
        for b in range(sizes[1]):
            for c in range(sizes[2]):
                move = (a, b, c)
                if not any(move) or (c and (a or b)):
                    continue
                target = {}
                for axis in range(3):
                    if move[axis]:
                        target.update(at(axis, move[axis]))
                pl.semaphore_signal(barrier, inc=1, device_id=target, device_id_type=MESH)
                total += 1

    loads = [
        pltpu.make_async_copy(modes_in, GU.at[0, 0, 0:27], ls.at[0]),
        pltpu.make_async_copy(vel_in, GU.at[0, 0, 27:30], ls.at[1]),
        pltpu.make_async_copy(disp_in, disp, ls.at[2]),
        pltpu.make_async_copy(tab_in, tab, ls.at[3]),
    ]
    for cp in loads:
        cp.start()

    def copy(src, dst, ss, sr, axis, by):
        return pltpu.make_async_remote_copy(
            src_ref=src, dst_ref=dst, send_sem=ss, recv_sem=sr,
            device_id=at(axis, by), device_id_type=MESH,
        )

    GX, GY = sizes[0], sizes[1]
    XG, YG, NS, EDGE = GX * X, GY * Y, GX * X // 2, 2 * SUBSTEPS
    HALF, FIELDS, SLOTS = Z // 2, 30, Z // EDGE

    def moved(move):
        target = {}
        for axis in range(3):
            if move[axis] % sizes[axis]:
                target.update(at(axis, move[axis] % sizes[axis] ))
        return target

    def remote(src, dst, ss, sr, move):
        return pltpu.make_async_remote_copy(
            src_ref=src, dst_ref=dst, send_sem=ss, recv_sem=sr,
            device_id=moved(move), device_id_type=MESH,
        )

    def plane_copy(ry):
        return remote(GU.at[0, 0], GU.at[0, ry], g1s.at[ry], g1r.at[ry], (0, -ry, 0))

    def core_copies(ry):
        return [
            remote(GU.at[0, ry], GU.at[rx, ry], g2s.at[rx, ry], g2r.at[rx, ry], (-rx, 0, 0))
            for rx in range(1, GX)
        ]

    def edge_copies():
        return [
            remote(ZP.at[side], ZR.at[0, 0, side], zs.at[side, 0], zr.at[side, 0], (0, 0, 2 * side - 1))
            for side in range(2)
        ]

    def edge_plane_copies():
        return [
            remote(ZR.at[0, 0], ZR.at[0, ry], zs.at[0, ry], zr.at[0, ry], (0, -ry, 0)) for ry in range(1, GY)
        ]

    def edge_core_copies():
        return [
            remote(ZR.at[0], ZR.at[rx], y2s.at[rx], y2r.at[rx], (-rx, 0, 0)) for rx in range(1, GX)
        ]

    slot2 = lax.broadcasted_iota(jnp.int32, (Y, Z), 1) // EDGE
    packs = -(-FIELDS * X // SLOTS)

    def pack_edges():
        acc = [[jnp.zeros((Y, Z), f32) for _ in range(packs)] for _ in range(2)]
        for m in range(FIELDS):
            for ix in range(X):
                t = m * X + ix
                v, p = t // SLOTS, EDGE * (t % SLOTS)
                x = GU[0, 0, m, ix]
                low = pltpu.roll(x, p, 1) if p else x
                high = pltpu.roll(x, (p + EDGE) % Z, 1) if (p + EDGE) % Z else x
                acc[0][v] = jnp.where(slot2 == t % SLOTS, low, acc[0][v])
                acc[1][v] = jnp.where(slot2 == t % SLOTS, high, acc[1][v])
        for side in range(2):
            for v in range(packs):
                ZP[side, v] = acc[side][v]

    def unweave():
        a_i = lax.broadcasted_iota(jnp.int32, (3 * Z, 3 * Z), 0)
        b_i = lax.broadcasted_iota(jnp.int32, (3 * Z, 3 * Z), 1)
        b_k = (b_i >= Z).astype(jnp.int32) + (b_i >= 2 * Z).astype(jnp.int32)
        perm[...] = (a_i == 3 * (b_i - b_k * Z) + b_k).astype(f32)
        slab[...] = jnp.zeros_like(slab)
        for c in range(3):
            for i in range(NX):
                slab[c * NX + i, 0:NY, :] = disp[c, i]
        spread = jnp.dot(
            slab[...].reshape(3 * NX * ROWS_Y, 3 * Z), perm[...],
            precision=lax.Precision.HIGHEST, preferred_element_type=f32,
        ).reshape(3, NX, ROWS_Y, 3 * Z)
        for c in range(3):
            for k in range(3):
                N[c, 0:NX, k] = spread[c, :, :, k * Z : (k + 1) * Z]

    devices = sizes[0] * sizes[1] * sizes[2]
    by_column = [(2,), (0, 1)]
    plans = [by_column, [(0, 1, 2)] if devices <= 64 else by_column]

    def row_stage(r, stage):
        block = 1
        stages = plans[r]
        for axes in stages[:stage]:
            for axis in axes:
                block *= sizes[axis]
        moves = [()]
        for axis in range(3):
            moves = [m + (b,) for m in moves for b in range(sizes[axis] if axis in stages[stage] else 1)]
        src = ROWS.at[r, 0:block]
        copies = [
            remote(src, ROWS.at[r, n * block : (n + 1) * block], rs.at[r, stage], rr.at[r, stage], m)
            for n, m in sorted(enumerate(moves), key=lambda nm: -sum(1 for b in nm[1] if b)) if n
        ]
        rest = ROWS.at[r, block : len(moves) * block]
        return copies, remote(rest, rest, rs.at[r, stage], rr.at[r, stage], moves[1])

    def rows_start(r, stage):
        for cp in row_stage(r, stage)[0]:
            cp.start()

    def rows_relay(r):
        for stage in range(len(plans[r]) - 1):
            row_stage(r, stage)[1].wait_recv()
            rows_start(r, stage + 1)

    def rows_finish(r):
        row_stage(r, len(plans[r]) - 1)[1].wait_recv()

    def rows_sent(r):
        for stage in range(len(plans[r])):
            row_stage(r, stage)[1].wait_send()

    in_lane = lambda n: functools.reduce(jnp.logical_or, [lane == c * (NX + 1) + n for c in range(3)])

    def rim_copies():
        out = [
            remote(N.at[:, 0, 0:3], NXR, ns.at[0], nr.at[0], (-1, 0, 0)),
            remote(NYS, NYR, ns.at[1], nr.at[1], (0, -1, 0)),
            remote(NYS.at[:, 0], NXYR, ns.at[2], nr.at[2], (-1, -1, 0)),
        ]
        return out

    def rim_column():
        return remote(NZS, NZR.at[0], ns.at[3], nr.at[3], (0, 0, -1))

    def rim_relays():
        return [
            remote(NZR.at[0], NZR.at[n], ns.at[3 + n], nr.at[3 + n], move)
            for n, move in ((1, (-1, 0, 0)), (2, (0, -1, 0)), (3, (-1, -1, 0)))
        ]

    def rim_pack():
        packed = jnp.zeros((ROWS_Y, Z), f32)
        for c in range(3):
            for i in range(NX):
                for k in range(3):
                    NYS[c, i, k : k + 1, :] = N[c, i, k, 0:1, :]
                packed = jnp.where(lane == c * (NX + 1) + i, N[c, i, 0][:, 0:1], packed)
        NZS[...] = packed

    def rim_unpack():
        for c in range(3):
            for k in range(3):
                N[c, NX, k] = NXR[c, k]
                N[c, NX, k, NY : NY + 1, :] = NXYR[c, k : k + 1, :]
                for i in range(NX):
                    N[c, i, k, NY : NY + 1, :] = NYR[c, i, k : k + 1, :]
        for c in range(3):
            for i in range(NX + 1):
                N[c, i, 3] = jnp.where(lane == Z - 1, 0.0, pltpu.roll(N[c, i, 0], Z - 1, 1))

    def rim_last():
        last = in_lane(NX)
        packed = jnp.where(last, pltpu.roll(NZR[1], NX, 1), NZR[0])
        below = jnp.where(last[0:1], pltpu.roll(NZR[3], NX, 1)[0:1], NZR[2][0:1])
        rows = [packed[j : j + 1] for j in range(NY)] + [below]
        pv = sum(tab[oTV + j] * rows[j] for j in range(NY + 1))
        pd = sum(tab[oTD + j] * rows[j] for j in range(NY + 1))
        end = lane == Z - 1
        for c in range(3):
            for i in range(NX + 1):
                n = c * (NX + 1) + i
                mv = jnp.where(end, pv[:, n : n + 1], 0.0)
                md = jnp.where(end, pd[:, n : n + 1], 0.0)
                for r in range(4):
                    A[0, c, i, r] = A[0, c, i, r] + float(value[r, 3]) * mv
                    A[1, c, i, r] = A[1, c, i, r] + float(value[r, 3]) * md
                    A[2, c, i, r] = A[2, c, i, r] + float(slope[r, 3]) * mv

    scale = [plus_values[m // 9] * plus_values[m // 3 % 3] * plus_values[m % 3] for m in range(27)]

    def assemble():
        def plane(x, carry):
            rx, ix = x // X, x % X
            for ry in range(GY):
                for m in range(FIELDS):
                    v = GU[rx, ry, m, ix]
                    if m < 27:
                        UM[0, m, x, ry * Y : ry * Y + Y, :] = scale[m] * v
                    else:
                        VM[m - 27, x, ry * Y : ry * Y + Y, :] = v
            return carry

        lax.fori_loop(0, XG, plane, 0)

    lanes = lax.broadcasted_iota(jnp.int32, (YG, Z), 1)
    W2, W3 = 2 * EDGE, 3 * EDGE

    def within(lo, hi):
        return (lanes >= lo) & (lanes < hi)

    def strip_own():
        def one(q, carry):
            for m in range(FIELDS):
                out = jnp.zeros((YG, Z), f32)
                for h in range(2):
                    t = UM[0, m, q + h * NS] if m < 27 else VM[m - 27, q + h * NS]
                    o = h * HALF
                    out = jnp.where(within(o, o + W2), pltpu.roll(t, o + W2, 1), out)
                    out = jnp.where(within(o + 2 * W2, o + 3 * W2), pltpu.roll(t, o + 2 * W2, 1), out)
                if m < 27:
                    US[0, m, q] = out
                else:
                    VS[m - 27, q] = out
            return carry

        lax.fori_loop(0, NS, one, 0)

    def strip_halo():
        for rx in range(GX):
            for ry in range(GY):
                ZA[rx, :, :, ry * Y : ry * Y + Y, :] = ZR[rx, ry]
        for q in range(NS):
            for m in range(FIELDS):
                out = US[0, m, q] if m < 27 else VS[m - 27, q]
                for h in range(2):
                    x = q + h * NS
                    rx, ix = x // X, x % X
                    t = m * X + ix
                    v, p = t // SLOTS, EDGE * (t % SLOTS)
                    for side in range(2):
                        o = h * HALF + W2 + side * EDGE
                        piece = ZA[rx, side, v]
                        by = (o - p) % Z
                        piece = pltpu.roll(piece, by, 1) if by else piece
                        if m < 27:
                            piece = scale[m] * piece
                        out = jnp.where(within(o, o + EDGE), piece, out)
                if m < 27:
                    US[0, m, q] = out
                else:
                    VS[m - 27, q] = out

    def ynext(t):
        return pltpu.roll(t, YG - 1, 0)

    def yprev(t):
        return pltpu.roll(t, 1, 0)

    def znext(t):
        return pltpu.roll(t, Z - 1, 1)

    def zprev(t):
        return pltpu.roll(t, 1, 1)

    def coefficients(V, C, nx, wrap):
        for q in range(nx):
            nxt = V[0, q + 1] if q < nx - 1 else wrap(V[0, 0])
            for d in range(3):
                v = V[d, q]
                ahead = nxt if d == 0 else ynext(v) if d == 1 else znext(v)
                face = 0.5 * (v + ahead)
                C[q, 3 * d] = jnp.maximum(face, 0.0)
                C[q, 3 * d + 1] = jnp.minimum(face, 0.0)
                C[q, 3 * d + 2] = 2.0 * v

    def line(u, hp, hm, v2, ahead, behind):
        e = u[0] + u[2]
        up = hp * (e + u[1]) + hm * ahead(e - u[1])
        low = behind(up)
        diff = low - up
        return diff, 3.0 * (v2 * u[0] - (low + up)), 5.0 * (v2 * u[1] + diff)

    def rate(src, dst, C, F, nx, wrap):
        for n in range(9):
            tp, tm = [], []
            for q in range(nx):
                u0, u1, u2 = src[n, q], src[9 + n, q], src[18 + n, q]
                e = u0 + u2
                tp.append(e + u1)
                tm.append(e - u1)
            for q in range(nx):
                nxt = tm[q + 1] if q < nx - 1 else wrap(tm[0])
                f = C[q, 0] * tp[q] + C[q, 1] * nxt
                F[q + 1, n] = f
                if q == nx - 1:
                    F[0, n] = wrap(f)

        def block(q, carry):
            vx = C[q, 2]
            for a in range(3):
                u = [src[9 * a + n, q] for n in range(9)]
                acc = []
                for n in range(9):
                    up, low = F[q + 1, n], F[q, n]
                    if a == 0:
                        acc.append(low - up)
                    elif a == 1:
                        acc.append(3.0 * (vx * src[n, q] - (low + up)))
                    else:
                        acc.append(5.0 * (vx * src[9 + n, q] + (low - up)))
                for d, st, ot, ahead, behind in ((1, 3, 1, ynext, yprev), (2, 1, 3, znext, zprev)):
                    hp, hm, v2 = C[q, 3 * d], C[q, 3 * d + 1], C[q, 3 * d + 2]
                    for o in range(3):
                        at_ = [ot * o + st * t for t in range(3)]
                        out = line([u[t] for t in at_], hp, hm, v2, ahead, behind)
                        for t in range(3):
                            acc[at_[t]] = acc[at_[t]] + out[t]
                for n in range(9):
                    dst[9 * a + n, q] = acc[n]
            return carry

        if nx <= 4:
            for q in range(nx):
                block(q, 0)
        else:
            lax.fori_loop(0, nx, block, 0)

    def powers(P, C, F, nx, wrap, first, last):
        def one(k, carry):
            rate(P.at[k], P.at[k + 1], C, F, nx, wrap)
            return carry

        lax.fori_loop(first, last, one, 0)

    def same(t):
        return t

    def half_turn(t):
        return pltpu.roll(t, HALF, 1)

    taylor = np.polynomial.polynomial.polypow([1.0, 1.0, 0.5], SUBSTEPS)

    def finish_field():
        U[...] = jnp.zeros_like(U)
        dt = DT[...]
        weight, power = [], None
        for k in range(1, 2 * SUBSTEPS + 1):
            power = dt if power is None else power * dt
            weight.append(float(taylor[k]) * power)

        def summed(P, m, q):
            out = P[0, m, q]
            for k in range(1, 2 * SUBSTEPS + 1):
                out = out + weight[k - 1] * P[k, m, q]
            return out

        for m in range(27):
            for ix in range(X):
                h, q = ix // NS, ix % NS
                t, s = summed(UM, m, ix), summed(US, m, q)
                o = h * HALF
                left = pltpu.roll(s, (Z - o - 2 * W2) % Z, 1)
                right = pltpu.roll(s, (Z - W2 - o) % Z, 1)
                t = jnp.where(lanes < EDGE, left, jnp.where(lanes >= Z - EDGE, right, t))
                U[m, ix * Y : ix * Y + Y, :] = (1.0 / scale[m]) * t[0:Y]

    def yz_of(src):
        def yz(i, carry):
            for c in range(3):
                yv, yd = [], []
                for k in range(4):
                    sv = sd = None
                    for j in range(NY + 1):
                        x = src[c, i, k, j : j + 1, :]
                        tv, td = tab[oTV + j] * x, tab[oTD + j] * x
                        sv = tv if sv is None else sv + tv
                        sd = td if sd is None else sd + td
                    yv.append(sv)
                    yd.append(sd)
                for r in range(4):
                    A[0, c, i, r] = sum(float(value[r, k]) * yv[k] for k in range(4))
                    A[1, c, i, r] = sum(float(value[r, k]) * yd[k] for k in range(4))
                    A[2, c, i, r] = sum(float(slope[r, k]) * yv[k] for k in range(4))
            return carry

        lax.fori_loop(0, NX + 1, yz, 0)

    def slopes_at(ix, r, c, d):
        tb = slope if d == 0 else value
        x = [A[d, c, 3 * ix + m, r] for m in range(4)]
        e0, e1, o0, o1 = x[0] + x[3], x[1] + x[2], x[0] - x[3], x[1] - x[2]
        even = lambda p, m: float(0.5 * (tb[p, m] + tb[p, 3 - m]))
        odd = lambda p, m: float(0.5 * (tb[p, m] - tb[p, 3 - m]))
        out = [None] * 4
        for p in range(2):
            a = even(p, 0) * e0 + even(p, 1) * e1
            b = odd(p, 0) * o0 + odd(p, 1) * o1
            out[p] = a + b
            out[3 - p] = b - a if d == 0 else a - b
        return out

    def jacobians(t):
        ix, r = t // 4, t % 4
        for c in range(3):
            for d in range(3):
                jac = slopes_at(ix, r, c, d)
                for p in range(4):
                    J[d, c, ix, p, r] = jac[p] + 1.0 if c == d else jac[p]

    for cp in loads[:2]:
        cp.wait()
    pl.semaphore_wait(barrier, total)
    for cp in core_copies(0):
        cp.start()
    for ry in range(1, GY):
        plane_copy(ry).start()
    speed = None
    for ix in range(X):
        here = jnp.abs(GU[0, 0, 27, ix]) + jnp.abs(GU[0, 0, 28, ix]) + jnp.abs(GU[0, 0, 29, ix])
        speed = here if speed is None else jnp.maximum(speed, here)
    ROWS[0, 0] = jnp.max(speed, axis=0, keepdims=True)
    rows_start(0, 0)
    pack_edges()
    for cp in edge_copies():
        cp.start()
    loads[2].wait()
    unweave()
    rim_pack()
    rim_column().start()
    for cp in rim_copies():
        cp.start()
    loads[3].wait()
    for cp in edge_copies():
        cp.wait_recv()
    for cp in edge_plane_copies():
        cp.start()
    for ry in range(1, GY):
        plane_copy(ry).wait_recv()
        for cp in core_copies(ry):
            cp.start()
    rows_relay(0)
    rim_column().wait_recv()
    for cp in rim_relays():
        cp.start()
    for cp in rim_copies():
        cp.wait()
    rim_unpack()
    yz_of(N)
    for ry in range(GY):
        for cp in core_copies(ry):
            cp.wait_recv()
    assemble()
    strip_own()
    coefficients(VM, CM, XG, same)
    for cp in edge_plane_copies():
        cp.wait_recv()
    for cp in edge_core_copies():
        cp.start()
    powers(UM, CM, FM, XG, same, 0, 2 * SUBSTEPS)
    for cp in rim_relays():
        cp.wait_recv()
    rim_last()

    def all_jacobians(t, carry):
        jacobians(t)
        return carry

    lax.fori_loop(0, 4 * X, all_jacobians, 0)
    for cp in edge_core_copies():
        cp.wait_recv()
    strip_halo()
    coefficients(VS, CS, NS, half_turn)
    powers(US, CS, FT, NS, half_turn, 0, 2 * SUBSTEPS)
    rows_finish(0)
    fastest = functools.reduce(jnp.maximum, [ROWS[0, n] for n in range(devices)])
    fastest = jnp.max(fastest, axis=(0, 1), keepdims=True)
    DT[...] = jnp.broadcast_to(courant / jnp.maximum(fastest, 0.25), (YG, Z))
    finish_field()
    def size_of(ix, carry):
        mid = {}
        for a in range(3):
            for r in range(4):
                mid[a, r] = None
            for c in range(3):
                t = None
                for b in range(3):
                    for e in range(Y):
                        term = tab[oL + b * Y + e] * U[a * 9 + b * 3 + c, pl.ds(ix * Y + e, 1), :]
                        t = term if t is None else t + term
                for r in range(4):
                    term = float(legendre[r, c]) * t
                    mid[a, r] = term if mid[a, r] is None else mid[a, r] + term
        for p in range(4):
            for r in range(4):
                s = sum(float(legendre[p, a]) * mid[a, r] for a in range(3))
                SIZ[ix, p, r] = jnp.exp(theta_size * s)
        return carry

    lax.fori_loop(0, X, size_of, 0)

    wrow = tab[oW]
    pairs = [(d, e) for d in range(3) for e in range(d, 3)]

    def dot3(p, q, d, e):
        return p[0][d] * q[0][e] + p[1][d] * q[1][e] + p[2][d] * q[2][e]

    def gauss_weight(r):
        return jnp.where((r == 0) | (r == 3), float(weights[0]), float(weights[1]))

    def gauss(t, esum):
        ix, r = t // 4, t % 4
        for p in range(4):
            size = SIZ[ix, p, r]
            inv = 1.0 / size
            M = [[J[d, c, ix, p, r] * inv for d in range(3)] for c in range(3)]
            D = [[None] * 3 for _ in range(3)]
            metric = None
            for d, e in pairs:
                dev = dot3(M, M, d, e)
                if d == e:
                    dev = dev - 1.0
                D[d][e] = D[e][d] = dev
                sq = dev * dev if d == e else 2.0 * (dev * dev)
                metric = sq if metric is None else metric + sq
            w = wrow * (gauss_weight(r) * float(weights[p]))
            size2 = size * size
            esum = esum + w * (size2 * size) * metric
            scale = (4.0 * w) * size2
            for c in range(3):
                for d in range(3):
                    g = M[c][0] * D[0][d] + M[c][1] * D[1][d] + M[c][2] * D[2][d]
                    G[d, c, ix, p, r] = scale * g
        return esum

    zero = jnp.zeros((ROWS_Y, Z), f32)
    esum = lax.fori_loop(0, 4 * X, gauss, zero)

    def back_c(c, carry):
        for i in range(NX + 1):
            bv = [None] * 4
            bd = [None] * 4
            for r in range(4):
                ga = []
                for d in range(3):
                    tb = slope if d == 0 else value
                    acc = None
                    for ix in range(X):
                        m = i - 3 * ix
                        if 0 <= m <= 3:
                            for p in range(4):
                                term = float(tb[p, m]) * G[d, c, ix, p, r]
                                acc = term if acc is None else acc + term
                    ga.append(acc)
                for k in range(4):
                    tv = float(value[r, k]) * ga[0] + float(slope[r, k]) * ga[2]
                    td = float(value[r, k]) * ga[1]
                    bv[k] = tv if bv[k] is None else bv[k] + tv
                    bd[k] = td if bd[k] is None else bd[k] + td
            for k in range(4):
                B[0, i, k] = bv[k]
                B[1, i, k] = bd[k]
        for i in range(NX + 1):
            for k in range(4):
                acc = None
                for s in range(ROWS_Y):
                    term = tab[oGV + s] * B[0, i, k, s : s + 1, :] + tab[oGD + s] * B[1, i, k, s : s + 1, :]
                    acc = term if acc is None else acc + term
                GN[c, i, k] = acc
        return carry

    lax.fori_loop(0, 3, back_c, 0)

    def row_of(column_of):
        out = zero
        for c in range(3):
            out = jnp.where(lane == c * ROWS_Y + row, column_of(c), out)
        return jnp.sum(out, axis=0, keepdims=True)

    far, near = zero, zero
    for c in range(3):
        for i in range(NX + 1):
            here = lane == c * (NX + 1) + i
            far = jnp.where(here, GN[c, i, 3][:, Z - 1 : Z], far)
            near = jnp.where(here, GN[c, i, 0][:, 0:1], near)
    FZS[0] = far
    FZS[1] = near
    for zs_, (k, at_) in enumerate(((3, Z - 1), (0, 0))):
        for xs_, i in enumerate((NX, 0)):
            FES[zs_, xs_] = row_of(lambda c: GN[c, i, k][:, at_ : at_ + 1])
        for ys_, j in enumerate((NY, 0)):
            FES[zs_, 2 + ys_] = FZS[zs_][j : j + 1]
    for c in range(3):
        for i in range(NX + 1):
            GN[c, i, 0] = GN[c, i, 0] + jnp.where(lane == 0, 0.0, pltpu.roll(GN[c, i, 3], 1, 1))
            for k in range(4):
                FYS[0, c, i, k : k + 1, :] = GN[c, i, k, NY : NY + 1, :]
                FYS[1, c, i, k : k + 1, :] = GN[c, i, k, 0:1, :]
    ways = (1, -1)

    def fold_copies():
        out = []

        def add(src, dst, move):
            n = len(out)
            out.append(remote(src, dst, fs.at[n], fr.at[n], move))

        for zs_ in range(2):
            for xs_ in range(2):
                for ys_ in range(2):
                    add(FES.at[zs_, xs_], FER.at[zs_, 4 + 2 * xs_ + ys_], (ways[xs_], ways[ys_], ways[zs_]))
            for ys_ in range(2):
                add(FES.at[zs_, 2 + ys_], FER.at[zs_, 2 + ys_], (0, ways[ys_], ways[zs_]))
            for xs_ in range(2):
                add(FES.at[zs_, xs_], FER.at[zs_, xs_], (ways[xs_], 0, ways[zs_]))
            add(FZS.at[zs_], FZR.at[zs_], (0, 0, ways[zs_]))
        for ys_ in range(2):
            for xs_ in range(2):
                add(FYS.at[ys_, :, (NX, 0)[xs_]], FXYR.at[xs_, ys_], (ways[xs_], ways[ys_], 0))
            add(FYS.at[ys_], FYR.at[ys_], (0, ways[ys_], 0))
        for xs_ in range(2):
            add(GN.at[:, (NX, 0)[xs_]], FXR.at[xs_], (ways[xs_], 0, 0))
        return out

    for cp in fold_copies():
        cp.start()
    for cp in fold_copies():
        cp.wait()

    lane1, row_j = lane[0:1], lane[0:1] % ROWS_Y
    planes = []
    for zs_ in range(2):
        p = FZR[zs_]
        p = p + jnp.where(row == 0, FER[zs_, 2], 0.0) + jnp.where(row == NY, FER[zs_, 3], 0.0)
        for xs_, i in enumerate((0, NX)):
            edge = FER[zs_, xs_]
            edge = edge + jnp.where(row_j == 0, pltpu.roll(FER[zs_, 4 + 2 * xs_], Z - NY, 1), 0.0)
            edge = edge + jnp.where(row_j == NY, pltpu.roll(FER[zs_, 5 + 2 * xs_], NY, 1), 0.0)
            for c in range(3):
                col = jnp.sum(jnp.where(lane == c * ROWS_Y + row, edge, 0.0), axis=1, keepdims=True)
                p = p + jnp.where(lane == c * (NX + 1) + i, col, 0.0)
        planes.append(p)
    first_row, last_row = row == 0, row == NY
    ssum = zero
    for c in range(3):
        for i in range(NX + 1):
            n = c * (NX + 1) + i
            out = []
            for k in range(4):
                low, high = FYR[0, c, i, k : k + 1, :], FYR[1, c, i, k : k + 1, :]
                g = GN[c, i, k]
                if i in (0, NX):
                    xs_ = 0 if i == 0 else 1
                    g = g + FXR[xs_, c, k]
                    low = low + FXYR[xs_, 0, c, k : k + 1, :]
                    high = high + FXYR[xs_, 1, c, k : k + 1, :]
                out.append(g + jnp.where(first_row, low, jnp.where(last_row, high, 0.0)))
            out[0] = out[0] + jnp.where(lane == 0, planes[0][:, n : n + 1], 0.0)
            out[3] = jnp.where(lane == Z - 1, out[3] + planes[1][:, n : n + 1], pltpu.roll(out[0], Z - 1, 1))
            for k in range(4):
                GN[c, i, k] = out[k]
                if i < NX and k < 3:
                    ssum = ssum + out[k] * out[k]
    ssum = jnp.where(row < NY, ssum, 0.0)
    elements = float(EL * Z * devices)
    entries = 81.0 * elements
    mine = jnp.sum(ssum, axis=(0, 1), keepdims=True)
    bound = trial_step / jnp.sqrt(1.0 + mine / entries)
    bound = jnp.broadcast_to(bound, (ROWS_Y, Z))
    yz_of(GN)

    def trial(t, sums):
        ix, r = t // 4, t % 4
        s2, s3, s4 = sums
        moves = [[slopes_at(ix, r, c, d) for d in range(3)] for c in range(3)]
        for p in range(4):
            size = SIZ[ix, p, r]
            inv = 1.0 / size
            move = -(inv * bound)
            M = [[J[d, c, ix, p, r] * inv for d in range(3)] for c in range(3)]
            K = [[moves[c][d][p] * move for d in range(3)] for c in range(3)]
            w = wrow * (gauss_weight(r) * float(weights[p])) * (size * size * size)
            q = [[None] * 4, [None] * 4]
            for d, e in pairs:
                d0 = dot3(M, M, d, e)
                d2 = dot3(K, K, d, e)
                if d == e:
                    d0 = d0 - 1.0
                    d1 = 2.0 * dot3(M, K, d, d)
                else:
                    d1 = dot3(M, K, d, e) + dot3(K, M, d, e)
                terms, own = (d1 * d1, d0 * d2, d1 * d2, d2 * d2), q[0 if d == e else 1]
                for n in range(4):
                    own[n] = terms[n] if own[n] is None else own[n] + terms[n]
            full = [q[0][n] + 2.0 * q[1][n] for n in range(4)]
            s2 = s2 + w * (full[0] + 2.0 * full[1])
            s3 = s3 + w * (2.0 * full[2])
            s4 = s4 + w * full[3]
        return s2, s3, s4

    sums = lax.fori_loop(0, 4 * X, trial, (zero,) * 3)
    block = zero
    for n, part in enumerate((esum, ssum) + tuple(sums)):
        block = jnp.where(row == n, jnp.sum(part, axis=0, keepdims=True), block)
    column = jnp.sum(block, axis=1, keepdims=True)
    sent = jnp.sum(jnp.where(lane == row, column, 0.0), axis=0, keepdims=True)
    ROWS[1, 0] = jnp.where(lane[0:1] < HALF, sent, 1.0 / bound[0:1])
    rows_start(1, 0)
    for c in range(3):
        for k in range(3):
            slab[c * NX : (c + 1) * NX, :, k * Z : (k + 1) * Z] = GN[c, 0:NX, k]
    woven = lax.dot_general(
        slab[...].reshape(3 * NX * ROWS_Y, 3 * Z), perm[...], (((1,), (1,)), ((), ())),
        precision=lax.Precision.HIGHEST, preferred_element_type=f32,
    ).reshape(3, NX, ROWS_Y, 3 * Z)
    grad[...] = woven[:, :, 0:NY, :]
    for ix in range(X):
        adv[:, ix] = U[:, ix * Y : ix * Y + Y, :]
    for ry in range(GY):
        if ry:
            plane_copy(ry).wait_send()
        for cp in core_copies(ry):
            cp.wait_send()
    for cp in edge_copies() + edge_plane_copies() + edge_core_copies() + [rim_column()] + rim_relays():
        cp.wait_send()
    rows_sent(0)
    rows_sent(1)
    rows_relay(1)
    rows_finish(1)
    every = [ROWS[1, n] for n in range(devices)]
    l1 = lax.broadcasted_iota(jnp.int32, (1, Z), 1)

    def lane_sum(x, n):
        return jnp.sum(jnp.where(l1 == n, x, 0.0), axis=1, keepdims=True)

    sums = sum(every)
    etot, stot = lane_sum(sums, 0), lane_sum(sums, 1)
    step = trial_step / jnp.sqrt(1.0 + stot / entries)
    higher = jnp.zeros((1, Z), f32)
    for x in every:
        h = step * pltpu.roll(x, HALF, 1)
        h2 = h * h
        power = jnp.where(l1 == 2, h2, jnp.where(l1 == 3, h2 * h, h2 * h2))
        higher = higher + x * power
    higher = jnp.sum(jnp.where((l1 >= 2) & (l1 < 5), higher, 0.0), axis=1, keepdims=True)
    ttot = (etot - step * stot) + higher
    checks[...] = jnp.where(
        l1 == 0, etot / elements, jnp.where(l1 == 1, stot / entries, ttot / elements)
    )


def publish(adv, grad, checks, adv_out, grad_out, checks_out, sem):
    copies = [
        pltpu.make_async_copy(grad, grad_out, sem.at[0]),
        pltpu.make_async_copy(adv, adv_out, sem.at[1]),
    ]
    for cp in copies:
        cp.start()
    row = checks[...]
    lane = lax.broadcasted_iota(jnp.int32, row.shape, 1)
    for n in range(3):
        checks_out[n] = jnp.sum(jnp.where(lane == n, row, 0.0))
    for cp in copies:
        cp.wait()


def solution(mesh):
    sizes = tuple(mesh.shape[a] for a in AXES)

    def on_device(displacement, size_field_modes, velocity):
        modes, X, Y, Z = size_field_modes.shape
        assert Y == 2 and displacement.shape == (3, 3 * X, 3 * Y, 3 * Z)
        R, NX, NY = 4 * Y, 3 * X, 3 * Y
        tab = jnp.asarray(row_tables(Y, Z))
        devices = sizes[0] * sizes[1] * sizes[2]
        GX, GY = sizes[0], sizes[1]
        XG, YG, NS = GX * X, GY * Y, GX * X // 2
        packs = -(-30 * X // (Z // (2 * SUBSTEPS)))
        assert YG == 8 and XG % 2 == 0 and min(sizes) > 1
        vm = lambda *shape: pltpu.VMEM(shape, jnp.float32)
        dma = lambda *shape: pltpu.SemaphoreType.DMA(shape)
        spec = pl.BlockSpec(memory_space=pltpu.VMEM)
        adv, grad, checks = pl.pallas_call(
            functools.partial(kernel, sizes, X, Y, Z),
            out_shape=(
                pltpu.VMEM(size_field_modes.shape, jnp.float32),
                pltpu.VMEM(displacement.shape, jnp.float32),
                pltpu.VMEM((1, Z), jnp.float32),
            ),
            in_specs=[pl.BlockSpec(memory_space=pl.ANY)] * 4,
            out_specs=(spec,) * 3,
            scratch_shapes=[
                vm(3, NX, NY, 3 * Z), vm(*tab.shape), vm(GX, GY, 30, X, Y, Z), vm(2, packs, Y, Z), vm(GX, GY, 2, packs, Y, Z), vm(GX, 2, packs, YG, Z),
                vm(2 * SUBSTEPS + 1, 27, XG, YG, Z), vm(3, XG, YG, Z), vm(XG, 9, YG, Z), vm(XG + 1, 9, YG, Z),
                vm(2 * SUBSTEPS + 1, 27, NS, YG, Z), vm(3, NS, YG, Z), vm(NS, 9, YG, Z), vm(NS + 1, 9, YG, Z),
                vm(3 * Z, 3 * Z), vm(3 * NX, R, 3 * Z), vm(27, R, Z),
                vm(2, devices, 1, Z),
                vm(3, NX + 1, 4, R, Z), vm(3, NX + 1, 4, R, Z),
                vm(3, 3, NX + 1, 4, R, Z), vm(3, 3, X, 4, 4, R, Z), vm(3, 3, X, 4, 4, R, Z), vm(2, NX + 1, 4, R, Z), vm(X, 4, 4, R, Z), vm(R, Z),
                vm(3, 3, R, Z), vm(3, NX, 3, Z), vm(3, NX, 3, Z), vm(3, 3, Z), vm(R, Z), vm(4, R, Z),
                vm(2, 3, 4, R, Z), vm(2, 3, NX + 1, 4, Z), vm(2, 3, NX + 1, 4, Z), vm(2, 2, 3, 4, Z), vm(2, R, Z), vm(2, R, Z), vm(2, 4, 1, Z), vm(2, 8, 1, Z),
                dma(4), dma(GY), dma(GY), dma(GX, GY), dma(GX, GY), dma(2, GY), dma(2, GY), dma(GX), dma(GX), dma(2, 2), dma(2, 2), dma(7), dma(7), dma(26), dma(26),
            ],
            compiler_params=pltpu.CompilerParams(collective_id=0, has_side_effects=True),
        )(displacement, size_field_modes, velocity, tab)
        return tuple(
            pl.pallas_call(
                publish,
                out_shape=(
                    jax.ShapeDtypeStruct(size_field_modes.shape, jnp.float32),
                    jax.ShapeDtypeStruct(displacement.shape, jnp.float32),
                    jax.ShapeDtypeStruct((3,), jnp.float32),
                ),
                in_specs=[spec] * 3,
                out_specs=(pl.BlockSpec(memory_space=pl.ANY),) * 2 + (pl.BlockSpec(memory_space=pltpu.SMEM),),
                scratch_shapes=[dma(2)],
            )(*(pltpu.with_memory_space_constraint(a, pltpu.VMEM) for a in (adv, grad, checks)))
        )

    return jax.shard_map(
        on_device,
        mesh=mesh,
        in_specs=(P(None, "gx", "gy", "gz"),) * 3,
        out_specs=(P(None, "gx", "gy", "gz"), P(None, "gx", "gy", "gz"), P()),
        check_vma=False,
    )
```

```python
import functools

import jax
import jax.numpy as jnp
import numpy as np
from jax import lax
from jax.experimental import pallas as pl
from jax.experimental.pallas import tpu as pltpu
from jax.sharding import PartitionSpec as P

SUBSTEPS = 4
MESH = pl.DeviceIdType.MESH
AXES = ("gx", "gy", "gz")

plus_values = (0.7071067811865476, 1.224744871391589, 1.5811388300841898)
g10 = 1.7320508075688772
g21 = 3.872983346207417
courant = 0.1
theta_size = 0.3
trial_step = 0.05


def tables_1d():
    points = np.array(
        [-0.8611363115940526, -0.3399810435848563, 0.3399810435848563, 0.8611363115940526]
    )
    weights = np.array(
        [0.3478548451374538, 0.6521451548625461, 0.6521451548625461, 0.3478548451374538]
    )
    points = 0.5 * (points + 1.0)
    weights = 0.5 * weights
    nodes = np.array([0.0, 1.0 / 3.0, 2.0 / 3.0, 1.0])
    value = np.zeros((4, 4))
    slope = np.zeros((4, 4))
    for m in range(4):
        others = [nodes[o] for o in range(4) if o != m]
        den = np.prod([nodes[m] - o for o in others])
        for q in range(4):
            g = points[q]
            value[q, m] = np.prod([g - o for o in others]) / den
            slope[q, m] = (
                sum(np.prod([g - others[t] for t in range(3) if t != s]) for s in range(3)) / den
            )
    c = 2.0 * points - 1.0
    legendre = np.stack(
        [
            np.full(4, plus_values[0]),
            plus_values[1] * c,
            plus_values[2] * 0.5 * (3.0 * c**2 - 1.0),
        ],
        axis=1,
    )
    return value, slope, legendre, weights


def row_tables(Y, Z):
    value, slope, legendre, weights = tables_1d()
    rows, nodes = 4 * Y, 3 * Y + 1
    tv = np.zeros((rows, rows))
    td = np.zeros((rows, rows))
    for e in range(Y):
        tv[4 * e : 4 * e + 4, 3 * e : 3 * e + 4] = value
        td[4 * e : 4 * e + 4, 3 * e : 3 * e + 4] = slope
    blocks = [tv[:, j] for j in range(nodes)] + [td[:, j] for j in range(nodes)]
    blocks += [tv[s, :] for s in range(rows)] + [td[s, :] for s in range(rows)]
    for b in range(3):
        for e in range(Y):
            col = np.zeros(rows)
            col[4 * e : 4 * e + 4] = legendre[:, b]
            blocks.append(col)
    blocks.append(np.tile(weights, Y))
    blocks += [np.tile(value[:, m], Y) for m in range(4)] + [np.tile(slope[:, m], Y) for m in range(4)]
    stacked = np.stack(blocks).astype(np.float32)
    return np.ascontiguousarray(np.broadcast_to(stacked[:, :, None], stacked.shape + (Z,)))


def kernel(sizes, X, Y, Z, disp_in, modes_in, vel_in, tab_in, adv, grad, checks,
           disp, tab, GU, ZP, ZR, ZA, UM, VM, CM, FM, US, VS, CS, FT,
           perm, slab, U, ROWS, N, GN, A, G, J, B, SIZ, DT,
           NXR, NYS, NYR, NXYR, NZS, NZR, FXR, FYS, FYR, FXYR, FZS, FZR, FES, FER,
           ls, g1s, g1r, g2s, g2r, zs, zr, y2s, y2r, rs, rr, ns, nr, fs, fr):
    value, slope, legendre, weights = tables_1d()
    NX, NY = 3 * X, 3 * Y
    ROWS_Y = 4 * Y
    EL = X * Y
    f32 = jnp.float32
    index = [lax.axis_index(a) for a in AXES]
    lane = lax.broadcasted_iota(jnp.int32, (ROWS_Y, Z), 1)
    row = lax.broadcasted_iota(jnp.int32, (ROWS_Y, Z), 0)
    oTV, oTD, oGV, oGD, oL, oW = 0, NY + 1, 2 * NY + 2, 2 * NY + 2 + ROWS_Y, 2 * NY + 2 + 2 * ROWS_Y, 2 * NY + 2 + 2 * ROWS_Y + 3 * Y

    def at(axis, by):
        n = sizes[axis]
        return {AXES[axis]: lax.rem(index[axis] + (by + n), n)}

    barrier = pltpu.get_barrier_semaphore()
    total = 0
    for a in range(sizes[0]):
        for b in range(sizes[1]):
            for c in range(sizes[2]):
                move = (a, b, c)
                if not any(move) or (c and (a or b)):
                    continue
                target = {}
                for axis in range(3):
                    if move[axis]:
                        target.update(at(axis, move[axis]))
                pl.semaphore_signal(barrier, inc=1, device_id=target, device_id_type=MESH)
                total += 1

    loads = [
        pltpu.make_async_copy(modes_in, GU.at[0, 0, 0:27], ls.at[0]),
        pltpu.make_async_copy(vel_in, GU.at[0, 0, 27:30], ls.at[1]),
        pltpu.make_async_copy(disp_in, disp, ls.at[2]),
        pltpu.make_async_copy(tab_in, tab, ls.at[3]),
    ]
    for cp in loads:
        cp.start()

    def copy(src, dst, ss, sr, axis, by):
        return pltpu.make_async_remote_copy(
            src_ref=src, dst_ref=dst, send_sem=ss, recv_sem=sr,
            device_id=at(axis, by), device_id_type=MESH,
        )

    GX, GY = sizes[0], sizes[1]
    XG, YG, NS, EDGE = GX * X, GY * Y, GX * X // 2, 2 * SUBSTEPS
    HALF, FIELDS, SLOTS = Z // 2, 30, Z // EDGE

    def moved(move):
        target = {}
        for axis in range(3):
            if move[axis] % sizes[axis]:
                target.update(at(axis, move[axis] % sizes[axis] ))
        return target

    def remote(src, dst, ss, sr, move):
        return pltpu.make_async_remote_copy(
            src_ref=src, dst_ref=dst, send_sem=ss, recv_sem=sr,
            device_id=moved(move), device_id_type=MESH,
        )

    def plane_copy(ry):
        return remote(GU.at[0, 0], GU.at[0, ry], g1s.at[ry], g1r.at[ry], (0, -ry, 0))

    def core_copies(ry):
        return [
            remote(GU.at[0, ry], GU.at[rx, ry], g2s.at[rx, ry], g2r.at[rx, ry], (-rx, 0, 0))
            for rx in range(1, GX)
        ]

    def edge_copies():
        return [
            remote(ZP.at[side], ZR.at[0, 0, side], zs.at[side, 0], zr.at[side, 0], (0, 0, 2 * side - 1))
            for side in range(2)
        ]

    def edge_plane_copies():
        return [
            remote(ZR.at[0, 0], ZR.at[0, ry], zs.at[0, ry], zr.at[0, ry], (0, -ry, 0)) for ry in range(1, GY)
        ]

    def edge_core_copies():
        return [
            remote(ZR.at[0], ZR.at[rx], y2s.at[rx], y2r.at[rx], (-rx, 0, 0)) for rx in range(1, GX)
        ]

    slot2 = lax.broadcasted_iota(jnp.int32, (Y, Z), 1) // EDGE
    packs = -(-FIELDS * X // SLOTS)

    def pack_edges():
        acc = [[jnp.zeros((Y, Z), f32) for _ in range(packs)] for _ in range(2)]
        for m in range(FIELDS):
            for ix in range(X):
                t = m * X + ix
                v, p = t // SLOTS, EDGE * (t % SLOTS)
                x = GU[0, 0, m, ix]
                low = pltpu.roll(x, p, 1) if p else x
                high = pltpu.roll(x, (p + EDGE) % Z, 1) if (p + EDGE) % Z else x
                acc[0][v] = jnp.where(slot2 == t % SLOTS, low, acc[0][v])
                acc[1][v] = jnp.where(slot2 == t % SLOTS, high, acc[1][v])
        for side in range(2):
            for v in range(packs):
                ZP[side, v] = acc[side][v]

    def unweave():
        a_i = lax.broadcasted_iota(jnp.int32, (3 * Z, 3 * Z), 0)
        b_i = lax.broadcasted_iota(jnp.int32, (3 * Z, 3 * Z), 1)
        b_k = (b_i >= Z).astype(jnp.int32) + (b_i >= 2 * Z).astype(jnp.int32)
        perm[...] = (a_i == 3 * (b_i - b_k * Z) + b_k).astype(f32)
        slab[...] = jnp.zeros_like(slab)
        for c in range(3):
            for i in range(NX):
                slab[c * NX + i, 0:NY, :] = disp[c, i]
        spread = jnp.dot(
            slab[...].reshape(3 * NX * ROWS_Y, 3 * Z), perm[...],
            precision=lax.Precision.HIGHEST, preferred_element_type=f32,
        ).reshape(3, NX, ROWS_Y, 3 * Z)
        for c in range(3):
            for k in range(3):
                N[c, 0:NX, k] = spread[c, :, :, k * Z : (k + 1) * Z]

    devices = sizes[0] * sizes[1] * sizes[2]
    by_column = [(2,), (0, 1)]
    plans = [by_column, [(0, 1, 2)] if devices <= 64 else by_column]

    def row_stage(r, stage):
        block = 1
        stages = plans[r]
        for axes in stages[:stage]:
            for axis in axes:
                block *= sizes[axis]
        moves = [()]
        for axis in range(3):
            moves = [m + (b,) for m in moves for b in range(sizes[axis] if axis in stages[stage] else 1)]
        src = ROWS.at[r, 0:block]
        copies = [
            remote(src, ROWS.at[r, n * block : (n + 1) * block], rs.at[r, stage], rr.at[r, stage], m)
            for n, m in sorted(enumerate(moves), key=lambda nm: -sum(1 for b in nm[1] if b)) if n
        ]
        rest = ROWS.at[r, block : len(moves) * block]
        return copies, remote(rest, rest, rs.at[r, stage], rr.at[r, stage], moves[1])

    def rows_start(r, stage):
        for cp in row_stage(r, stage)[0]:
            cp.start()

    def rows_relay(r):
        for stage in range(len(plans[r]) - 1):
            row_stage(r, stage)[1].wait_recv()
            rows_start(r, stage + 1)

    def rows_finish(r):
        row_stage(r, len(plans[r]) - 1)[1].wait_recv()

    def rows_sent(r):
        for stage in range(len(plans[r])):
            row_stage(r, stage)[1].wait_send()

    in_lane = lambda n: functools.reduce(jnp.logical_or, [lane == c * (NX + 1) + n for c in range(3)])

    def rim_copies():
        out = [
            remote(N.at[:, 0, 0:3], NXR, ns.at[0], nr.at[0], (-1, 0, 0)),
            remote(NYS, NYR, ns.at[1], nr.at[1], (0, -1, 0)),
            remote(NYS.at[:, 0], NXYR, ns.at[2], nr.at[2], (-1, -1, 0)),
        ]
        return out

    def rim_column():
        return remote(NZS, NZR.at[0], ns.at[3], nr.at[3], (0, 0, -1))

    def rim_relays():
        return [
            remote(NZR.at[0], NZR.at[n], ns.at[3 + n], nr.at[3 + n], move)
            for n, move in ((1, (-1, 0, 0)), (2, (0, -1, 0)), (3, (-1, -1, 0)))
        ]

    def rim_pack():
        packed = jnp.zeros((ROWS_Y, Z), f32)
        for c in range(3):
            for i in range(NX):
                for k in range(3):
                    NYS[c, i, k : k + 1, :] = N[c, i, k, 0:1, :]
                packed = jnp.where(lane == c * (NX + 1) + i, N[c, i, 0][:, 0:1], packed)
        NZS[...] = packed

    def rim_unpack():
        for c in range(3):
            for k in range(3):
                N[c, NX, k] = NXR[c, k]
                N[c, NX, k, NY : NY + 1, :] = NXYR[c, k : k + 1, :]
                for i in range(NX):
                    N[c, i, k, NY : NY + 1, :] = NYR[c, i, k : k + 1, :]
        for c in range(3):
            for i in range(NX + 1):
                N[c, i, 3] = jnp.where(lane == Z - 1, 0.0, pltpu.roll(N[c, i, 0], Z - 1, 1))

    def rim_last():
        last = in_lane(NX)
        packed = jnp.where(last, pltpu.roll(NZR[1], NX, 1), NZR[0])
        below = jnp.where(last[0:1], pltpu.roll(NZR[3], NX, 1)[0:1], NZR[2][0:1])
        rows = [packed[j : j + 1] for j in range(NY)] + [below]
        pv = sum(tab[oTV + j] * rows[j] for j in range(NY + 1))
        pd = sum(tab[oTD + j] * rows[j] for j in range(NY + 1))
        end = lane == Z - 1
        for c in range(3):
            for i in range(NX + 1):
                n = c * (NX + 1) + i
                mv = jnp.where(end, pv[:, n : n + 1], 0.0)
                md = jnp.where(end, pd[:, n : n + 1], 0.0)
                for r in range(4):
                    A[0, c, i, r] = A[0, c, i, r] + float(value[r, 3]) * mv
                    A[1, c, i, r] = A[1, c, i, r] + float(value[r, 3]) * md
                    A[2, c, i, r] = A[2, c, i, r] + float(slope[r, 3]) * mv

    scale = [plus_values[m // 9] * plus_values[m // 3 % 3] * plus_values[m % 3] for m in range(27)]

    def assemble():
        def plane(x, carry):
            rx, ix = x // X, x % X
            for ry in range(GY):
                for m in range(FIELDS):
                    v = GU[rx, ry, m, ix]
                    if m < 27:
                        UM[0, m, x, ry * Y : ry * Y + Y, :] = scale[m] * v
                    else:
                        VM[m - 27, x, ry * Y : ry * Y + Y, :] = v
            return carry

        lax.fori_loop(0, XG, plane, 0)

    lanes = lax.broadcasted_iota(jnp.int32, (YG, Z), 1)
    W2, W3 = 2 * EDGE, 3 * EDGE

    def within(lo, hi):
        return (lanes >= lo) & (lanes < hi)

    def strip_own():
        def one(q, carry):
            for m in range(FIELDS):
                out = jnp.zeros((YG, Z), f32)
                for h in range(2):
                    t = UM[0, m, q + h * NS] if m < 27 else VM[m - 27, q + h * NS]
                    o = h * HALF
                    out = jnp.where(within(o, o + W2), pltpu.roll(t, o + W2, 1), out)
                    out = jnp.where(within(o + 2 * W2, o + 3 * W2), pltpu.roll(t, o + 2 * W2, 1), out)
                if m < 27:
                    US[0, m, q] = out
                else:
                    VS[m - 27, q] = out
            return carry

        lax.fori_loop(0, NS, one, 0)

    def strip_halo():
        for rx in range(GX):
            for ry in range(GY):
                ZA[rx, :, :, ry * Y : ry * Y + Y, :] = ZR[rx, ry]
        for q in range(NS):
            for m in range(FIELDS):
                out = US[0, m, q] if m < 27 else VS[m - 27, q]
                for h in range(2):
                    x = q + h * NS
                    rx, ix = x // X, x % X
                    t = m * X + ix
                    v, p = t // SLOTS, EDGE * (t % SLOTS)
                    for side in range(2):
                        o = h * HALF + W2 + side * EDGE
                        piece = ZA[rx, side, v]
                        by = (o - p) % Z
                        piece = pltpu.roll(piece, by, 1) if by else piece
                        if m < 27:
                            piece = scale[m] * piece
                        out = jnp.where(within(o, o + EDGE), piece, out)
                if m < 27:
                    US[0, m, q] = out
                else:
                    VS[m - 27, q] = out

    def ynext(t):
        return pltpu.roll(t, YG - 1, 0)

    def yprev(t):
        return pltpu.roll(t, 1, 0)

    def znext(t):
        return pltpu.roll(t, Z - 1, 1)

    def zprev(t):
        return pltpu.roll(t, 1, 1)

    def coefficients(V, C, nx, wrap):
        for q in range(nx):
            nxt = V[0, q + 1] if q < nx - 1 else wrap(V[0, 0])
            for d in range(3):
                v = V[d, q]
                ahead = nxt if d == 0 else ynext(v) if d == 1 else znext(v)
                face = 0.5 * (v + ahead)
                C[q, 3 * d] = jnp.maximum(face, 0.0)
                C[q, 3 * d + 1] = jnp.minimum(face, 0.0)
                C[q, 3 * d + 2] = 2.0 * v

    def line(u, hp, hm, v2, ahead, behind):
        e = u[0] + u[2]
        up = hp * (e + u[1]) + hm * ahead(e - u[1])
        low = behind(up)
        diff = low - up
        return diff, 3.0 * (v2 * u[0] - (low + up)), 5.0 * (v2 * u[1] + diff)

    def rate(src, dst, C, F, nx, wrap):
        for n in range(9):
            tp, tm = [], []
            for q in range(nx):
                u0, u1, u2 = src[n, q], src[9 + n, q], src[18 + n, q]
                e = u0 + u2
                tp.append(e + u1)
                tm.append(e - u1)
            for q in range(nx):
                nxt = tm[q + 1] if q < nx - 1 else wrap(tm[0])
                f = C[q, 0] * tp[q] + C[q, 1] * nxt
                F[q + 1, n] = f
                if q == nx - 1:
                    F[0, n] = wrap(f)

        def block(q, carry):
            vx = C[q, 2]
            for a in range(3):
                u = [src[9 * a + n, q] for n in range(9)]
                acc = []
                for n in range(9):
                    up, low = F[q + 1, n], F[q, n]
                    if a == 0:
                        acc.append(low - up)
                    elif a == 1:
                        acc.append(3.0 * (vx * src[n, q] - (low + up)))
                    else:
                        acc.append(5.0 * (vx * src[9 + n, q] + (low - up)))
                for d, st, ot, ahead, behind in ((1, 3, 1, ynext, yprev), (2, 1, 3, znext, zprev)):
                    hp, hm, v2 = C[q, 3 * d], C[q, 3 * d + 1], C[q, 3 * d + 2]
                    for o in range(3):
                        at_ = [ot * o + st * t for t in range(3)]
                        out = line([u[t] for t in at_], hp, hm, v2, ahead, behind)
                        for t in range(3):
                            acc[at_[t]] = acc[at_[t]] + out[t]
                for n in range(9):
                    dst[9 * a + n, q] = acc[n]
            return carry

        if nx <= 4:
            for q in range(nx):
                block(q, 0)
        else:
            lax.fori_loop(0, nx, block, 0)

    def powers(P, C, F, nx, wrap, first, last):
        def one(k, carry):
            rate(P.at[k], P.at[k + 1], C, F, nx, wrap)
            return carry

        lax.fori_loop(first, last, one, 0)

    def same(t):
        return t

    def half_turn(t):
        return pltpu.roll(t, HALF, 1)

    taylor = np.polynomial.polynomial.polypow([1.0, 1.0, 0.5], SUBSTEPS)

    def finish_field():
        U[...] = jnp.zeros_like(U)
        dt = DT[...]
        weight, power = [], None
        for k in range(1, 2 * SUBSTEPS + 1):
            power = dt if power is None else power * dt
            weight.append(float(taylor[k]) * power)

        def summed(P, m, q):
            out = P[0, m, q]
            for k in range(1, 2 * SUBSTEPS + 1):
                out = out + weight[k - 1] * P[k, m, q]
            return out

        for m in range(27):
            for ix in range(X):
                h, q = ix // NS, ix % NS
                t, s = summed(UM, m, ix), summed(US, m, q)
                o = h * HALF
                left = pltpu.roll(s, (Z - o - 2 * W2) % Z, 1)
                right = pltpu.roll(s, (Z - W2 - o) % Z, 1)
                t = jnp.where(lanes < EDGE, left, jnp.where(lanes >= Z - EDGE, right, t))
                U[m, ix * Y : ix * Y + Y, :] = (1.0 / scale[m]) * t[0:Y]

    def apply(T, x, anti, parts=None):
        e0, e1, o0, o1 = parts or (x[0] + x[3], x[1] + x[2], x[0] - x[3], x[1] - x[2])
        out = [None] * 4
        for p in range(2):
            a = float(0.5 * (T[p, 0] + T[p, 3])) * e0 + float(0.5 * (T[p, 1] + T[p, 2])) * e1
            b = float(0.5 * (T[p, 0] - T[p, 3])) * o0 + float(0.5 * (T[p, 1] - T[p, 2])) * o1
            out[p] = a + b
            out[3 - p] = b - a if anti else a - b
        return out

    def halves(x):
        return x[0] + x[3], x[1] + x[2], x[0] - x[3], x[1] - x[2]

    oM = oW + 1
    element = row // 4

    def yz_of(src):
        def yz(i, carry):
            for c in range(3):
                yv, yd = [], []
                for k in range(4):
                    sv = sd = None
                    for m in range(4):
                        x = src[c, i, k, 3 * (Y - 1) + m : 3 * (Y - 1) + m + 1, :]
                        for e in range(Y - 2, -1, -1):
                            x = jnp.where(element == e, src[c, i, k, 3 * e + m : 3 * e + m + 1, :], x)
                        tv, td = tab[oM + m] * x, tab[oM + 4 + m] * x
                        sv = tv if sv is None else sv + tv
                        sd = td if sd is None else sd + td
                    yv.append(sv)
                    yd.append(sd)
                parts = halves(yv)
                outs = apply(value, yv, False, parts), apply(value, yd, False), apply(slope, yv, True, parts)
                for d in range(3):
                    for r in range(4):
                        A[d, c, i, r] = outs[d][r]
            return carry

        lax.fori_loop(0, NX + 1, yz, 0)

    def slopes_at(ix, r, c, d):
        tb = slope if d == 0 else value
        return apply(tb, [A[d, c, 3 * ix + m, r] for m in range(4)], d == 0)

    def jacobians(t):
        ix, r = t // 4, t % 4
        for c in range(3):
            for d in range(3):
                jac = slopes_at(ix, r, c, d)
                for p in range(4):
                    J[d, c, ix, p, r] = jac[p] + 1.0 if c == d else jac[p]

    for cp in loads[:2]:
        cp.wait()
    pl.semaphore_wait(barrier, total)
    for cp in core_copies(0):
        cp.start()
    for ry in range(1, GY):
        plane_copy(ry).start()
    speed = None
    for ix in range(X):
        here = jnp.abs(GU[0, 0, 27, ix]) + jnp.abs(GU[0, 0, 28, ix]) + jnp.abs(GU[0, 0, 29, ix])
        speed = here if speed is None else jnp.maximum(speed, here)
    ROWS[0, 0] = jnp.max(speed, axis=0, keepdims=True)
    rows_start(0, 0)
    pack_edges()
    for cp in edge_copies():
        cp.start()
    loads[2].wait()
    unweave()
    rim_pack()
    rim_column().start()
    for cp in rim_copies():
        cp.start()
    loads[3].wait()
    for cp in edge_copies():
        cp.wait_recv()
    for cp in edge_plane_copies():
        cp.start()
    for ry in range(1, GY):
        plane_copy(ry).wait_recv()
        for cp in core_copies(ry):
            cp.start()
    rows_relay(0)
    rim_column().wait_recv()
    for cp in rim_relays():
        cp.start()
    for cp in rim_copies():
        cp.wait()
    rim_unpack()
    yz_of(N)
    for ry in range(GY):
        for cp in core_copies(ry):
            cp.wait_recv()
    assemble()
    strip_own()
    coefficients(VM, CM, XG, same)
    for cp in edge_plane_copies():
        cp.wait_recv()
    for cp in edge_core_copies():
        cp.start()
    powers(UM, CM, FM, XG, same, 0, 2 * SUBSTEPS)
    for cp in rim_relays():
        cp.wait_recv()
    rim_last()

    def all_jacobians(t, carry):
        jacobians(t)
        return carry

    lax.fori_loop(0, 4 * X, all_jacobians, 0)
    for cp in edge_core_copies():
        cp.wait_recv()
    strip_halo()
    coefficients(VS, CS, NS, half_turn)
    powers(US, CS, FT, NS, half_turn, 0, 2 * SUBSTEPS)
    rows_finish(0)
    fastest = functools.reduce(jnp.maximum, [ROWS[0, n] for n in range(devices)])
    fastest = jnp.max(fastest, axis=(0, 1), keepdims=True)
    DT[...] = jnp.broadcast_to(courant / jnp.maximum(fastest, 0.25), (YG, Z))
    finish_field()
    def size_of(ix, carry):
        mid = {}
        for a in range(3):
            for r in range(4):
                mid[a, r] = None
            for c in range(3):
                t = None
                for b in range(3):
                    for e in range(Y):
                        term = tab[oL + b * Y + e] * U[a * 9 + b * 3 + c, pl.ds(ix * Y + e, 1), :]
                        t = term if t is None else t + term
                for r in range(4):
                    term = float(legendre[r, c]) * t
                    mid[a, r] = term if mid[a, r] is None else mid[a, r] + term
        for p in range(4):
            for r in range(4):
                s = sum(float(legendre[p, a]) * mid[a, r] for a in range(3))
                SIZ[ix, p, r] = jnp.exp(theta_size * s)
        return carry

    lax.fori_loop(0, X, size_of, 0)

    wrow = tab[oW]
    pairs = [(d, e) for d in range(3) for e in range(d, 3)]

    def dot3(p, q, d, e):
        return p[0][d] * q[0][e] + p[1][d] * q[1][e] + p[2][d] * q[2][e]

    def gauss_weight(r):
        return jnp.where((r == 0) | (r == 3), float(weights[0]), float(weights[1]))

    def gauss(t, esum):
        ix, r = t // 4, t % 4
        for p in range(4):
            size = SIZ[ix, p, r]
            inv = 1.0 / size
            M = [[J[d, c, ix, p, r] * inv for d in range(3)] for c in range(3)]
            D = [[None] * 3 for _ in range(3)]
            metric = None
            for d, e in pairs:
                dev = dot3(M, M, d, e)
                if d == e:
                    dev = dev - 1.0
                D[d][e] = D[e][d] = dev
                sq = dev * dev if d == e else 2.0 * (dev * dev)
                metric = sq if metric is None else metric + sq
            w = wrow * (gauss_weight(r) * float(weights[p]))
            size2 = size * size
            esum = esum + w * (size2 * size) * metric
            scale = (4.0 * w) * size2
            for c in range(3):
                for d in range(3):
                    g = M[c][0] * D[0][d] + M[c][1] * D[1][d] + M[c][2] * D[2][d]
                    G[d, c, ix, p, r] = scale * g
        return esum

    zero = jnp.zeros((ROWS_Y, Z), f32)
    esum = lax.fori_loop(0, 4 * X, gauss, zero)

    def back_c(c, carry):
        spread = [[[None] * (NX + 1) for _ in range(4)] for _ in range(3)]
        for d in range(3):
            tb = slope if d == 0 else value
            for r in range(4):
                for ix in range(X):
                    out = apply(tb.T, [G[d, c, ix, p, r] for p in range(4)], d == 0)
                    for m in range(4):
                        was = spread[d][r][3 * ix + m]
                        spread[d][r][3 * ix + m] = out[m] if was is None else was + out[m]
        for i in range(NX + 1):
            ga = [[spread[d][r][i] for r in range(4)] for d in range(3)]
            first, third = apply(value.T, ga[0], False), apply(slope.T, ga[2], True)
            bv = [first[k] + third[k] for k in range(4)]
            bd = apply(value.T, ga[1], False)
            for k in range(4):
                B[0, i, k] = bv[k]
                B[1, i, k] = bd[k]
        for i in range(NX + 1):
            for k in range(4):
                acc = None
                for s in range(ROWS_Y):
                    term = tab[oGV + s] * B[0, i, k, s : s + 1, :] + tab[oGD + s] * B[1, i, k, s : s + 1, :]
                    acc = term if acc is None else acc + term
                GN[c, i, k] = acc
        return carry

    lax.fori_loop(0, 3, back_c, 0)

    def row_of(column_of):
        out = zero
        for c in range(3):
            out = jnp.where(lane == c * ROWS_Y + row, column_of(c), out)
        return jnp.sum(out, axis=0, keepdims=True)

    far, near = zero, zero
    for c in range(3):
        for i in range(NX + 1):
            here = lane == c * (NX + 1) + i
            far = jnp.where(here, GN[c, i, 3][:, Z - 1 : Z], far)
            near = jnp.where(here, GN[c, i, 0][:, 0:1], near)
    FZS[0] = far
    FZS[1] = near
    for zs_, (k, at_) in enumerate(((3, Z - 1), (0, 0))):
        for xs_, i in enumerate((NX, 0)):
            FES[zs_, xs_] = row_of(lambda c: GN[c, i, k][:, at_ : at_ + 1])
        for ys_, j in enumerate((NY, 0)):
            FES[zs_, 2 + ys_] = FZS[zs_][j : j + 1]
    for c in range(3):
        for i in range(NX + 1):
            GN[c, i, 0] = GN[c, i, 0] + jnp.where(lane == 0, 0.0, pltpu.roll(GN[c, i, 3], 1, 1))
            for k in range(4):
                FYS[0, c, i, k : k + 1, :] = GN[c, i, k, NY : NY + 1, :]
                FYS[1, c, i, k : k + 1, :] = GN[c, i, k, 0:1, :]
    ways = (1, -1)

    def fold_copies():
        out = []

        def add(src, dst, move):
            n = len(out)
            out.append(remote(src, dst, fs.at[n], fr.at[n], move))

        for zs_ in range(2):
            for xs_ in range(2):
                for ys_ in range(2):
                    add(FES.at[zs_, xs_], FER.at[zs_, 4 + 2 * xs_ + ys_], (ways[xs_], ways[ys_], ways[zs_]))
            for ys_ in range(2):
                add(FES.at[zs_, 2 + ys_], FER.at[zs_, 2 + ys_], (0, ways[ys_], ways[zs_]))
            for xs_ in range(2):
                add(FES.at[zs_, xs_], FER.at[zs_, xs_], (ways[xs_], 0, ways[zs_]))
            add(FZS.at[zs_], FZR.at[zs_], (0, 0, ways[zs_]))
        for ys_ in range(2):
            for xs_ in range(2):
                add(FYS.at[ys_, :, (NX, 0)[xs_]], FXYR.at[xs_, ys_], (ways[xs_], ways[ys_], 0))
            add(FYS.at[ys_], FYR.at[ys_], (0, ways[ys_], 0))
        for xs_ in range(2):
            add(GN.at[:, (NX, 0)[xs_]], FXR.at[xs_], (ways[xs_], 0, 0))
        return out

    for cp in fold_copies():
        cp.start()
    for cp in fold_copies():
        cp.wait()

    lane1, row_j = lane[0:1], lane[0:1] % ROWS_Y
    planes = []
    for zs_ in range(2):
        p = FZR[zs_]
        p = p + jnp.where(row == 0, FER[zs_, 2], 0.0) + jnp.where(row == NY, FER[zs_, 3], 0.0)
        for xs_, i in enumerate((0, NX)):
            edge = FER[zs_, xs_]
            edge = edge + jnp.where(row_j == 0, pltpu.roll(FER[zs_, 4 + 2 * xs_], Z - NY, 1), 0.0)
            edge = edge + jnp.where(row_j == NY, pltpu.roll(FER[zs_, 5 + 2 * xs_], NY, 1), 0.0)
            for c in range(3):
                col = jnp.sum(jnp.where(lane == c * ROWS_Y + row, edge, 0.0), axis=1, keepdims=True)
                p = p + jnp.where(lane == c * (NX + 1) + i, col, 0.0)
        planes.append(p)
    first_row, last_row = row == 0, row == NY
    ssum = zero
    for c in range(3):
        for i in range(NX + 1):
            n = c * (NX + 1) + i
            out = []
            for k in range(4):
                low, high = FYR[0, c, i, k : k + 1, :], FYR[1, c, i, k : k + 1, :]
                g = GN[c, i, k]
                if i in (0, NX):
                    xs_ = 0 if i == 0 else 1
                    g = g + FXR[xs_, c, k]
                    low = low + FXYR[xs_, 0, c, k : k + 1, :]
                    high = high + FXYR[xs_, 1, c, k : k + 1, :]
                out.append(g + jnp.where(first_row, low, jnp.where(last_row, high, 0.0)))
            out[0] = out[0] + jnp.where(lane == 0, planes[0][:, n : n + 1], 0.0)
            out[3] = jnp.where(lane == Z - 1, out[3] + planes[1][:, n : n + 1], pltpu.roll(out[0], Z - 1, 1))
            for k in range(4):
                GN[c, i, k] = out[k]
                if i < NX and k < 3:
                    ssum = ssum + out[k] * out[k]
    ssum = jnp.where(row < NY, ssum, 0.0)
    elements = float(EL * Z * devices)
    entries = 81.0 * elements
    mine = jnp.sum(ssum, axis=(0, 1), keepdims=True)
    bound = trial_step / jnp.sqrt(1.0 + mine / entries)
    bound = jnp.broadcast_to(bound, (ROWS_Y, Z))
    yz_of(GN)

    def trial(t, sums):
        ix, r = t // 4, t % 4
        s2, s3, s4 = sums
        moves = [[slopes_at(ix, r, c, d) for d in range(3)] for c in range(3)]
        for p in range(4):
            size = SIZ[ix, p, r]
            inv = 1.0 / size
            move = -(inv * bound)
            M = [[J[d, c, ix, p, r] * inv for d in range(3)] for c in range(3)]
            K = [[moves[c][d][p] * move for d in range(3)] for c in range(3)]
            w = wrow * (gauss_weight(r) * float(weights[p])) * (size * size * size)
            q = [[None] * 4, [None] * 4]
            for d, e in pairs:
                d0 = dot3(M, M, d, e)
                d2 = dot3(K, K, d, e)
                if d == e:
                    d0 = d0 - 1.0
                    d1 = 2.0 * dot3(M, K, d, d)
                else:
                    d1 = dot3(M, K, d, e) + dot3(K, M, d, e)
                terms, own = (d1 * d1, d0 * d2, d1 * d2, d2 * d2), q[0 if d == e else 1]
                for n in range(4):
                    own[n] = terms[n] if own[n] is None else own[n] + terms[n]
            full = [q[0][n] + 2.0 * q[1][n] for n in range(4)]
            s2 = s2 + w * (full[0] + 2.0 * full[1])
            s3 = s3 + w * (2.0 * full[2])
            s4 = s4 + w * full[3]
        return s2, s3, s4

    sums = lax.fori_loop(0, 4 * X, trial, (zero,) * 3)
    block = zero
    for n, part in enumerate((esum, ssum) + tuple(sums)):
        block = jnp.where(row == n, jnp.sum(part, axis=0, keepdims=True), block)
    column = jnp.sum(block, axis=1, keepdims=True)
    sent = jnp.sum(jnp.where(lane == row, column, 0.0), axis=0, keepdims=True)
    ROWS[1, 0] = jnp.where(lane[0:1] < HALF, sent, 1.0 / bound[0:1])
    rows_start(1, 0)
    for c in range(3):
        for k in range(3):
            slab[c * NX : (c + 1) * NX, :, k * Z : (k + 1) * Z] = GN[c, 0:NX, k]
    woven = lax.dot_general(
        slab[...].reshape(3 * NX * ROWS_Y, 3 * Z), perm[...], (((1,), (1,)), ((), ())),
        precision=lax.Precision.HIGHEST, preferred_element_type=f32,
    ).reshape(3, NX, ROWS_Y, 3 * Z)
    grad[...] = woven[:, :, 0:NY, :]
    for ix in range(X):
        adv[:, ix] = U[:, ix * Y : ix * Y + Y, :]
    for ry in range(GY):
        if ry:
            plane_copy(ry).wait_send()
        for cp in core_copies(ry):
            cp.wait_send()
    for cp in edge_copies() + edge_plane_copies() + edge_core_copies() + [rim_column()] + rim_relays():
        cp.wait_send()
    rows_sent(0)
    rows_sent(1)
    rows_relay(1)
    rows_finish(1)
    every = [ROWS[1, n] for n in range(devices)]
    l1 = lax.broadcasted_iota(jnp.int32, (1, Z), 1)

    def lane_sum(x, n):
        return jnp.sum(jnp.where(l1 == n, x, 0.0), axis=1, keepdims=True)

    sums = sum(every)
    etot, stot = lane_sum(sums, 0), lane_sum(sums, 1)
    step = trial_step / jnp.sqrt(1.0 + stot / entries)
    higher = jnp.zeros((1, Z), f32)
    for x in every:
        h = step * pltpu.roll(x, HALF, 1)
        h2 = h * h
        power = jnp.where(l1 == 2, h2, jnp.where(l1 == 3, h2 * h, h2 * h2))
        higher = higher + x * power
    higher = jnp.sum(jnp.where((l1 >= 2) & (l1 < 5), higher, 0.0), axis=1, keepdims=True)
    ttot = (etot - step * stot) + higher
    checks[...] = jnp.where(
        l1 == 0, etot / elements, jnp.where(l1 == 1, stot / entries, ttot / elements)
    )


def publish(adv, grad, checks, adv_out, grad_out, checks_out, sem):
    copies = [
        pltpu.make_async_copy(grad, grad_out, sem.at[0]),
        pltpu.make_async_copy(adv, adv_out, sem.at[1]),
    ]
    for cp in copies:
        cp.start()
    row = checks[...]
    lane = lax.broadcasted_iota(jnp.int32, row.shape, 1)
    for n in range(3):
        checks_out[n] = jnp.sum(jnp.where(lane == n, row, 0.0))
    for cp in copies:
        cp.wait()


def solution(mesh):
    sizes = tuple(mesh.shape[a] for a in AXES)

    def on_device(displacement, size_field_modes, velocity):
        modes, X, Y, Z = size_field_modes.shape
        assert Y == 2 and displacement.shape == (3, 3 * X, 3 * Y, 3 * Z)
        R, NX, NY = 4 * Y, 3 * X, 3 * Y
        tab = jnp.asarray(row_tables(Y, Z))
        devices = sizes[0] * sizes[1] * sizes[2]
        GX, GY = sizes[0], sizes[1]
        XG, YG, NS = GX * X, GY * Y, GX * X // 2
        packs = -(-30 * X // (Z // (2 * SUBSTEPS)))
        assert YG == 8 and XG % 2 == 0 and min(sizes) > 1
        vm = lambda *shape: pltpu.VMEM(shape, jnp.float32)
        dma = lambda *shape: pltpu.SemaphoreType.DMA(shape)
        spec = pl.BlockSpec(memory_space=pltpu.VMEM)
        adv, grad, checks = pl.pallas_call(
            functools.partial(kernel, sizes, X, Y, Z),
            out_shape=(
                pltpu.VMEM(size_field_modes.shape, jnp.float32),
                pltpu.VMEM(displacement.shape, jnp.float32),
                pltpu.VMEM((1, Z), jnp.float32),
            ),
            in_specs=[pl.BlockSpec(memory_space=pl.ANY)] * 4,
            out_specs=(spec,) * 3,
            scratch_shapes=[
                vm(3, NX, NY, 3 * Z), vm(*tab.shape), vm(GX, GY, 30, X, Y, Z), vm(2, packs, Y, Z), vm(GX, GY, 2, packs, Y, Z), vm(GX, 2, packs, YG, Z),
                vm(2 * SUBSTEPS + 1, 27, XG, YG, Z), vm(3, XG, YG, Z), vm(XG, 9, YG, Z), vm(XG + 1, 9, YG, Z),
                vm(2 * SUBSTEPS + 1, 27, NS, YG, Z), vm(3, NS, YG, Z), vm(NS, 9, YG, Z), vm(NS + 1, 9, YG, Z),
                vm(3 * Z, 3 * Z), vm(3 * NX, R, 3 * Z), vm(27, R, Z),
                vm(2, devices, 1, Z),
                vm(3, NX + 1, 4, R, Z), vm(3, NX + 1, 4, R, Z),
                vm(3, 3, NX + 1, 4, R, Z), vm(3, 3, X, 4, 4, R, Z), vm(3, 3, X, 4, 4, R, Z), vm(2, NX + 1, 4, R, Z), vm(X, 4, 4, R, Z), vm(R, Z),
                vm(3, 3, R, Z), vm(3, NX, 3, Z), vm(3, NX, 3, Z), vm(3, 3, Z), vm(R, Z), vm(4, R, Z),
                vm(2, 3, 4, R, Z), vm(2, 3, NX + 1, 4, Z), vm(2, 3, NX + 1, 4, Z), vm(2, 2, 3, 4, Z), vm(2, R, Z), vm(2, R, Z), vm(2, 4, 1, Z), vm(2, 8, 1, Z),
                dma(4), dma(GY), dma(GY), dma(GX, GY), dma(GX, GY), dma(2, GY), dma(2, GY), dma(GX), dma(GX), dma(2, 2), dma(2, 2), dma(7), dma(7), dma(26), dma(26),
            ],
            compiler_params=pltpu.CompilerParams(collective_id=0, has_side_effects=True),
        )(displacement, size_field_modes, velocity, tab)
        return tuple(
            pl.pallas_call(
                publish,
                out_shape=(
                    jax.ShapeDtypeStruct(size_field_modes.shape, jnp.float32),
                    jax.ShapeDtypeStruct(displacement.shape, jnp.float32),
                    jax.ShapeDtypeStruct((3,), jnp.float32),
                ),
                in_specs=[spec] * 3,
                out_specs=(pl.BlockSpec(memory_space=pl.ANY),) * 2 + (pl.BlockSpec(memory_space=pltpu.SMEM),),
                scratch_shapes=[dma(2)],
            )(*(pltpu.with_memory_space_constraint(a, pltpu.VMEM) for a in (adv, grad, checks)))
        )

    return jax.shard_map(
        on_device,
        mesh=mesh,
        in_specs=(P(None, "gx", "gy", "gz"),) * 3,
        out_specs=(P(None, "gx", "gy", "gz"), P(None, "gx", "gy", "gz"), P()),
        check_vma=False,
    )
```
